256 devices in a mesh: depth: 8 (over z), col: 4 (over y), row: 8 (over x, core).
Axes of the slice: x: 4, y: 4, z: 8, core: 2. Of those that a mesh axis runs over, the one named last changes fastest.
Arguments:
- a_mat: bfloat16 [16384, 16384], P(('row', 'depth'), 'col')
- b_mat: bfloat16 [16384, 16384], P(('row', 'depth'), 'col')
Outputs:
- output: bfloat16 [16384, 16384], P(('row', 'depth'), 'col')
All inputs are finite; a program needn't handle non-finite values.
Results may differ from the reference program's by a relative error of at most 0.001.
Values are sent between devices in bfloat16 or wider.
A program may use at most 768 MiB of HBM per device.

```python
import jax
import jax.numpy as jnp

N = 16384


def setup_inputs(seed: int = 0) -> dict:
    key_a, key_b = jax.random.split(jax.random.key(seed))
    unit_scale = N ** -0.25
    a_vals = jax.random.normal(key_a, (N, N), jnp.float32) + unit_scale
    b_vals = jax.random.normal(key_b, (N, N), jnp.float32) + unit_scale
    a_mat = (a_vals * unit_scale).astype(jnp.bfloat16)
    b_mat = (b_vals * unit_scale).astype(jnp.bfloat16)
    return {"a_mat": a_mat, "b_mat": b_mat}


def reference(a_mat, b_mat):
    return jnp.dot(a_mat, b_mat, preferred_element_type=jnp.float32).astype(jnp.bfloat16)
```

```python
import jax
import jax.numpy as jnp
from jax import lax
from jax.sharding import PartitionSpec as P


def solution(mesh):
    def local_product(a_blk, b_blk):
        b_full = lax.all_gather(b_blk, "depth", axis=0, tiled=True)
        a_rows = lax.all_gather(a_blk, "col", axis=1, tiled=True)
        a_k = lax.all_to_all(a_rows, "row", split_axis=1, concat_axis=0, tiled=True)
        part = jnp.dot(a_k, b_full, preferred_element_type=jnp.float32)
        c_part = lax.psum_scatter(part, "row", scatter_dimension=0, tiled=True)
        return c_part.astype(jnp.bfloat16)

    block_spec = P(("row", "depth"), "col")
    return jax.shard_map(local_product, mesh=mesh, in_specs=(block_spec, block_spec), out_specs=block_spec, check_vma=False)
```

```python
import functools

import jax
import jax.numpy as jnp
from jax import lax
from jax.experimental import pallas as pl
from jax.experimental.pallas import tpu as pltpu
from jax.sharding import PartitionSpec as P

MESH = pl.DeviceIdType.MESH
X_N, Y_N, Z_N = 4, 4, 8
CHUNKS = 16
C0_SLOTS = 4
OUT_SLOTS = 4

A_SCHEDULE = (
    (-1, ("s1", 0)), (0, ("r1", 0)), (3, ("s1", 1)), (4, ("s2", 0)), (4, ("s2f", 0)), (5, ("r1", 1)),
    (8, ("ag", 0)), (8, ("s2f", 1)), (8, ("s2", 1)), (8, ("r2", 0)), (11, ("r2", 1)), (11, ("fw", 0, 0)),
    (12, ("fw", 0, 1)), (14, ("ag", 1)), (15, ("gw", 0)), (18, ("fw", 1, 0)), (19, ("fw", 1, 1)),
    (22, ("ag", 2)), (22, ("gw", 1)), (25, ("fw", 2, 0)), (26, ("fw", 2, 1)), (29, ("ag", 3)), (29, ("gw", 2)),
    (38, ("fw", 3, 0)), (43, ("fw", 3, 1)), (45, ("gw", 3)),
)
C_BASE = (10, 14, 19, 28)
C_START = (15, 22, 29, 45)


def kernel(a_hbm, b_hbm, c_hbm, a_all, s1, rl1, rl2, b_all, crecv, c0, outst,
           bl_sem, zr_sem, zs_sem, dr_sem, s1_sem, r1_sem, r2_sem, s2_sem, ag_sem, fw_sem, as_sem,
           cr_sem, cs_sem, c0_sem, out_sem):
    row, y, z = lax.axis_index("row"), lax.axis_index("col"), lax.axis_index("depth")
    x, c = row // 2, row % 2
    width = b_all.shape[3]
    rows_q = s1.shape[2]
    half = rows_q // 2
    lo, hi = pl.ds(0, half), pl.ds(half, half)

    def at_x(dx):
        return {"row": 2 * ((x + dx + X_N) % X_N) + c}

    def at_y(dy):
        return {"col": (y + dy + Y_N) % Y_N}

    step = 1 - 2 * c
    z_long = {"depth": (z + step + Z_N) % Z_N}
    z_short = {"depth": (z - step + Z_N) % Z_N}
    partner = {"row": 2 * x + 1 - c}

    def send(src, dst, ssem, rsem, dev):
        pltpu.make_async_remote_copy(src_ref=src, dst_ref=dst, send_sem=ssem, recv_sem=rsem,
                                     device_id=dev, device_id_type=MESH).start()

    def wait(ref, sem):
        pltpu.make_async_copy(ref, ref, sem).wait()

    e_own = (y - x + Y_N) % Y_N
    flip = e_own // 3
    j_own = e_own

    def b_local(m):
        return pltpu.make_async_copy(b_hbm.at[:, pl.ds(pl.multiple_of(m * width, width), width)],
                                     b_all.at[m, c * Z_N + z], bl_sem.at[m])

    b_local(0).start()

    barrier = pltpu.get_barrier_semaphore()
    for dev in (at_x(1), at_x(-1), at_y(1), at_y(-1), z_long, z_short, partner):
        pl.semaphore_signal(barrier, inc=1, device_id=dev, device_id_type=MESH)
    lax.fori_loop(1, CHUNKS, lambda m, _: (b_local(m).start(), 0)[1], 0)
    pl.semaphore_wait(barrier, 7)

    def s1_dst(e, o, j, rows=None):
        def final():
            return a_all.at[3, o, j] if rows is None else a_all.at[3, o, j, rows]

        def staged():
            return s1.at[(e + Y_N - 1) % Y_N, o] if rows is None else s1.at[(e + Y_N - 1) % Y_N, o, rows]
        return final, staged

    def by_e(e, o, j, rows, fn):
        final, staged = s1_dst(e, o, j, rows)

        @pl.when(e == 0)
        def _():
            fn(final())

        @pl.when(e != 0)
        def _():
            fn(staged())

    def a_event(event):
        kind = event[0]
        if kind == "s1":
            o = event[1]
            h = (o + flip) % 2
            send(a_hbm.at[h, 2, lo], rl1.at[0, o], as_sem.at[0], r1_sem.at[0, o], at_y(1))
            send(a_hbm.at[h, 2, hi], rl1.at[1, o], as_sem.at[0], r1_sem.at[1, o], at_y(-1))
            sem = s1_sem.at[e_own, o]
            by_e(e_own, o, 1, None, lambda dst: send(a_hbm.at[h, 1], dst, as_sem.at[0], sem, at_y(1)))
            by_e(e_own, o, 3, None, lambda dst: send(a_hbm.at[h, 3], dst, as_sem.at[0], sem, at_y(-1)))
            by_e(e_own, o, 0, None, lambda dst: pltpu.make_async_copy(a_hbm.at[h, 0], dst, sem).start())
        elif kind == "r1":
            o = event[1]
            for d, dy, rows in ((0, 1, lo), (1, -1, hi)):
                e = (y - dy - x + 2 * Y_N) % Y_N
                wait(rl1.at[d, o], r1_sem.at[d, o])
                by_e(e, o, 2, rows, lambda dst: send(rl1.at[d, o], dst, as_sem.at[0], s1_sem.at[e, o], at_y(dy)))
        elif kind == "s2":
            o = event[1]
            wait(s1.at[0, o], s1_sem.at[1, o])
            wait(s1.at[2, o], s1_sem.at[3, o])
            g = 2 * o
            j = (y - x - 1 + 2 * Y_N) % Y_N
            send(s1.at[0, o], a_all.at[g, o, j], as_sem.at[1], s2_sem.at[g, o], at_x(1))
            j = (y - x + 1 + Y_N) % Y_N
            send(s1.at[2, o], a_all.at[g, 1 - o, j], as_sem.at[1], s2_sem.at[g, 1 - o], at_x(-1))
        elif kind == "s2f":
            o = event[1]
            wait(s1.at[1, o], s1_sem.at[2, o])
            send(s1.at[1, o, lo], rl2.at[0, o], as_sem.at[1], r2_sem.at[0, o], at_x(1))
            send(s1.at[1, o, hi], rl2.at[1, o], as_sem.at[1], r2_sem.at[1, o], at_x(-1))
        elif kind == "r2":
            o = event[1]
            for d, dx, rows in ((0, 1, lo), (1, -1, hi)):
                j = (y - x - dx + 2 * Y_N) % Y_N
                wait(rl2.at[d, o], r2_sem.at[d, o])
                send(rl2.at[d, o], a_all.at[1, o, j, rows], as_sem.at[1], s2_sem.at[1, o], at_x(dx))
        elif kind == "ag":
            g = event[1]
            for d in range(2):
                mine = a_all.at[g, d, j_own]
                wait(mine, s1_sem.at[0, d] if g == 3 else s2_sem.at[g, d])
                send(mine, mine, as_sem.at[2 + g], ag_sem.at[g, d, 0], at_y(1))
                send(mine, mine, as_sem.at[2 + g], ag_sem.at[g, d, 1], at_y(-1))
        elif kind == "fw":
            g, d = event[1:]
            for k, dy, rows in ((0, 1, lo), (1, -1, hi)):
                j = (y - dy - x + 2 * Y_N) % Y_N
                wait(a_all.at[g, d, j], ag_sem.at[g, d, k])
                part = a_all.at[g, d, j, rows]
                send(part, part, as_sem.at[2 + g], fw_sem.at[g, d, k], at_y(dy))
        elif kind == "gw":
            g = event[1]
            for d in range(2):
                j = (j_own + 2) % Y_N
                wait(a_all.at[g, d, j, lo], fw_sem.at[g, d, 0])
                wait(a_all.at[g, d, j, hi], fw_sem.at[g, d, 1])

    def block(hop):
        return c * Z_N + (z - hop * step + 2 * Z_N) % Z_N

    def hand_over(m, kb):
        send(b_all.at[m, kb], b_all.at[m, kb], zs_sem.at[m], dr_sem.at[m], partner)

    def forward_long(m, hop):
        piece = b_all.at[m, block(hop)]
        send(piece, piece, zs_sem.at[m], zr_sem.at[m, hop], z_long)

    def forward_short(m, hop):
        piece = b_all.at[m, block(-hop)]
        send(piece, piece, zs_sem.at[m], zr_sem.at[m, 4 + hop], z_short)

    def b_own(m):
        b_local(m).wait()
        forward_long(m, 0)
        forward_short(m, 0)
        hand_over(m, block(0))

    def b_hop(m, hop):
        wait(b_all.at[m, block(hop)], zr_sem.at[m, hop - 1])
        forward_long(m, hop)
        hand_over(m, block(hop))
        wait(b_all.at[m, block(-hop)], zr_sem.at[m, 4 + hop - 1])
        if hop < 3:
            forward_short(m, hop)
        hand_over(m, block(-hop))

    def b_last(m):
        wait(b_all.at[m, block(4)], zr_sem.at[m, 3])
        hand_over(m, block(4))

    def in_range(m):
        return (m >= 0) & (m < CHUNKS)

    def b_slot(s):
        t, u = s // 4, s % 4
        pl.when((u == 0) & in_range(t + 1))(lambda: b_own(t + 1))
        pl.when((u == 1) & in_range(t - 1))(lambda: b_hop(t - 1, 2))
        pl.when((u == 1) & in_range(t - 2))(lambda: b_last(t - 2))
        pl.when((u == 2) & in_range(t))(lambda: b_hop(t, 1))
        pl.when((u == 3) & in_range(t - 1))(lambda: b_hop(t - 1, 3))

    def product(g, m):
        a = a_all[g].reshape(-1, a_all.shape[-1])
        b = b_all[m].reshape(-1, width)
        return jnp.dot(a, b, preferred_element_type=jnp.float32).reshape(crecv.shape[2:])

    def c_stage(g, m):
        if g == 0:
            eight = b_all.at[m, pl.ds(0, Z_N)]
            wait(eight, dr_sem.at[m])
            slot = m % C0_SLOTS

            @pl.when(m >= C0_SLOTS)
            def _():
                wait(c0.at[slot], c0_sem.at[slot])
            c0[slot] = product(0, m)
            src, ssem = c0.at[slot], c0_sem.at[slot]
        else:
            part = product(g, m)
            for d in range(2):
                wait(crecv.at[m, g - 1, d], cr_sem.at[m, g - 1, d])
            if g == 3:
                slot = m % OUT_SLOTS

                @pl.when(m >= OUT_SLOTS)
                def _():
                    out_copy(m - OUT_SLOTS).wait()
                outst[slot] = (crecv[m, g - 1] + part).reshape(outst.shape[1:]).astype(outst.dtype)
                out_copy(m).start()
                return
            crecv[m, g - 1] += part
            src, ssem = crecv.at[m, g - 1], cs_sem.at[m]
        send(src.at[0], crecv.at[m, g, 0], ssem, cr_sem.at[m, g, 0], at_x(1))
        send(src.at[1], crecv.at[m, g, 1], ssem, cr_sem.at[m, g, 1], at_x(-1))

    def out_copy(m):
        return pltpu.make_async_copy(outst.at[m % OUT_SLOTS],
                                     c_hbm.at[:, pl.ds(pl.multiple_of(m * width, width), width)],
                                     out_sem.at[m % OUT_SLOTS])

    def c_slot(s):
        for g in (3, 2, 1, 0):
            base, start = C_BASE[g], C_START[g]
            cross = max(start - base, 0)
            m_late = (s - base) // 4
            late = ((s - base) % 4 == 0) & (m_late >= cross) & (m_late < CHUNKS)
            m_early = (s - start) // 3
            early = ((s - start) % 3 == 0) & (m_early >= 0) & (m_early < min(cross, CHUNKS))
            m = jnp.where(early, m_early, m_late)
            pl.when(early | late)(functools.partial(c_stage, g, m))

    for slot, event in A_SCHEDULE:
        if slot < 0:
            a_event(event)
    b_own(0)
    last_a = max(slot for slot, _ in A_SCHEDULE)
    n_slots = max(max(C_BASE[g] + 4 * (CHUNKS - 1), C_START[g] + 3 * (CHUNKS - 1)) for g in range(4)) + 1

    def first_part(s, carry):
        b_slot(s)
        for slot in sorted({slot for slot, _ in A_SCHEDULE if slot >= 0}):
            @pl.when(s == slot)
            def _():
                for at, event in A_SCHEDULE:
                    if at == slot:
                        a_event(event)
        c_slot(s)
        return carry

    def second_part(s, carry):
        b_slot(s)
        c_slot(s)
        return carry

    lax.fori_loop(0, last_a + 1, first_part, 0)
    lax.fori_loop(last_a + 1, n_slots, second_part, 0)

    def drain(m, carry):
        wait(b_all.at[m, pl.ds(0, 15)], zs_sem.at[m])
        wait(crecv.at[m, pl.ds(0, 2)], cs_sem.at[m])
        return carry

    lax.fori_loop(0, CHUNKS, drain, 0)
    wait(a_all.at[0], as_sem.at[0])
    wait(a_all.at[0], as_sem.at[1])
    for g in range(4):
        wait(a_all.at[0, :, pl.ds(0, 3)], as_sem.at[2 + g])
    for slot in range(C0_SLOTS):
        wait(c0.at[slot], c0_sem.at[slot])
    for m in range(CHUNKS - OUT_SLOTS, CHUNKS):
        out_copy(m).wait()


def solution(mesh):
    def local_product(a_blk, b_blk):
        rows, cols = a_blk.shape
        width = cols // CHUNKS
        rows_q = rows // 8
        dma = pltpu.SemaphoreType.DMA
        return pl.pallas_call(
            kernel,
            name="matmul_3d",
            out_shape=jax.ShapeDtypeStruct((rows, cols), jnp.bfloat16),
            in_specs=[pl.BlockSpec(memory_space=pl.ANY)] * 2,
            out_specs=pl.BlockSpec(memory_space=pl.ANY),
            scratch_shapes=[
                pltpu.VMEM((4, 2, 4, rows_q, cols), jnp.bfloat16),
                pltpu.VMEM((3, 2, rows_q, cols), jnp.bfloat16),
                pltpu.VMEM((2, 2, rows_q // 2, cols), jnp.bfloat16),
                pltpu.VMEM((2, 2, rows_q // 2, cols), jnp.bfloat16),
                pltpu.VMEM((CHUNKS, 2 * Z_N, rows, width), jnp.bfloat16),
                pltpu.VMEM((CHUNKS, 3, 2, rows // 2, width), jnp.float32),
                pltpu.VMEM((C0_SLOTS, 2, rows // 2, width), jnp.float32),
                pltpu.VMEM((OUT_SLOTS, rows, width), jnp.bfloat16),
                dma((CHUNKS,)), dma((CHUNKS, 7)), dma((CHUNKS,)), dma((CHUNKS,)),
                dma((4, 2)), dma((2, 2)), dma((2, 2)), dma((3, 2)), dma((4, 2, 2)), dma((4, 2, 2)), dma((6,)),
                dma((CHUNKS, 3, 2)), dma((CHUNKS,)), dma((C0_SLOTS,)), dma((OUT_SLOTS,)),
            ],
            compiler_params=pltpu.CompilerParams(
                collective_id=0, has_side_effects=True, vmem_limit_bytes=67043328
            ),
        )(a_blk.reshape(2, 4, rows_q, cols), b_blk)

    block_spec = P(("row", "depth"), "col")
    return jax.shard_map(local_product, mesh=mesh, in_specs=(block_spec, block_spec), out_specs=block_spec, check_vma=False)
```

```python
import jax
import jax.numpy as jnp
from jax import lax
from jax.experimental import pallas as pl
from jax.experimental.pallas import tpu as pltpu
from jax.sharding import PartitionSpec as P

MESH = pl.DeviceIdType.MESH
X_N, Y_N, Z_N = 4, 4, 8
BLOCKS = 16
SLOTS = 4
LOOP = 8
S1, R1, S2, S2F, R2, AG, FW, OWN, LONG, SHORT, SUM = range(11)
WIDE = 14
SPLIT = 4
ALL = 2
ORDER = (
    (7, 0), (0, 0, 0), (7, 1), (0, 0, 1), (7, 2), (1, 0, 0, 1), (1, 0, 0, 0), (0, 1, 0), (7, 3), (1, 0, 1, 1),
    (9, 1, 1), (8, 1, 1), (2, 0, 0), (1, 0, 1, 0), (0, 1, 1), (8, 0, 1), (9, 3, 1), (8, 2, 1), (9, 2, 1), (2, 0, 1),
    (9, 1, 2), (1, 1, 0, 0), (1, 1, 0, 1), (9, 0, 1), (5, 0, 0, 1), (8, 0, 2), (5, 0, 0, 0), (1, 1, 1, 1),
    (1, 1, 1, 0), (8, 1, 2), (3, 1, 0), (2, 1, 0), (9, 3, 2), (8, 3, 1), (5, 0, 1, 1), (3, 0, 0), (8, 2, 2),
    (6, 0, 0, 1), (5, 0, 1, 0), (4, 1, 0, 0), (7, 4), (4, 1, 0, 1), (3, 1, 1), (8, 3, 2), (8, 2, 3), (9, 1, 3),
    (9, 2, 2), (5, 1, 0, 1), (8, 0, 3), (3, 0, 1), (6, 0, 1, 1), (4, 0, 0, 1), (9, 0, 2), (8, 1, 3), (8, 4, 1),
    (4, 1, 1, 1), (8, 3, 3), (4, 0, 0, 0), (6, 0, 0, 0), (4, 0, 1, 0), (4, 1, 1, 0), (2, 1, 1), (6, 0, 1, 0),
    (4, 0, 1, 1), (5, 1, 0, 0), (7, 5), (6, 1, 0, 1), (8, 0, 4), (8, 2, 4), (9, 3, 3), (9, 0, 3), (9, 2, 3),
    (10, 0, 0, 0), (8, 1, 4), (5, 1, 1, 1), (9, 4, 1), (10, 2, 0, 0), (8, 4, 2), (10, 2, 0, 1), (10, 1, 0, 0),
    (6, 1, 0, 0), (5, 1, 1, 0), (7, 6), (8, 3, 4), (10, 3, 0, 1), (5, 2, 0, 0), (10, 3, 0, 0), (9, 4, 2),
    (10, 0, 0, 1), (8, 5, 1), (8, 4, 3), (10, 2, 1, 0), (8, 6, 1), (5, 2, 0, 1), (10, 0, 1, 0), (9, 5, 1),
    (10, 1, 0, 1), (10, 1, 1, 0), (6, 1, 1, 1), (6, 1, 1, 0), (9, 6, 1), (8, 5, 2), (10, 3, 1, 0), (8, 4, 4),
    (5, 2, 1, 0), (6, 2, 0, 0), (7, 7), (9, 4, 3), (10, 4, 0, 2), (9, 5, 2), (8, 6, 2), (10, 3, 1, 1), (5, 2, 1, 1),
    (10, 1, 1, 1), (8, 5, 3), (9, 6, 2), (10, 2, 1, 1), (7, 8), (6, 2, 0, 1), (6, 2, 1, 0), (10, 0, 1, 1),
    (10, 4, 1, 2), (9, 5, 3), (8, 7, 1), (8, 6, 3), (6, 2, 1, 1), (5, 3, 1, 0), (8, 5, 4), (10, 2, 2, 0),
    (10, 5, 0, 2), (7, 9), (10, 3, 2, 1), (10, 4, 2, 2), (9, 6, 3), (9, 7, 1), (8, 8, 1), (5, 3, 0, 0), (8, 7, 2),
    (5, 3, 1, 1), (10, 2, 2, 1), (8, 6, 4), (8, 9, 1), (10, 6, 0, 2), (7, 10), (10, 0, 2, 1), (8, 8, 2),
    (10, 5, 1, 2), (6, 3, 0, 0), (10, 1, 2, 1), (8, 7, 3), (5, 3, 0, 1), (9, 8, 1), (8, 9, 2), (10, 6, 1, 2),
    (9, 7, 2), (6, 3, 1, 1), (6, 3, 0, 1), (8, 8, 3), (7, 11), (10, 1, 2, 0), (10, 5, 2, 2), (6, 3, 1, 0), (9, 9, 1),
    (10, 0, 2, 0), (8, 7, 4), (8, 9, 3), (10, 3, 2, 0), (9, 7, 3), (9, 8, 2), (9, 10, 1), (10, 7, 0, 2), (8, 10, 1),
    (9, 9, 2), (10, 6, 2, 2), (8, 8, 4), (8, 11, 1), (9, 8, 3), (10, 8, 0, 2), (9, 11, 1), (10, 7, 1, 2), (8, 10, 2),
    (10, 0, 3, 0), (9, 10, 2), (8, 9, 4), (7, 12), (9, 9, 3), (10, 9, 0, 2), (10, 0, 3, 1), (8, 11, 2), (10, 8, 1, 2),
    (8, 10, 3), (8, 12, 1), (10, 7, 2, 2), (9, 12, 1), (8, 11, 3), (9, 10, 3), (9, 11, 2), (10, 9, 1, 2), (8, 10, 4),
    (7, 13), (10, 1, 3, 0), (10, 8, 2, 2), (8, 12, 2), (9, 12, 2), (7, 14), (10, 10, 0, 2), (10, 1, 3, 1),
    (10, 9, 2, 2), (8, 11, 4), (9, 11, 3), (8, 12, 3), (10, 11, 0, 2), (8, 13, 1), (10, 2, 3, 0), (10, 2, 3, 1),
    (9, 12, 3), (7, 15), (9, 14, 1), (10, 10, 1, 2), (9, 13, 1), (8, 12, 4), (7, 16), (10, 12, 0, 2), (10, 3, 3, 0),
    (8, 13, 2), (10, 11, 1, 2), (8, 16, 1), (8, 14, 1), (7, 17), (10, 3, 3, 1), (9, 13, 2), (8, 15, 1),
    (10, 10, 2, 2), (10, 4, 3, 2), (10, 12, 1, 2), (8, 13, 3), (8, 14, 2), (10, 11, 2, 2), (8, 16, 2), (9, 15, 1),
    (9, 14, 2), (9, 13, 3), (8, 13, 4), (8, 17, 1), (8, 15, 2), (9, 16, 1), (8, 14, 3), (10, 13, 0, 2),
    (10, 12, 2, 2), (8, 16, 3), (8, 17, 2), (8, 15, 3), (9, 15, 2), (9, 17, 1), (9, 16, 2), (9, 14, 3), (8, 14, 4),
    (10, 14, 0, 2), (8, 17, 3), (10, 13, 1, 2), (10, 5, 3, 2), (8, 15, 4), (9, 15, 3), (8, 16, 4), (9, 17, 2),
    (9, 16, 3), (10, 15, 0, 2), (10, 16, 0, 2), (10, 14, 1, 2), (9, 17, 3), (8, 17, 4), (10, 17, 0, 2),
    (10, 15, 1, 2), (10, 6, 3, 2), (10, 16, 1, 2), (10, 13, 2, 2), (10, 17, 1, 2), (10, 7, 3, 2), (10, 14, 2, 2),
    (10, 8, 3, 2), (10, 9, 3, 2), (10, 15, 2, 2), (10, 10, 3, 2), (10, 16, 2, 2), (10, 17, 2, 2), (10, 11, 3, 2),
    (10, 12, 3, 2), (10, 13, 3, 2), (10, 14, 3, 2), (10, 15, 3, 2), (10, 16, 3, 2), (10, 17, 3, 2),
)


def chunk(n):
    return (n, None) if n < WIDE else (WIDE + (n - WIDE) // 2, (n - WIDE) % 2)


CHUNKS = WIDE + 2 * (BLOCKS - WIDE)


def kernel(a_hbm, b_hbm, c_hbm, a_own, a_all, s1, rl1, rl2, b_all, crecv, c0, outst, prod,
           ld_sem, zr_sem, zs_sem, dr_sem, s1_sem, r1_sem, r2_sem, s2_sem, ag_sem, fw_sem, as_sem,
           cr_sem, cs_sem, c0_sem, out_sem):
    row, y, z = lax.axis_index("row"), lax.axis_index("col"), lax.axis_index("depth")
    x, c = row // 2, row % 2
    width = b_all.shape[3]
    narrow = width // 2
    cols = a_own.shape[4]
    part_cols = (pl.ds(0, cols // 2), pl.ds(cols // 2, cols // 2))
    rest = slice(None)

    def at_x(dx):
        return {"row": 2 * ((x + dx + X_N) % X_N) + c}

    def at_y(dy):
        return {"col": (y + dy + Y_N) % Y_N}

    step = 1 - 2 * c
    z_long = {"depth": (z + step + Z_N) % Z_N}
    z_short = {"depth": (z - step + Z_N) % Z_N}
    partner = {"row": 2 * x + 1 - c}

    def send(src, dst, ssem, rsem, dev):
        pltpu.make_async_remote_copy(src_ref=src, dst_ref=dst, send_sem=ssem, recv_sem=rsem,
                                     device_id=dev, device_id_type=MESH).start()

    def wait(ref, sem):
        pltpu.make_async_copy(ref, ref, sem).wait()

    e_own = (y - x + Y_N) % Y_N
    flip = e_own // 3
    j_own = e_own

    def b_local(m, sem):
        return pltpu.make_async_copy(b_hbm.at[:, pl.ds(pl.multiple_of(m * width, width), width)],
                                     b_all.at[m, c * Z_N + z], ld_sem.at[sem])

    a_load = pltpu.make_async_copy(a_hbm, a_own, ld_sem.at[2])
    a_load.start()
    b_local(0, 0).start()
    barrier = pltpu.get_barrier_semaphore()
    for dev in (at_x(1), at_x(-1), at_y(1), at_y(-1), z_long, z_short, partner):
        pl.semaphore_signal(barrier, inc=1, device_id=dev, device_id_type=MESH)
    lax.fori_loop(1, BLOCKS, lambda m, _: (b_local(m, 1).start(), 0)[1], 0)

    def by_e(e, o, r, j, part, fn):
        col_part = rest if part is None else part_cols[part]

        @pl.when(e == 0)
        def _():
            fn(a_all.at[3, o, j, r, :, col_part])

        @pl.when(e != 0)
        def _():
            fn(s1.at[(e + Y_N - 1) % Y_N, o, r, :, col_part])

    for o in range(2):
        for r in range(2):
            by_e(e_own, o, r, 0, None, lambda dst: pltpu.make_async_copy(
                a_hbm.at[(o + flip) % 2, 0, r], dst, s1_sem.at[e_own, o, r]).start())
    pl.semaphore_wait(barrier, 7)
    a_load.wait()

    def ev_s1(o, r):
        h = (o + flip) % 2
        send(a_own.at[h, 2, r, :, part_cols[0]], rl1.at[0, o, r], as_sem, r1_sem.at[0, o, r], at_y(1))
        send(a_own.at[h, 2, r, :, part_cols[1]], rl1.at[1, o, r], as_sem, r1_sem.at[1, o, r], at_y(-1))
        sem = s1_sem.at[e_own, o, r]
        by_e(e_own, o, r, 1, None, lambda dst: send(a_own.at[h, 1, r], dst, as_sem, sem, at_y(1)))
        by_e(e_own, o, r, 3, None, lambda dst: send(a_own.at[h, 3, r], dst, as_sem, sem, at_y(-1)))

    def ev_r1(o, r, d):
        dy = 1 - 2 * d
        e = (y - dy - x + 2 * Y_N) % Y_N
        wait(rl1.at[d, o, r], r1_sem.at[d, o, r])
        by_e(e, o, r, 2, d, lambda dst: send(rl1.at[d, o, r], dst, as_sem, s1_sem.at[e, o, r], at_y(dy)))

    def ev_s2(o, r):
        wait(s1.at[0, o, r], s1_sem.at[1, o, r])
        wait(s1.at[2, o, r], s1_sem.at[3, o, r])
        g = 2 * o
        j = (y - x - 1 + 2 * Y_N) % Y_N
        send(s1.at[0, o, r], a_all.at[g, o, j, r], as_sem, s2_sem.at[g, o, r], at_x(1))
        j = (y - x + 1 + Y_N) % Y_N
        send(s1.at[2, o, r], a_all.at[g, 1 - o, j, r], as_sem, s2_sem.at[g, 1 - o, r], at_x(-1))

    def ev_s2f(o, r):
        wait(s1.at[1, o, r], s1_sem.at[2, o, r])
        for d in range(2):
            send(s1.at[1, o, r, :, part_cols[d]], rl2.at[d, o, r], as_sem, r2_sem.at[d, o, r], at_x(1 - 2 * d))

    def ev_r2(o, r, d):
        dx = 1 - 2 * d
        j = (y - x - dx + 2 * Y_N) % Y_N
        wait(rl2.at[d, o, r], r2_sem.at[d, o, r])
        send(rl2.at[d, o, r], a_all.at[1, o, j, r, :, part_cols[d]], as_sem, s2_sem.at[1, o, r], at_x(dx))

    def ev_ag(g, r, d):
        quarter = a_all.at[g, d, j_own, r]
        wait(quarter, s1_sem.at[0, d, r] if g == 3 else s2_sem.at[g, d, r])
        send(quarter, quarter, as_sem, ag_sem.at[g, d, r], at_y(1))
        send(quarter, quarter, as_sem, ag_sem.at[g, d, r], at_y(-1))

    def ev_fw(g, r, d):
        wait(a_all.at[0, 0, 0], ag_sem.at[g, d, r])
        for k, dy in ((0, 1), (1, -1)):
            j = (y - dy - x + 2 * Y_N) % Y_N
            part = a_all.at[g, d, j, r, :, part_cols[k]]
            send(part, part, as_sem, fw_sem.at[g, r], at_y(dy))

    def group_complete(g, r):
        wait(a_all.at[0, 0, 0], fw_sem.at[g, r])

    def block(hop):
        return c * Z_N + (z - hop * step + 2 * Z_N) % Z_N

    def lanes_of(n):
        half = chunk(n)[1]
        return rest if half is None else pl.ds(half * narrow, narrow)

    def piece(n, kb):
        return b_all.at[chunk(n)[0], kb, :, lanes_of(n)]

    def hand_over(n, kb):
        send(piece(n, kb), piece(n, kb), zs_sem.at[chunk(n)[0] // 4], dr_sem.at[n], partner)

    def forward_long(n, hop):
        p = piece(n, block(hop))
        send(p, p, zs_sem.at[chunk(n)[0] // 4], zr_sem.at[n, hop], z_long)

    def forward_short(n, hop):
        p = piece(n, block(-hop))
        send(p, p, zs_sem.at[chunk(n)[0] // 4], zr_sem.at[n, 4 + hop], z_short)

    def ev_own(n):
        if n == 0:
            b_local(0, 0).wait()
        elif n == 1:
            wait(b_all.at[0, pl.ds(0, BLOCKS - 1)], ld_sem.at[1])
        forward_long(n, 0)
        forward_short(n, 0)
        hand_over(n, block(0))

    def ev_long(n, hop):
        wait(piece(n, block(hop)), zr_sem.at[n, hop - 1])
        if hop < 4:
            forward_long(n, hop)
        hand_over(n, block(hop))

    def ev_short(n, hop):
        wait(piece(n, block(-hop)), zr_sem.at[n, 4 + hop - 1])
        if hop < 3:
            forward_short(n, hop)
        hand_over(n, block(-hop))

    def handed_over(n):
        wait(b_all.at[0, pl.ds(0, Z_N), :, lanes_of(n)], dr_sem.at[n])

    def dot(a, b):
        return jnp.dot(a.reshape(-1, cols), b.reshape(cols, -1), preferred_element_type=jnp.float32)

    def out_copy(src, q, first, size, slot):
        return pltpu.make_async_copy(src, c_hbm.at[:, :, q, :, pl.ds(pl.multiple_of(first, size), size)],
                                     out_sem.at[slot])

    def sum_stage(n, g, q, m, lanes, first, size, when, reuse, old):
        slot = n % SLOTS
        keep = rest if isinstance(lanes, slice) else pl.ds(0, narrow)
        qi = 0 if isinstance(q, slice) else q

        def pass_on(src, ssem):
            for d in range(2):
                send(src.at[d], crecv.at[m, g, d, :, q, :, lanes], ssem, cr_sem.at[n, g, qi], at_x(1 - 2 * d))

        def arrived():
            wait(crecv.at[m, g - 1, :, :, q, :, lanes], cr_sem.at[n, g - 1, qi])

        def begin():
            reuse(lambda: wait(c0.at[slot, :, :, :, :, old], c0_sem.at[slot]))
            c0[slot, :, :, q, :, keep] = prod[:, :, q, :, keep]
            pass_on(c0.at[slot, :, :, q, :, keep], c0_sem.at[slot])

        def middle():
            arrived()
            crecv[m, g - 1, :, :, q, :, lanes] += prod[:, :, q, :, keep]
            pass_on(crecv.at[m, g - 1, :, :, q, :, lanes], cs_sem.at[m // 4])

        def end():
            arrived()
            reuse(lambda: wait(outst.at[slot, :, :, :, :, old], out_sem.at[slot]))
            total = crecv[m, g - 1, :, :, q, :, lanes] + prod[:, :, q, :, keep]
            outst[slot, :, :, q, :, keep] = total.astype(outst.dtype)
            out_copy(outst.at[slot, :, :, q, :, keep], q, first, size, slot).start()

        a = a_all[g, :, :, q]
        prod[:, :, q, :, keep] = dot(a, b_all[m, :, :, lanes]).reshape(a.shape[:-1] + (size,))
        when(g == 0, begin)
        when((g == 1) | (g == 2), middle)
        when(g == 3, end)

    def branch(cond, fn):
        pl.when(cond)(fn)

    def fixed(cond, fn):
        if cond:
            fn()

    def sum_loop(code, split, wide):
        n, g, q = code // 8, code // 2 % 4, code % 2
        if split:
            pl.when(n < SPLIT)(lambda: sum_stage(n, g, q, n, rest, n * width, width, branch, lambda fn: None, rest))
        if wide:
            pl.when(n >= SPLIT)(lambda: sum_stage(n, g, rest, n, rest, n * width, width, branch,
                                                  pl.when(n >= SLOTS), rest))

    def sum_narrow(n, g):
        m, half = chunk(n)
        old = rest if n - SLOTS < WIDE else pl.ds(0, narrow)
        sum_stage(n, g, rest, m, lanes_of(n), m * width + half * narrow, narrow, fixed, lambda fn: fn(), old)

    events = {S1: ev_s1, R1: ev_r1, S2: ev_s2, S2F: ev_s2f, R2: ev_r2, AG: ev_ag, FW: ev_fw,
              OWN: ev_own, LONG: ev_long, SHORT: ev_short}
    steps, before, complete, handed = [], [], set(), set()
    for kind, *args in ORDER:
        if kind != SUM:
            before.append((events[kind], args))
            continue
        n, g, q = args
        for r in (range(2) if q == ALL else (q,)):
            if (g, r) not in complete:
                complete.add((g, r))
                before.append((group_complete, (g, r)))
        if n not in handed:
            handed.add(n)
            before.append((handed_over, (n,)))
        if n >= WIDE:
            before.append((sum_narrow, (n, g)))
        else:
            steps.append((before, (n * 4 + g) * 2 + q % 2, q != ALL))
            before = []

    def run(todo):
        for fn, args in todo:
            fn(*args)

    def in_loop(first, last):
        part = steps[first:last]

        def body(k, carry):
            code = part[0][1]
            for i, (todo, this, _) in enumerate(part):
                code = jnp.where(k == first + i, this, code)
                if todo:
                    pl.when(k == first + i)(lambda: run(todo))
            sum_loop(code, any(s for _, _, s in part), any(not s for _, _, s in part))
            return carry

        lax.fori_loop(first, last, body, 0)

    for first in range(0, len(steps), LOOP):
        in_loop(first, min(first + LOOP, len(steps)))
    run(before)

    for i in range(BLOCKS // 4):
        wait(b_all.at[pl.ds(0, 4), pl.ds(0, 15)], zs_sem.at[i])
        wait(crecv.at[pl.ds(0, 4), pl.ds(0, 2)], cs_sem.at[i])
    wait(b_all.at[pl.ds(0, 5)], as_sem)
    for n in range(CHUNKS - SLOTS, CHUNKS):
        keep = rest if n < WIDE else pl.ds(0, narrow)
        wait(c0.at[n % SLOTS, :, :, :, :, keep], c0_sem.at[n % SLOTS])
        wait(outst.at[n % SLOTS, :, :, :, :, keep], out_sem.at[n % SLOTS])


def solution(mesh):
    def local_product(a_blk, b_blk):
        rows, cols = a_blk.shape
        width = cols // BLOCKS
        few = rows // 16
        dma = pltpu.SemaphoreType.DMA
        c_blk = pl.pallas_call(
            kernel,
            name="matmul_3d",
            out_shape=jax.ShapeDtypeStruct((2, 4, 2, few, cols), jnp.bfloat16),
            in_specs=[pl.BlockSpec(memory_space=pl.ANY)] * 2,
            out_specs=pl.BlockSpec(memory_space=pl.ANY),
            scratch_shapes=[
                pltpu.VMEM((2, 4, 2, few, cols), jnp.bfloat16),
                pltpu.VMEM((4, 2, 4, 2, few, cols), jnp.bfloat16),
                pltpu.VMEM((3, 2, 2, few, cols), jnp.bfloat16),
                pltpu.VMEM((2, 2, 2, few, cols // 2), jnp.bfloat16),
                pltpu.VMEM((2, 2, 2, few, cols // 2), jnp.bfloat16),
                pltpu.VMEM((BLOCKS, 2 * Z_N, rows, width), jnp.bfloat16),
                pltpu.VMEM((BLOCKS, 3, 2, 4, 2, few, width), jnp.float32),
                pltpu.VMEM((SLOTS, 2, 4, 2, few, width), jnp.float32),
                pltpu.VMEM((SLOTS, 2, 4, 2, few, width), jnp.bfloat16),
                pltpu.VMEM((2, 4, 2, few, width), jnp.float32),
                dma((3,)), dma((CHUNKS, 7)), dma((BLOCKS // 4,)), dma((CHUNKS,)),
                dma((4, 2, 2)), dma((2, 2, 2)), dma((2, 2, 2)), dma((3, 2, 2)), dma((4, 2, 2)), dma((4, 2)), dma,
                dma((CHUNKS, 3, 2 if SPLIT else 1)), dma((BLOCKS // 4,)), dma((SLOTS,)), dma((SLOTS,)),
            ],
            compiler_params=pltpu.CompilerParams(
                collective_id=0, has_side_effects=True, vmem_limit_bytes=67043328
            ),
        )(a_blk.reshape(2, 4, 2, few, cols), b_blk)
        return c_blk.reshape(rows, cols)

    block_spec = P(("row", "depth"), "col")
    return jax.shard_map(local_product, mesh=mesh, in_specs=(block_spec, block_spec), out_specs=block_spec, check_vma=False)
```

```python
import jax
import jax.numpy as jnp
from jax import lax
from jax.experimental import pallas as pl
from jax.experimental.pallas import tpu as pltpu
from jax.sharding import PartitionSpec as P

MESH = pl.DeviceIdType.MESH
X_N, Y_N, Z_N = 4, 4, 8
BLOCKS = 16
SLOTS = 4
LOOP = 8
WIDE = 14
SPLIT = 4
ALL = 2
Z_SEMS, C_SEMS = 5, 7

PROGRAM = (
    "iaaiajfijbfbakjgibcflncmkkllbfjacdndomgcgmhlonodbamheheofkgn",
    "odppcetatpotebohpgtdobfnqqnfachuqeqopcguauuodagbqoonrrrndrhv",
    "ebpfvvcoeobhcpgqdarcfhsoqedfagbpfrodergavhpbqehcgfspqcbhrdgw",
    "dqrfceawsshpwaerdgbpqfaebfahsacpgbqfsbrdqwccrfbghsecfsdpdrgh",
    "gcdeepqdghheppsqehspqrssqqrsrrrsssss",
)


def chunk(n):
    return (n, None) if n < WIDE else (WIDE + (n - WIDE) // 2, (n - WIDE) % 2)


CHUNKS = WIDE + 2 * (BLOCKS - WIDE)


def kernel(a_hbm, b_hbm, c_out, a_own, a_all, s1, rl1, rl2, b_all, crecv, c0, prod,
           ld_sem, zr_sem, zs_sem, dr_sem, s1_sem, r1_sem, r2_sem, s2_sem, ag_sem, fw_sem, as_sem,
           cr_sem, cs_sem, c0_sem):
    row, y, z = lax.axis_index("row"), lax.axis_index("col"), lax.axis_index("depth")
    x, c = row // 2, row % 2
    width = b_all.shape[3]
    narrow = width // 2
    cols = a_own.shape[4]
    part_cols = (pl.ds(0, cols // 2), pl.ds(cols // 2, cols // 2))
    rest = slice(None)

    def at_x(dx):
        return {"row": 2 * ((x + dx + X_N) % X_N) + c}

    def at_y(dy):
        return {"col": (y + dy + Y_N) % Y_N}

    step = 1 - 2 * c
    z_long = {"depth": (z + step + Z_N) % Z_N}
    z_short = {"depth": (z - step + Z_N) % Z_N}
    partner = {"row": 2 * x + 1 - c}

    def send(src, dst, ssem, rsem, dev):
        pltpu.make_async_remote_copy(src_ref=src, dst_ref=dst, send_sem=ssem, recv_sem=rsem,
                                     device_id=dev, device_id_type=MESH).start()

    def wait(ref, sem):
        pltpu.make_async_copy(ref, ref, sem).wait()

    e_own = (y - x + Y_N) % Y_N
    flip = e_own // 3
    j_own = e_own

    def b_local(m, sem):
        return pltpu.make_async_copy(b_hbm.at[:, pl.ds(pl.multiple_of(m * width, width), width)],
                                     b_all.at[m, c * Z_N + z], ld_sem.at[sem])

    a_load = pltpu.make_async_copy(a_hbm, a_own, ld_sem.at[2])
    a_load.start()
    b_local(0, 0).start()
    barrier = pltpu.get_barrier_semaphore()
    for dev in (at_x(1), at_x(-1), at_y(1), at_y(-1), z_long, z_short, partner):
        pl.semaphore_signal(barrier, inc=1, device_id=dev, device_id_type=MESH)
    lax.fori_loop(1, BLOCKS, lambda m, _: (b_local(m, 1).start(), 0)[1], 0)

    def by_e(e, o, r, j, part, fn):
        col_part = rest if part is None else part_cols[part]

        @pl.when(e == 0)
        def _():
            fn(a_all.at[3, o, j, r, :, col_part])

        @pl.when(e != 0)
        def _():
            fn(s1.at[(e + Y_N - 1) % Y_N, o, r, :, col_part])

    for o in range(2):
        for r in range(2):
            by_e(e_own, o, r, 0, None, lambda dst: pltpu.make_async_copy(
                a_hbm.at[(o + flip) % 2, 0, r], dst, s1_sem.at[e_own, o, r]).start())
    pl.semaphore_wait(barrier, 7)
    a_load.wait()

    def ev_s1(o, r):
        h = (o + flip) % 2
        send(a_own.at[h, 2, r, :, part_cols[0]], rl1.at[0, o, r], as_sem, r1_sem.at[0, o, r], at_y(1))
        send(a_own.at[h, 2, r, :, part_cols[1]], rl1.at[1, o, r], as_sem, r1_sem.at[1, o, r], at_y(-1))
        sem = s1_sem.at[e_own, o, r]
        by_e(e_own, o, r, 1, None, lambda dst: send(a_own.at[h, 1, r], dst, as_sem, sem, at_y(1)))
        by_e(e_own, o, r, 3, None, lambda dst: send(a_own.at[h, 3, r], dst, as_sem, sem, at_y(-1)))

    def ev_r1(o, r, d):
        dy = 1 - 2 * d
        e = (y - dy - x + 2 * Y_N) % Y_N
        wait(rl1.at[d, o, r], r1_sem.at[d, o, r])
        by_e(e, o, r, 2, d, lambda dst: send(rl1.at[d, o, r], dst, as_sem, s1_sem.at[e, o, r], at_y(dy)))

    def ev_s2(o, r):
        wait(s1.at[0, o, r], s1_sem.at[1, o, r])
        wait(s1.at[2, o, r], s1_sem.at[3, o, r])
        g = 2 * o
        j = (y - x - 1 + 2 * Y_N) % Y_N
        send(s1.at[0, o, r], a_all.at[g, o, j, r], as_sem, s2_sem.at[g, o, r], at_x(1))
        j = (y - x + 1 + Y_N) % Y_N
        send(s1.at[2, o, r], a_all.at[g, 1 - o, j, r], as_sem, s2_sem.at[g, 1 - o, r], at_x(-1))

    def ev_s2f(o, r):
        wait(s1.at[1, o, r], s1_sem.at[2, o, r])
        for d in range(2):
            send(s1.at[1, o, r, :, part_cols[d]], rl2.at[d, o, r], as_sem, r2_sem.at[d, o, r], at_x(1 - 2 * d))

    def ev_r2(o, r, d):
        dx = 1 - 2 * d
        j = (y - x - dx + 2 * Y_N) % Y_N
        wait(rl2.at[d, o, r], r2_sem.at[d, o, r])
        send(rl2.at[d, o, r], a_all.at[1, o, j, r, :, part_cols[d]], as_sem, s2_sem.at[1, o, r], at_x(dx))

    def ev_ag(g, r, d):
        quarter = a_all.at[g, d, j_own, r]
        wait(quarter, s1_sem.at[0, d, r] if g == 3 else s2_sem.at[g, d, r])
        send(quarter, quarter, as_sem, ag_sem.at[g, d, r], at_y(1))
        send(quarter, quarter, as_sem, ag_sem.at[g, d, r], at_y(-1))

    def ev_fw(g, r, d):
        wait(a_all.at[0, 0, 0], ag_sem.at[g, d, r])
        for k, dy in ((0, 1), (1, -1)):
            j = (y - dy - x + 2 * Y_N) % Y_N
            part = a_all.at[g, d, j, r, :, part_cols[k]]
            send(part, part, as_sem, fw_sem.at[g, r], at_y(dy))

    def group_complete(g, r):
        wait(a_all.at[0, 0, 0], fw_sem.at[g, r])

    def block(hop):
        return c * Z_N + (z - hop * step + 2 * Z_N) % Z_N

    def lanes_of(n):
        half = chunk(n)[1]
        return rest if half is None else pl.ds(half * narrow, narrow)

    def piece(n, kb):
        return b_all.at[chunk(n)[0], kb, :, lanes_of(n)]

    def hand_over(n, kb):
        send(piece(n, kb), piece(n, kb), zs_sem.at[chunk(n)[0] // 4], dr_sem.at[n], partner)

    def forward_long(n, hop):
        p = piece(n, block(hop))
        send(p, p, zs_sem.at[chunk(n)[0] // 4], zr_sem.at[n % Z_SEMS, hop], z_long)

    def forward_short(n, hop):
        p = piece(n, block(-hop))
        send(p, p, zs_sem.at[chunk(n)[0] // 4], zr_sem.at[n % Z_SEMS, 4 + hop], z_short)

    def ev_own(n):
        if n == 0:
            b_local(0, 0).wait()
        elif n == 1:
            wait(b_all.at[0, pl.ds(0, BLOCKS - 1)], ld_sem.at[1])
        forward_long(n, 0)
        forward_short(n, 0)
        hand_over(n, block(0))

    def ev_long(n, hop):
        wait(piece(n, block(hop)), zr_sem.at[n % Z_SEMS, hop - 1])
        if hop < 4:
            forward_long(n, hop)
        hand_over(n, block(hop))

    def ev_short(n, hop):
        wait(piece(n, block(-hop)), zr_sem.at[n % Z_SEMS, 4 + hop - 1])
        if hop < 3:
            forward_short(n, hop)
        hand_over(n, block(-hop))

    def handed_over(n):
        wait(b_all.at[0, pl.ds(0, Z_N), :, lanes_of(n)], dr_sem.at[n])

    def dot(a, b):
        return jnp.dot(a.reshape(-1, cols), b.reshape(cols, -1), preferred_element_type=jnp.float32)

    def sum_sem(n, q):
        return 2 * SPLIT + (n - SPLIT) % C_SEMS if isinstance(q, slice) else 2 * n + q

    def sum_stage(n, g, q, m, lanes, first, size, when, reuse, old):
        slot = n % SLOTS
        keep = rest if isinstance(lanes, slice) else pl.ds(0, narrow)
        arrivals = sum_sem(n, q)

        def pass_on(src, ssem):
            for d in range(2):
                send(src.at[d], crecv.at[m, g, d, :, q, :, lanes], ssem, cr_sem.at[arrivals, g], at_x(1 - 2 * d))

        def arrived():
            wait(crecv.at[m, g - 1, :, :, q, :, lanes], cr_sem.at[arrivals, g - 1])

        def begin():
            reuse(lambda: wait(c0.at[slot, :, :, :, :, old], c0_sem.at[slot]))
            c0[slot, :, :, q, :, keep] = prod[:, :, q, :, keep]
            pass_on(c0.at[slot, :, :, q, :, keep], c0_sem.at[slot])

        def middle():
            arrived()
            crecv[m, g - 1, :, :, q, :, lanes] += prod[:, :, q, :, keep]
            pass_on(crecv.at[m, g - 1, :, :, q, :, lanes], cs_sem.at[m // 4])

        def end():
            arrived()
            total = crecv[m, g - 1, :, :, q, :, lanes] + prod[:, :, q, :, keep]
            c_out[:, :, q, :, pl.ds(pl.multiple_of(first, size), size)] = total.astype(c_out.dtype)

        a = a_all[g, :, :, q]
        prod[:, :, q, :, keep] = dot(a, b_all[m, :, :, lanes]).reshape(a.shape[:-1] + (size,))
        when(g == 0, begin)
        when((g == 1) | (g == 2), middle)
        when(g == 3, end)

    def branch(cond, fn):
        pl.when(cond)(fn)

    def fixed(cond, fn):
        if cond:
            fn()

    def sum_loop(code, split, wide):
        n, g, q = code // 8, code // 2 % 4, code % 2
        if split:
            pl.when(n < SPLIT)(lambda: sum_stage(n, g, q, n, rest, n * width, width, branch, lambda fn: None, rest))
        if wide:
            pl.when(n >= SPLIT)(lambda: sum_stage(n, g, rest, n, rest, n * width, width, branch,
                                                  pl.when(n >= SLOTS), rest))

    def sum_narrow(n, g):
        m, half = chunk(n)
        old = rest if n - SLOTS < WIDE else pl.ds(0, narrow)
        sum_stage(n, g, rest, m, lanes_of(n), m * width + half * narrow, narrow, fixed, lambda fn: fn(), old)

    def both(fn):
        def two(*args):
            fn(*args, 0)
            fn(*args, 1)
        return two

    chunks = range(CHUNKS)
    queues = {"a": [(ev_own, (n,)) for n in chunks]}
    for hop in range(1, 5):
        queues["abcde"[hop]] = [(ev_long, (n, hop)) for n in chunks]
    for hop in range(1, 4):
        queues["efgh"[hop]] = [(ev_short, (n, hop)) for n in chunks]
    by_half = [(o, r) for o in range(2) for r in range(2)]
    by_row = [(o, r) for r in range(2) for o in range(2)]
    queues["i"] = [(ev_s1, p) for p in by_half]
    queues["j"] = [(both(ev_r1), p) for p in by_half]
    queues["k"] = [(ev_s2, p) for p in by_half]
    queues["l"] = [(ev_s2f, p) for p in by_row]
    queues["m"] = [(both(ev_r2), p) for p in by_row]
    groups = [(g, r) for g in range(4) for r in range(2)]
    queues["n"] = [(both(ev_ag), p) for p in groups]
    queues["o"] = [(ev_fw, p + (d,)) for p in groups for d in range(2)]
    for g in range(4):
        queues["pqrs"[g]] = [(None, (n, g, 0 if n < SPLIT else ALL)) for n in chunks]
        queues["tuvw"[g]] = [(None, (n, g, 1)) for n in range(SPLIT)]

    steps, before, complete, handed = [], [], set(), set()
    for letter in "".join(PROGRAM):
        fn, args = queues[letter].pop(0)
        if fn is not None:
            before.append((fn, args))
            continue
        n, g, q = args
        for r in (range(2) if q == ALL else (q,)):
            if (g, r) not in complete:
                complete.add((g, r))
                before.append((group_complete, (g, r)))
        if n not in handed:
            handed.add(n)
            before.append((handed_over, (n,)))
        if n >= WIDE:
            before.append((sum_narrow, (n, g)))
        else:
            steps.append((before, (n * 4 + g) * 2 + q % 2, q != ALL))
            before = []

    def run(todo):
        for fn, args in todo:
            fn(*args)

    def in_loop(first, last):
        part = steps[first:last]

        def body(k, carry):
            code = part[0][1]
            for i, (todo, this, _) in enumerate(part):
                code = jnp.where(k == first + i, this, code)
                if todo:
                    pl.when(k == first + i)(lambda: run(todo))
            sum_loop(code, any(s for _, _, s in part), any(not s for _, _, s in part))
            return carry

        lax.fori_loop(first, last, body, 0)

    for first in range(0, len(steps), LOOP):
        in_loop(first, min(first + LOOP, len(steps)))
    run(before)

    for i in range(BLOCKS // 4):
        wait(b_all.at[pl.ds(0, 4), pl.ds(0, 15)], zs_sem.at[i])
        wait(crecv.at[pl.ds(0, 4), pl.ds(0, 2)], cs_sem.at[i])
    wait(b_all.at[pl.ds(0, 5)], as_sem)
    for n in range(CHUNKS - SLOTS, CHUNKS):
        keep = rest if n < WIDE else pl.ds(0, narrow)
        wait(c0.at[n % SLOTS, :, :, :, :, keep], c0_sem.at[n % SLOTS])


def solution(mesh):
    def local_product(a_blk, b_blk):
        rows, cols = a_blk.shape
        width = cols // BLOCKS
        few = rows // 16
        dma = pltpu.SemaphoreType.DMA
        c_blk = pl.pallas_call(
            kernel,
            name="matmul_3d",
            out_shape=pltpu.VMEM((2, 4, 2, few, cols), jnp.bfloat16),
            in_specs=[pl.BlockSpec(memory_space=pl.ANY)] * 2,
            out_specs=pl.BlockSpec(memory_space=pltpu.VMEM),
            scratch_shapes=[
                pltpu.VMEM((2, 4, 2, few, cols), jnp.bfloat16),
                pltpu.VMEM((4, 2, 4, 2, few, cols), jnp.bfloat16),
                pltpu.VMEM((3, 2, 2, few, cols), jnp.bfloat16),
                pltpu.VMEM((2, 2, 2, few, cols // 2), jnp.bfloat16),
                pltpu.VMEM((2, 2, 2, few, cols // 2), jnp.bfloat16),
                pltpu.VMEM((BLOCKS, 2 * Z_N, rows, width), jnp.bfloat16),
                pltpu.VMEM((BLOCKS, 3, 2, 4, 2, few, width), jnp.float32),
                pltpu.VMEM((SLOTS, 2, 4, 2, few, width), jnp.float32),
                pltpu.VMEM((2, 4, 2, few, width), jnp.float32),
                dma((3,)), dma((Z_SEMS, 7)), dma((BLOCKS // 4,)), dma((CHUNKS,)),
                dma((4, 2, 2)), dma((2, 2, 2)), dma((2, 2, 2)), dma((3, 2, 2)), dma((4, 2, 2)), dma((4, 2)), dma,
                dma((2 * SPLIT + C_SEMS, 3)), dma((BLOCKS // 4,)), dma((SLOTS,)),
            ],
            compiler_params=pltpu.CompilerParams(
                collective_id=0, has_side_effects=True, vmem_limit_bytes=61 * 1024 * 1024
            ),
        )(a_blk.reshape(2, 4, 2, few, cols), b_blk)
        return c_blk.reshape(rows, cols)

    block_spec = P(("row", "depth"), "col")
    return jax.shard_map(local_product, mesh=mesh, in_specs=(block_spec, block_spec), out_specs=block_spec, check_vma=False)
```

```python
import jax
import jax.numpy as jnp
from jax import lax
from jax.experimental import pallas as pl
from jax.experimental.pallas import tpu as pltpu
from jax.sharding import PartitionSpec as P

MESH = pl.DeviceIdType.MESH
X_N, Y_N, Z_N = 4, 4, 8
BLOCKS = 16
SLOTS = 8
LOOP = 8
WIDE = 14
SPLIT = 6
ALL = 2
Z_SEMS, C_SEMS = 6, 6

PROGRAM = (
    "aaijabaibkiabjcljfnaifkklcgjdnbbmoomchffclneglkodmdmgofdgopa",
    "ehcoehpnttnegtbphqdopaqbfoqchetnqatobpuufguuoboqcogudfrcrcav",
    "nvvdhrvgeprndrdtoohfeaqvfpehbgufrebpacqvchgqoaprdssdgbsohreb",
    "qfhescpawpgfdraswbcqehqgbpafswrdrcscwhaqewafgdbpbfdswrghebcq",
    "fcfghepcsdpggrddhesqshheqpepprqsqqrrsrsrssss",
)


def chunk(n):
    return (n, None) if n < WIDE else (WIDE + (n - WIDE) // 2, (n - WIDE) % 2)


CHUNKS = WIDE + 2 * (BLOCKS - WIDE)


def kernel(a_hbm, b_hbm, c_out, a_own, a_all, s1, rl1, rl2, b_all, crecv, c0, prod,
           ld_sem, zr_sem, zs_sem, dr_sem, s1_sem, r1_sem, r2_sem, s2_sem, ag_sem, fw_sem, as_sem,
           cr_sem, cs_sem, c0_sem):
    row, y, z = lax.axis_index("row"), lax.axis_index("col"), lax.axis_index("depth")
    x, c = row // 2, row % 2
    width = b_all.shape[3]
    narrow = width // 2
    cols = a_own.shape[4]
    part_cols = (pl.ds(0, cols // 2), pl.ds(cols // 2, cols // 2))
    rest = slice(None)

    def at_x(dx):
        return {"row": 2 * ((x + dx + X_N) % X_N) + c}

    def at_y(dy):
        return {"col": (y + dy + Y_N) % Y_N}

    step = 1 - 2 * c
    z_long = {"depth": (z + step + Z_N) % Z_N}
    z_short = {"depth": (z - step + Z_N) % Z_N}
    partner = {"row": 2 * x + 1 - c}

    def send(src, dst, ssem, rsem, dev):
        pltpu.make_async_remote_copy(src_ref=src, dst_ref=dst, send_sem=ssem, recv_sem=rsem,
                                     device_id=dev, device_id_type=MESH).start()

    def wait(ref, sem):
        pltpu.make_async_copy(ref, ref, sem).wait()

    e_own = (y - x + Y_N) % Y_N
    flip = e_own // 3
    j_own = e_own

    def b_local(m, sem):
        return pltpu.make_async_copy(b_hbm.at[:, pl.ds(pl.multiple_of(m * width, width), width)],
                                     b_all.at[m, c * Z_N + z], ld_sem.at[sem])

    a_load = pltpu.make_async_copy(a_hbm, a_own, ld_sem.at[2])
    a_load.start()
    b_local(0, 0).start()
    barrier = pltpu.get_barrier_semaphore()
    for dev in (at_x(1), at_x(-1), at_y(1), at_y(-1), z_long, z_short, partner):
        pl.semaphore_signal(barrier, inc=1, device_id=dev, device_id_type=MESH)
    lax.fori_loop(1, BLOCKS, lambda m, _: (b_local(m, 1).start(), 0)[1], 0)

    def by_e(e, o, r, j, part, fn):
        col_part = rest if part is None else part_cols[part]

        @pl.when(e == 0)
        def _():
            fn(a_all.at[3, o, j, r, :, col_part])

        @pl.when(e != 0)
        def _():
            fn(s1.at[(e + Y_N - 1) % Y_N, o, r, :, col_part])

    for o in range(2):
        for r in range(2):
            by_e(e_own, o, r, 0, None, lambda dst: pltpu.make_async_copy(
                a_hbm.at[(o + flip) % 2, 0, r], dst, s1_sem.at[e_own, o, r]).start())
    pl.semaphore_wait(barrier, 7)
    a_load.wait()

    def ev_s1(o, r):
        h = (o + flip) % 2
        send(a_own.at[h, 2, r, :, part_cols[0]], rl1.at[0, o, r], as_sem, r1_sem.at[0, o, r], at_y(1))
        send(a_own.at[h, 2, r, :, part_cols[1]], rl1.at[1, o, r], as_sem, r1_sem.at[1, o, r], at_y(-1))
        sem = s1_sem.at[e_own, o, r]
        by_e(e_own, o, r, 1, None, lambda dst: send(a_own.at[h, 1, r], dst, as_sem, sem, at_y(1)))
        by_e(e_own, o, r, 3, None, lambda dst: send(a_own.at[h, 3, r], dst, as_sem, sem, at_y(-1)))

    def ev_r1(o, r, d):
        dy = 1 - 2 * d
        e = (y - dy - x + 2 * Y_N) % Y_N
        wait(rl1.at[d, o, r], r1_sem.at[d, o, r])
        by_e(e, o, r, 2, d, lambda dst: send(rl1.at[d, o, r], dst, as_sem, s1_sem.at[e, o, r], at_y(dy)))

    def ev_s2(o, r):
        wait(s1.at[0, o, r], s1_sem.at[1, o, r])
        wait(s1.at[2, o, r], s1_sem.at[3, o, r])
        g = 2 * o
        j = (y - x - 1 + 2 * Y_N) % Y_N
        send(s1.at[0, o, r], a_all.at[g, o, j, r], as_sem, s2_sem.at[g, o, r], at_x(1))
        j = (y - x + 1 + Y_N) % Y_N
        send(s1.at[2, o, r], a_all.at[g, 1 - o, j, r], as_sem, s2_sem.at[g, 1 - o, r], at_x(-1))

    def ev_s2f(o, r):
        wait(s1.at[1, o, r], s1_sem.at[2, o, r])
        for d in range(2):
            send(s1.at[1, o, r, :, part_cols[d]], rl2.at[d, o, r], as_sem, r2_sem.at[d, o, r], at_x(1 - 2 * d))

    def ev_r2(o, r, d):
        dx = 1 - 2 * d
        j = (y - x - dx + 2 * Y_N) % Y_N
        wait(rl2.at[d, o, r], r2_sem.at[d, o, r])
        send(rl2.at[d, o, r], a_all.at[1, o, j, r, :, part_cols[d]], as_sem, s2_sem.at[1, o, r], at_x(dx))

    def ev_ag(g, r, d):
        quarter = a_all.at[g, d, j_own, r]
        wait(quarter, s1_sem.at[0, d, r] if g == 3 else s2_sem.at[g, d, r])
        send(quarter, quarter, as_sem, ag_sem.at[g, d, r], at_y(1))
        send(quarter, quarter, as_sem, ag_sem.at[g, d, r], at_y(-1))

    def ev_fw(g, r, d):
        wait(a_all.at[0, 0, 0], ag_sem.at[g, d, r])
        for k, dy in ((0, 1), (1, -1)):
            j = (y - dy - x + 2 * Y_N) % Y_N
            part = a_all.at[g, d, j, r, :, part_cols[k]]
            send(part, part, as_sem, fw_sem.at[g, r], at_y(dy))

    def group_complete(g, r):
        wait(a_all.at[0, 0, 0], fw_sem.at[g, r])

    def block(hop):
        return c * Z_N + (z - hop * step + 2 * Z_N) % Z_N

    def lanes_of(n):
        half = chunk(n)[1]
        return rest if half is None else pl.ds(half * narrow, narrow)

    def piece(n, kb):
        return b_all.at[chunk(n)[0], kb, :, lanes_of(n)]

    def hand_over(n, kb):
        send(piece(n, kb), piece(n, kb), zs_sem.at[chunk(n)[0] // 4], dr_sem.at[n], partner)

    def forward_long(n, hop):
        p = piece(n, block(hop))
        send(p, p, zs_sem.at[chunk(n)[0] // 4], zr_sem.at[n % Z_SEMS, hop], z_long)

    def forward_short(n, hop):
        p = piece(n, block(-hop))
        send(p, p, zs_sem.at[chunk(n)[0] // 4], zr_sem.at[n % Z_SEMS, 4 + hop], z_short)

    def ev_own(n):
        if n == 0:
            b_local(0, 0).wait()
        elif n == 1:
            wait(b_all.at[0, pl.ds(0, BLOCKS - 1)], ld_sem.at[1])
        forward_long(n, 0)
        forward_short(n, 0)
        hand_over(n, block(0))

    def ev_long(n, hop):
        wait(piece(n, block(hop)), zr_sem.at[n % Z_SEMS, hop - 1])
        if hop < 4:
            forward_long(n, hop)
        hand_over(n, block(hop))

    def ev_short(n, hop):
        wait(piece(n, block(-hop)), zr_sem.at[n % Z_SEMS, 4 + hop - 1])
        if hop < 3:
            forward_short(n, hop)
        hand_over(n, block(-hop))

    def handed_over(n):
        wait(b_all.at[0, pl.ds(0, Z_N), :, lanes_of(n)], dr_sem.at[n])

    def dot(a, b):
        return jnp.dot(a.reshape(-1, cols), b.reshape(cols, -1), preferred_element_type=jnp.float32)

    def sum_sem(n, q):
        return 2 * SPLIT + (n - SPLIT) % C_SEMS if isinstance(q, slice) else 2 * n + q

    def sum_stage(n, g, q, m, lanes, first, size, when, reuse, old):
        slot = n % SLOTS
        keep = rest if isinstance(lanes, slice) else pl.ds(0, narrow)
        arrivals = sum_sem(n, q)

        def pass_on(src, ssem):
            for d in range(2):
                send(src.at[d], crecv.at[m, g, d, :, q, :, lanes], ssem, cr_sem.at[arrivals, g], at_x(1 - 2 * d))

        def arrived():
            wait(crecv.at[m, g - 1, :, :, q, :, lanes], cr_sem.at[arrivals, g - 1])

        def begin():
            reuse(lambda: wait(c0.at[slot, :, :, :, :, old], c0_sem.at[slot]))
            c0[slot, :, :, q, :, keep] = prod[:, :, q, :, keep]
            pass_on(c0.at[slot, :, :, q, :, keep], c0_sem.at[slot])

        def middle():
            arrived()
            crecv[m, g - 1, :, :, q, :, lanes] += prod[:, :, q, :, keep]
            pass_on(crecv.at[m, g - 1, :, :, q, :, lanes], cs_sem.at[m // 4])

        def end():
            arrived()
            total = crecv[m, g - 1, :, :, q, :, lanes] + prod[:, :, q, :, keep]
            c_out[:, :, q, :, pl.ds(pl.multiple_of(first, size), size)] = total.astype(c_out.dtype)

        a = a_all[g, :, :, q]
        prod[:, :, q, :, keep] = dot(a, b_all[m, :, :, lanes]).reshape(a.shape[:-1] + (size,))
        when(g == 0, begin)
        when((g == 1) | (g == 2), middle)
        when(g == 3, end)

    def branch(cond, fn):
        pl.when(cond)(fn)

    def fixed(cond, fn):
        if cond:
            fn()

    def sum_loop(code, split, wide):
        n, g, q = code // 8, code // 2 % 4, code % 2
        if split:
            pl.when(n < SPLIT)(lambda: sum_stage(n, g, q, n, rest, n * width, width, branch, lambda fn: None, rest))
        if wide:
            pl.when(n >= SPLIT)(lambda: sum_stage(n, g, rest, n, rest, n * width, width, branch,
                                                  pl.when(n >= SLOTS), rest))

    def sum_narrow(n, g):
        m, half = chunk(n)
        old = rest if n - SLOTS < WIDE else pl.ds(0, narrow)
        sum_stage(n, g, rest, m, lanes_of(n), m * width + half * narrow, narrow, fixed, lambda fn: fn(), old)

    def both(fn):
        def two(*args):
            fn(*args, 0)
            fn(*args, 1)
        return two

    chunks = range(CHUNKS)
    queues = {"a": [(ev_own, (n,)) for n in chunks]}
    for hop in range(1, 5):
        queues["abcde"[hop]] = [(ev_long, (n, hop)) for n in chunks]
    for hop in range(1, 4):
        queues["efgh"[hop]] = [(ev_short, (n, hop)) for n in chunks]
    by_half = [(o, r) for o in range(2) for r in range(2)]
    by_row = [(o, r) for r in range(2) for o in range(2)]
    queues["i"] = [(ev_s1, p) for p in by_row]
    queues["j"] = [(both(ev_r1), p) for p in by_row]
    queues["k"] = [(ev_s2, p) for p in by_row]
    queues["l"] = [(ev_s2f, p) for p in by_row]
    queues["m"] = [(both(ev_r2), p) for p in by_row]
    groups = [(g, r) for g in range(4) for r in range(2)]
    queues["n"] = [(both(ev_ag), p) for p in groups]
    queues["o"] = [(ev_fw, p + (d,)) for p in groups for d in range(2)]
    for g in range(4):
        queues["pqrs"[g]] = [(None, (n, g, 0 if n < SPLIT else ALL)) for n in chunks]
        queues["tuvw"[g]] = [(None, (n, g, 1)) for n in range(SPLIT)]

    steps, before, complete, handed = [], [], set(), set()
    for letter in "".join(PROGRAM):
        fn, args = queues[letter].pop(0)
        if fn is not None:
            before.append((fn, args))
            continue
        n, g, q = args
        for r in (range(2) if q == ALL else (q,)):
            if (g, r) not in complete:
                complete.add((g, r))
                before.append((group_complete, (g, r)))
        if n not in handed:
            handed.add(n)
            before.append((handed_over, (n,)))
        if n >= WIDE:
            before.append((sum_narrow, (n, g)))
        else:
            steps.append((before, (n * 4 + g) * 2 + q % 2, q != ALL))
            before = []

    def run(todo):
        for fn, args in todo:
            fn(*args)

    def in_loop(first, last):
        part = steps[first:last]

        def body(k, carry):
            code = part[0][1]
            for i, (todo, this, _) in enumerate(part):
                code = jnp.where(k == first + i, this, code)
                if todo:
                    pl.when(k == first + i)(lambda: run(todo))
            sum_loop(code, any(s for _, _, s in part), any(not s for _, _, s in part))
            return carry

        lax.fori_loop(first, last, body, 0)

    for first in range(0, len(steps), LOOP):
        in_loop(first, min(first + LOOP, len(steps)))
    run(before)

    for i in range(BLOCKS // 4):
        wait(b_all.at[pl.ds(0, 4), pl.ds(0, 15)], zs_sem.at[i])
        wait(crecv.at[pl.ds(0, 4), pl.ds(0, 2)], cs_sem.at[i])
    wait(b_all.at[pl.ds(0, 5)], as_sem)
    for n in range(CHUNKS - SLOTS, CHUNKS):
        keep = rest if n < WIDE else pl.ds(0, narrow)
        wait(c0.at[n % SLOTS, :, :, :, :, keep], c0_sem.at[n % SLOTS])


def solution(mesh):
    def local_product(a_blk, b_blk):
        rows, cols = a_blk.shape
        width = cols // BLOCKS
        few = rows // 16
        dma = pltpu.SemaphoreType.DMA
        c_blk = pl.pallas_call(
            kernel,
            name="matmul_3d",
            out_shape=pltpu.VMEM((2, 4, 2, few, cols), jnp.bfloat16),
            in_specs=[pl.BlockSpec(memory_space=pl.ANY)] * 2,
            out_specs=pl.BlockSpec(memory_space=pltpu.VMEM),
            scratch_shapes=[
                pltpu.VMEM((2, 4, 2, few, cols), jnp.bfloat16),
                pltpu.VMEM((4, 2, 4, 2, few, cols), jnp.bfloat16),
                pltpu.VMEM((3, 2, 2, few, cols), jnp.bfloat16),
                pltpu.VMEM((2, 2, 2, few, cols // 2), jnp.bfloat16),
                pltpu.VMEM((2, 2, 2, few, cols // 2), jnp.bfloat16),
                pltpu.VMEM((BLOCKS, 2 * Z_N, rows, width), jnp.bfloat16),
                pltpu.VMEM((BLOCKS, 3, 2, 4, 2, few, width), jnp.float32),
                pltpu.VMEM((SLOTS, 2, 4, 2, few, width), jnp.float32),
                pltpu.VMEM((2, 4, 2, few, width), jnp.float32),
                dma((3,)), dma((Z_SEMS, 7)), dma((BLOCKS // 4,)), dma((CHUNKS,)),
                dma((4, 2, 2)), dma((2, 2, 2)), dma((2, 2, 2)), dma((3, 2, 2)), dma((4, 2, 2)), dma((4, 2)), dma,
                dma((2 * SPLIT + C_SEMS, 3)), dma((BLOCKS // 4,)), dma((SLOTS,)),
            ],
            compiler_params=pltpu.CompilerParams(
                collective_id=0, has_side_effects=True, vmem_limit_bytes=61 * 1024 * 1024
            ),
        )(a_blk.reshape(2, 4, 2, few, cols), b_blk)
        return c_blk.reshape(rows, cols)

    block_spec = P(("row", "depth"), "col")
    return jax.shard_map(local_product, mesh=mesh, in_specs=(block_spec, block_spec), out_specs=block_spec, check_vma=False)
```

```python
import jax
import jax.numpy as jnp
from jax import lax
from jax.experimental import pallas as pl
from jax.experimental.pallas import tpu as pltpu
from jax.sharding import PartitionSpec as P

MESH = pl.DeviceIdType.MESH
X_N, Y_N, Z_N = 4, 4, 8
BLOCKS = 16
SLOTS = 8
LOOP = 8
WIDE = 14
SPLIT = 4
ALL = 2
Z_SEMS, C_SEMS = 6, 6

PROGRAM = (
    "aiaaijajibiabkbkffjcnlccabkmflfjdngglommldocdbnmoeoebkhgdogh",
    "ppofeanhttcphfeqcqgtbootnpdgquduuncuhfeaqohaepopbogqdfornnfr",
    "rhbcvarvqvcdvgegoboadfrephaprochsqebsfobgspsgqfdwrqccsheardd",
    "pwgrahfebawpehqbcpbqgcdfrcsqdfrgaehagdpewharbsefhbpqfbcgpcss",
    "cfqgddrdhgsehqserhspepprsqsqqrrrssss",
)


def chunk(n):
    return (n, None) if n < WIDE else (WIDE + (n - WIDE) // 2, (n - WIDE) % 2)


CHUNKS = WIDE + 2 * (BLOCKS - WIDE)


def kernel(a_hbm, b_hbm, c_out, a_own, a_all, s1, rl1, rl2, b_all, crecv, c0, prod,
           ld_sem, zr_sem, zs_sem, dr_sem, s1_sem, r1_sem, r2_sem, s2_sem, ag_sem, fw_sem, as_sem,
           cr_sem, cs_sem, c0_sem):
    row, y, z = lax.axis_index("row"), lax.axis_index("col"), lax.axis_index("depth")
    x, c = row // 2, row % 2
    width = b_all.shape[3]
    narrow = width // 2
    cols = a_own.shape[4]
    part_cols = (pl.ds(0, cols // 2), pl.ds(cols // 2, cols // 2))
    rest = slice(None)

    def at_x(dx):
        return {"row": 2 * ((x + dx + X_N) % X_N) + c}

    def at_y(dy):
        return {"col": (y + dy + Y_N) % Y_N}

    step = 1 - 2 * c
    z_long = {"depth": (z + step + Z_N) % Z_N}
    z_short = {"depth": (z - step + Z_N) % Z_N}
    partner = {"row": 2 * x + 1 - c}

    def send(src, dst, ssem, rsem, dev):
        pltpu.make_async_remote_copy(src_ref=src, dst_ref=dst, send_sem=ssem, recv_sem=rsem,
                                     device_id=dev, device_id_type=MESH).start()

    def wait(ref, sem):
        pltpu.make_async_copy(ref, ref, sem).wait()

    e_own = (y - x + Y_N) % Y_N
    flip = e_own // 3
    j_own = e_own

    def b_local(m, sem):
        return pltpu.make_async_copy(b_hbm.at[:, pl.ds(pl.multiple_of(m * width, width), width)],
                                     b_all.at[m, c * Z_N + z], ld_sem.at[sem])

    a_load = pltpu.make_async_copy(a_hbm, a_own, ld_sem.at[2])
    a_load.start()
    b_local(0, 0).start()
    barrier = pltpu.get_barrier_semaphore()
    for dev in (at_x(1), at_x(-1), at_y(1), at_y(-1), z_long, z_short, partner):
        pl.semaphore_signal(barrier, inc=1, device_id=dev, device_id_type=MESH)
    lax.fori_loop(1, BLOCKS, lambda m, _: (b_local(m, 1).start(), 0)[1], 0)

    def by_e(e, o, r, j, part, fn):
        col_part = rest if part is None else part_cols[part]

        @pl.when(e == 0)
        def _():
            fn(a_all.at[3, o, j, r, :, col_part])

        @pl.when(e != 0)
        def _():
            fn(s1.at[(e + Y_N - 1) % Y_N, o, r, :, col_part])

    for o in range(2):
        for r in range(2):
            by_e(e_own, o, r, 0, None, lambda dst: pltpu.make_async_copy(
                a_hbm.at[(o + flip) % 2, 0, r], dst, s1_sem.at[e_own, o, r]).start())
    pl.semaphore_wait(barrier, 7)
    a_load.wait()

    def ev_s1(o, r):
        h = (o + flip) % 2
        send(a_own.at[h, 2, r, :, part_cols[0]], rl1.at[0, o, r], as_sem, r1_sem.at[0, o, r], at_y(1))
        send(a_own.at[h, 2, r, :, part_cols[1]], rl1.at[1, o, r], as_sem, r1_sem.at[1, o, r], at_y(-1))
        sem = s1_sem.at[e_own, o, r]
        by_e(e_own, o, r, 1, None, lambda dst: send(a_own.at[h, 1, r], dst, as_sem, sem, at_y(1)))
        by_e(e_own, o, r, 3, None, lambda dst: send(a_own.at[h, 3, r], dst, as_sem, sem, at_y(-1)))

    def ev_r1(o, r, d):
        dy = 1 - 2 * d
        e = (y - dy - x + 2 * Y_N) % Y_N
        wait(rl1.at[d, o, r], r1_sem.at[d, o, r])
        by_e(e, o, r, 2, d, lambda dst: send(rl1.at[d, o, r], dst, as_sem, s1_sem.at[e, o, r], at_y(dy)))

    def ev_s2(o, r):
        wait(s1.at[0, o, r], s1_sem.at[1, o, r])
        wait(s1.at[2, o, r], s1_sem.at[3, o, r])
        g = 2 * o
        j = (y - x - 1 + 2 * Y_N) % Y_N
        send(s1.at[0, o, r], a_all.at[g, o, j, r], as_sem, s2_sem.at[g, o, r], at_x(1))
        j = (y - x + 1 + Y_N) % Y_N
        send(s1.at[2, o, r], a_all.at[g, 1 - o, j, r], as_sem, s2_sem.at[g, 1 - o, r], at_x(-1))

    def ev_s2f(o, r):
        wait(s1.at[1, o, r], s1_sem.at[2, o, r])
        for d in range(2):
            send(s1.at[1, o, r, :, part_cols[d]], rl2.at[d, o, r], as_sem, r2_sem.at[d, o, r], at_x(1 - 2 * d))

    def ev_r2(o, r, d):
        dx = 1 - 2 * d
        j = (y - x - dx + 2 * Y_N) % Y_N
        wait(rl2.at[d, o, r], r2_sem.at[d, o, r])
        send(rl2.at[d, o, r], a_all.at[1, o, j, r, :, part_cols[d]], as_sem, s2_sem.at[1, o, r], at_x(dx))

    def ev_ag(g, r, d):
        quarter = a_all.at[g, d, j_own, r]
        wait(quarter, s1_sem.at[0, d, r] if g == 3 else s2_sem.at[g, d, r])
        send(quarter, quarter, as_sem, ag_sem.at[g, d, r], at_y(1))
        send(quarter, quarter, as_sem, ag_sem.at[g, d, r], at_y(-1))

    def ev_fw(g, r, d):
        wait(a_all.at[0, 0, 0], ag_sem.at[g, d, r])
        for k, dy in ((0, 1), (1, -1)):
            j = (y - dy - x + 2 * Y_N) % Y_N
            part = a_all.at[g, d, j, r, :, part_cols[k]]
            send(part, part, as_sem, fw_sem.at[g, r], at_y(dy))

    def group_complete(g, r):
        wait(a_all.at[0, 0, 0], fw_sem.at[g, r])

    def block(hop):
        return c * Z_N + (z - hop * step + 2 * Z_N) % Z_N

    def lanes_of(n):
        half = chunk(n)[1]
        return rest if half is None else pl.ds(half * narrow, narrow)

    def piece(n, kb):
        return b_all.at[chunk(n)[0], kb, :, lanes_of(n)]

    def hand_over(n, kb):
        send(piece(n, kb), piece(n, kb), zs_sem.at[chunk(n)[0] // 4], dr_sem.at[n], partner)

    def forward_long(n, hop):
        p = piece(n, block(hop))
        send(p, p, zs_sem.at[chunk(n)[0] // 4], zr_sem.at[n % Z_SEMS, hop], z_long)

    def forward_short(n, hop):
        p = piece(n, block(-hop))
        send(p, p, zs_sem.at[chunk(n)[0] // 4], zr_sem.at[n % Z_SEMS, 4 + hop], z_short)

    def ev_own(n):
        if n == 0:
            b_local(0, 0).wait()
        elif n == 1:
            wait(b_all.at[0, pl.ds(0, BLOCKS - 1)], ld_sem.at[1])
        forward_long(n, 0)
        forward_short(n, 0)
        hand_over(n, block(0))

    def ev_long(n, hop):
        wait(piece(n, block(hop)), zr_sem.at[n % Z_SEMS, hop - 1])
        if hop < 4:
            forward_long(n, hop)
        hand_over(n, block(hop))

    def ev_short(n, hop):
        wait(piece(n, block(-hop)), zr_sem.at[n % Z_SEMS, 4 + hop - 1])
        if hop < 3:
            forward_short(n, hop)
        hand_over(n, block(-hop))

    def handed_over(n):
        wait(b_all.at[0, pl.ds(0, Z_N), :, lanes_of(n)], dr_sem.at[n])

    def dot(a, b):
        return jnp.dot(a.reshape(-1, cols), b.reshape(cols, -1), preferred_element_type=jnp.float32)

    def sum_sem(n, q):
        return 2 * SPLIT + (n - SPLIT) % C_SEMS if isinstance(q, slice) else 2 * n + q

    def sum_stage(n, g, q, m, lanes, first, size, when, reuse, old):
        slot = n % SLOTS
        keep = rest if isinstance(lanes, slice) else pl.ds(0, narrow)
        arrivals = sum_sem(n, q)

        def pass_on(src, ssem):
            for d in range(2):
                send(src.at[d], crecv.at[m, g, d, :, q, :, lanes], ssem, cr_sem.at[arrivals, g], at_x(1 - 2 * d))

        def arrived():
            wait(crecv.at[m, g - 1, :, :, q, :, lanes], cr_sem.at[arrivals, g - 1])

        def begin():
            reuse(lambda: wait(c0.at[slot, :, :, :, :, old], c0_sem.at[slot]))
            c0[slot, :, :, q, :, keep] = prod[:, :, q, :, keep]
            pass_on(c0.at[slot, :, :, q, :, keep], c0_sem.at[slot])

        def middle():
            arrived()
            crecv[m, g - 1, :, :, q, :, lanes] += prod[:, :, q, :, keep]
            pass_on(crecv.at[m, g - 1, :, :, q, :, lanes], cs_sem.at[m // 4])

        def end():
            arrived()
            total = crecv[m, g - 1, :, :, q, :, lanes] + prod[:, :, q, :, keep]
            c_out[:, :, q, :, pl.ds(pl.multiple_of(first, size), size)] = total.astype(c_out.dtype)

        a = a_all[g, :, :, q]
        prod[:, :, q, :, keep] = dot(a, b_all[m, :, :, lanes]).reshape(a.shape[:-1] + (size,))
        when(g == 0, begin)
        when((g == 1) | (g == 2), middle)
        when(g == 3, end)

    def branch(cond, fn):
        pl.when(cond)(fn)

    def fixed(cond, fn):
        if cond:
            fn()

    def sum_loop(code, split, wide):
        n, g, q = code // 8, code // 2 % 4, code % 2
        if split:
            pl.when(n < SPLIT)(lambda: sum_stage(n, g, q, n, rest, n * width, width, branch, lambda fn: None, rest))
        if wide:
            pl.when(n >= SPLIT)(lambda: sum_stage(n, g, rest, n, rest, n * width, width, branch,
                                                  pl.when(n >= SLOTS), rest))

    def sum_narrow(n, g):
        m, half = chunk(n)
        old = rest if n - SLOTS < WIDE else pl.ds(0, narrow)
        sum_stage(n, g, rest, m, lanes_of(n), m * width + half * narrow, narrow, fixed, lambda fn: fn(), old)

    def both(fn):
        def two(*args):
            fn(*args, 0)
            fn(*args, 1)
        return two

    chunks = range(CHUNKS)
    queues = {"a": [(ev_own, (n,)) for n in chunks]}
    for hop in range(1, 5):
        queues["abcde"[hop]] = [(ev_long, (n, hop)) for n in chunks]
    for hop in range(1, 4):
        queues["efgh"[hop]] = [(ev_short, (n, hop)) for n in chunks]
    by_half = [(o, r) for o in range(2) for r in range(2)]
    by_row = [(o, r) for r in range(2) for o in range(2)]
    queues["i"] = [(ev_s1, p) for p in by_half]
    queues["j"] = [(both(ev_r1), p) for p in by_half]
    queues["k"] = [(ev_s2, p) for p in by_half]
    queues["l"] = [(ev_s2f, p) for p in by_row]
    queues["m"] = [(both(ev_r2), p) for p in by_row]
    groups = [(g, r) for g in range(4) for r in range(2)]
    queues["n"] = [(both(ev_ag), p) for p in groups]
    queues["o"] = [(ev_fw, p + (d,)) for p in groups for d in range(2)]
    for g in range(4):
        queues["pqrs"[g]] = [(None, (n, g, 0 if n < SPLIT else ALL)) for n in chunks]
        queues["tuvw"[g]] = [(None, (n, g, 1)) for n in range(SPLIT)]

    steps, before, complete, handed = [], [], set(), set()
    for letter in "".join(PROGRAM):
        fn, args = queues[letter].pop(0)
        if fn is not None:
            before.append((fn, args))
            continue
        n, g, q = args
        for r in (range(2) if q == ALL else (q,)):
            if (g, r) not in complete:
                complete.add((g, r))
                before.append((group_complete, (g, r)))
        if n not in handed:
            handed.add(n)
            before.append((handed_over, (n,)))
        if n >= WIDE:
            before.append((sum_narrow, (n, g)))
        else:
            steps.append((before, (n * 4 + g) * 2 + q % 2, q != ALL))
            before = []

    def run(todo):
        for fn, args in todo:
            fn(*args)

    def in_loop(first, last):
        part = steps[first:last]

        def body(k, carry):
            code = part[0][1]
            for i, (todo, this, _) in enumerate(part):
                code = jnp.where(k == first + i, this, code)
                if todo:
                    pl.when(k == first + i)(lambda: run(todo))
            sum_loop(code, any(s for _, _, s in part), any(not s for _, _, s in part))
            return carry

        lax.fori_loop(first, last, body, 0)

    for first in range(0, len(steps), LOOP):
        in_loop(first, min(first + LOOP, len(steps)))
    run(before)

    for i in range(BLOCKS // 4):
        wait(b_all.at[pl.ds(0, 4), pl.ds(0, 15)], zs_sem.at[i])
        wait(crecv.at[pl.ds(0, 4), pl.ds(0, 2)], cs_sem.at[i])
    wait(b_all.at[pl.ds(0, 5)], as_sem)
    for n in range(CHUNKS - SLOTS, CHUNKS):
        keep = rest if n < WIDE else pl.ds(0, narrow)
        wait(c0.at[n % SLOTS, :, :, :, :, keep], c0_sem.at[n % SLOTS])


def solution(mesh):
    def local_product(a_blk, b_blk):
        rows, cols = a_blk.shape
        width = cols // BLOCKS
        few = rows // 16
        dma = pltpu.SemaphoreType.DMA
        c_blk = pl.pallas_call(
            kernel,
            name="matmul_3d",
            out_shape=pltpu.VMEM((2, 4, 2, few, cols), jnp.bfloat16),
            in_specs=[pl.BlockSpec(memory_space=pl.ANY)] * 2,
            out_specs=pl.BlockSpec(memory_space=pltpu.VMEM),
            scratch_shapes=[
                pltpu.VMEM((2, 4, 2, few, cols), jnp.bfloat16),
                pltpu.VMEM((4, 2, 4, 2, few, cols), jnp.bfloat16),
                pltpu.VMEM((3, 2, 2, few, cols), jnp.bfloat16),
                pltpu.VMEM((2, 2, 2, few, cols // 2), jnp.bfloat16),
                pltpu.VMEM((2, 2, 2, few, cols // 2), jnp.bfloat16),
                pltpu.VMEM((BLOCKS, 2 * Z_N, rows, width), jnp.bfloat16),
                pltpu.VMEM((BLOCKS, 3, 2, 4, 2, few, width), jnp.float32),
                pltpu.VMEM((SLOTS, 2, 4, 2, few, width), jnp.float32),
                pltpu.VMEM((2, 4, 2, few, width), jnp.float32),
                dma((3,)), dma((Z_SEMS, 7)), dma((BLOCKS // 4,)), dma((CHUNKS,)),
                dma((4, 2, 2)), dma((2, 2, 2)), dma((2, 2, 2)), dma((3, 2, 2)), dma((4, 2, 2)), dma((4, 2)), dma,
                dma((2 * SPLIT + C_SEMS, 3)), dma((BLOCKS // 4,)), dma((SLOTS,)),
            ],
            compiler_params=pltpu.CompilerParams(
                collective_id=0, has_side_effects=True, vmem_limit_bytes=61 * 1024 * 1024
            ),
        )(a_blk.reshape(2, 4, 2, few, cols), b_blk)
        return c_blk.reshape(rows, cols)

    block_spec = P(("row", "depth"), "col")
    return jax.shard_map(local_product, mesh=mesh, in_specs=(block_spec, block_spec), out_specs=block_spec, check_vma=False)
```

```python
import jax
import jax.numpy as jnp
from jax import lax
from jax.experimental import pallas as pl
from jax.experimental.pallas import tpu as pltpu
from jax.sharding import PartitionSpec as P

MESH = pl.DeviceIdType.MESH
X_N, Y_N, Z_N = 4, 4, 8
BLOCKS = 16
SLOTS = 8
LOOP = 8
WIDE = 14
SPLIT = 6
ALL = 2
Z_SEMS, C_SEMS = 6, 6

PROGRAM = (
    "aaijabaibkiabjcljfnaifkklcgjdnbbmoomchffclneglkodmdmgofdgopa",
    "ehcoehpnttnegtbphqdopaqbfoqchetnqatobpuufguuoboqcogudfrcrcav",
    "nvvdhrvgeprndrdtoohfeaqvfpehbgufrebpacqvchgqoaprdssdgbsohreb",
    "qfhescpawpgfdraswbcqehqgbpafswrdrcscwhaqewafgdbpbfdswrghebcq",
    "fcfghepcsdpggrddhesqshheqpepprqsqqrrsrsrssss",
)


def chunk(n):
    return (n, None) if n < WIDE else (WIDE + (n - WIDE) // 2, (n - WIDE) % 2)


CHUNKS = WIDE + 2 * (BLOCKS - WIDE)


def kernel(a_hbm, b_hbm, c_out, a_own, a_all, s1, rl1, rl2, b_all, crecv, c0, prod,
           ld_sem, zr_sem, zs_sem, dr_sem, s1_sem, r1_sem, r2_sem, s2_sem, ag_sem, fw_sem, as_sem,
           cr_sem, cs_sem, c0_sem):
    row, y, z = lax.axis_index("row"), lax.axis_index("col"), lax.axis_index("depth")
    x, c = row // 2, row % 2
    width = b_all.shape[3]
    narrow = width // 2
    cols = a_own.shape[4]
    part_cols = (pl.ds(0, cols // 2), pl.ds(cols // 2, cols // 2))
    rest = slice(None)

    def at_x(dx):
        return {"row": 2 * ((x + dx + X_N) % X_N) + c}

    def at_y(dy):
        return {"col": (y + dy + Y_N) % Y_N}

    step = 1 - 2 * c
    z_long = {"depth": (z + step + Z_N) % Z_N}
    z_short = {"depth": (z - step + Z_N) % Z_N}
    partner = {"row": 2 * x + 1 - c}

    def send(src, dst, ssem, rsem, dev):
        pltpu.make_async_remote_copy(src_ref=src, dst_ref=dst, send_sem=ssem, recv_sem=rsem,
                                     device_id=dev, device_id_type=MESH).start()

    def wait(ref, sem):
        pltpu.make_async_copy(ref, ref, sem).wait()

    e_own = (y - x + Y_N) % Y_N
    flip = e_own // 3
    j_own = e_own

    def b_local(m, sem):
        return pltpu.make_async_copy(b_hbm.at[:, pl.ds(pl.multiple_of(m * width, width), width)],
                                     b_all.at[m, c * Z_N + z], ld_sem.at[sem])

    def a_load(r):
        return pltpu.make_async_copy(a_hbm.at[:, :, r], a_own.at[:, :, r], ld_sem.at[2 + r])

    a_load(0).start()
    b_local(0, 0).start()
    a_load(1).start()
    barrier = pltpu.get_barrier_semaphore()
    for dev in (at_x(1), at_x(-1), at_y(1), at_y(-1), z_long, z_short, partner):
        pl.semaphore_signal(barrier, inc=1, device_id=dev, device_id_type=MESH)
    lax.fori_loop(1, BLOCKS, lambda m, _: (b_local(m, 1).start(), 0)[1], 0)

    def quarter_sem(e, o, r):
        return s1_sem.at[(e + 1) % 2 * (2 - e // 2), o, r]

    def by_e(e, o, r, j, part, fn):
        col_part = rest if part is None else part_cols[part]

        @pl.when(e == 0)
        def _():
            fn(a_all.at[3, o, j, r, :, col_part])

        @pl.when(e != 0)
        def _():
            fn(s1.at[(e + Y_N - 1) % Y_N, o, r, :, col_part])

    for o in range(2):
        for r in range(2):
            by_e(e_own, o, r, 0, None, lambda dst: pltpu.make_async_copy(
                a_hbm.at[(o + flip) % 2, 0, r], dst, quarter_sem(e_own, o, r)).start())
    pl.semaphore_wait(barrier, 7)
    loaded = set()

    def ev_s1(o, r):
        if r not in loaded:
            loaded.add(r)
            a_load(r).wait()
        h = (o + flip) % 2
        send(a_own.at[h, 2, r, :, part_cols[0]], rl1.at[0, o, r], as_sem, r1_sem.at[o, r], at_y(1))
        send(a_own.at[h, 2, r, :, part_cols[1]], rl1.at[1, o, r], as_sem, r1_sem.at[o, r], at_y(-1))
        sem = quarter_sem(e_own, o, r)
        by_e(e_own, o, r, 1, None, lambda dst: send(a_own.at[h, 1, r], dst, as_sem, sem, at_y(1)))
        by_e(e_own, o, r, 3, None, lambda dst: send(a_own.at[h, 3, r], dst, as_sem, sem, at_y(-1)))

    def ev_r1(o, r):
        wait(rl1.at[:, o, r], r1_sem.at[o, r])
        for d, dy in ((0, 1), (1, -1)):
            e = (y - dy - x + 2 * Y_N) % Y_N
            by_e(e, o, r, 2, d, lambda dst: send(rl1.at[d, o, r], dst, as_sem, quarter_sem(e, o, r), at_y(dy)))

    def ev_s2(o, r):
        wait(s1.at[pl.ds(0, 2), o, r], quarter_sem(1, o, r))
        g = 2 * o
        j = (y - x - 1 + 2 * Y_N) % Y_N
        send(s1.at[0, o, r], a_all.at[g, o, j, r], as_sem, s2_sem.at[g, r], at_x(1))
        j = (y - x + 1 + Y_N) % Y_N
        send(s1.at[2, o, r], a_all.at[g, 1 - o, j, r], as_sem, s2_sem.at[g, r], at_x(-1))

    def ev_s2f(o, r):
        wait(s1.at[1, o, r], quarter_sem(2, o, r))
        for d in range(2):
            send(s1.at[1, o, r, :, part_cols[d]], rl2.at[d, o, r], as_sem, r2_sem.at[o, r], at_x(1 - 2 * d))

    def ev_r2(o, r):
        wait(rl2.at[:, o, r], r2_sem.at[o, r])
        for d, dx in ((0, 1), (1, -1)):
            j = (y - x - dx + 2 * Y_N) % Y_N
            send(rl2.at[d, o, r], a_all.at[1, o, j, r, :, part_cols[d]], as_sem, s2_sem.at[1, r], at_x(dx))

    def ev_ag(g, r):
        if g == 3:
            for o in range(2):
                wait(a_all.at[g, o, j_own, r], quarter_sem(0, o, r))
        else:
            wait(a_all.at[g, :, j_own, r], s2_sem.at[g, r])
        for d in range(2):
            quarter = a_all.at[g, d, j_own, r]
            send(quarter, quarter, as_sem, ag_sem.at[g, d, r], at_y(1))
            send(quarter, quarter, as_sem, ag_sem.at[g, d, r], at_y(-1))

    def ev_fw(g, r, d):
        wait(a_all.at[0, 0, 0], ag_sem.at[g, d, r])
        for k, dy in ((0, 1), (1, -1)):
            j = (y - dy - x + 2 * Y_N) % Y_N
            part = a_all.at[g, d, j, r, :, part_cols[k]]
            send(part, part, as_sem, fw_sem.at[g, r], at_y(dy))

    def group_complete(g, r):
        wait(a_all.at[0, 0, 0], fw_sem.at[g, r])

    def block(hop):
        return c * Z_N + (z - hop * step + 2 * Z_N) % Z_N

    def lanes_of(n):
        half = chunk(n)[1]
        return rest if half is None else pl.ds(half * narrow, narrow)

    def piece(n, kb):
        return b_all.at[chunk(n)[0], kb, :, lanes_of(n)]

    def hand_over(n, kb):
        send(piece(n, kb), piece(n, kb), zs_sem.at[chunk(n)[0] // 4], dr_sem.at[n], partner)

    def forward_long(n, hop):
        p = piece(n, block(hop))
        send(p, p, zs_sem.at[chunk(n)[0] // 4], zr_sem.at[n % Z_SEMS, hop], z_long)

    def forward_short(n, hop):
        p = piece(n, block(-hop))
        send(p, p, zs_sem.at[chunk(n)[0] // 4], zr_sem.at[n % Z_SEMS, 4 + hop], z_short)

    def ev_own(n):
        if n == 0:
            b_local(0, 0).wait()
        elif n == 1:
            wait(b_all.at[0, pl.ds(0, BLOCKS - 1)], ld_sem.at[1])
        forward_long(n, 0)
        forward_short(n, 0)
        hand_over(n, block(0))

    def ev_long(n, hop):
        wait(piece(n, block(hop)), zr_sem.at[n % Z_SEMS, hop - 1])
        if hop < 4:
            forward_long(n, hop)
        hand_over(n, block(hop))

    def ev_short(n, hop):
        wait(piece(n, block(-hop)), zr_sem.at[n % Z_SEMS, 4 + hop - 1])
        if hop < 3:
            forward_short(n, hop)
        hand_over(n, block(-hop))

    def handed_over(n):
        wait(b_all.at[0, pl.ds(0, Z_N), :, lanes_of(n)], dr_sem.at[n])

    def dot(a, b):
        return jnp.dot(a.reshape(-1, cols), b.reshape(cols, -1), preferred_element_type=jnp.float32)

    def sum_sem(n, q):
        return 2 * SPLIT + (n - SPLIT) % C_SEMS if isinstance(q, slice) else 2 * n + q

    def sum_stage(n, g, q, m, lanes, first, size, when, reuse, old):
        slot = n % SLOTS
        keep = rest if isinstance(lanes, slice) else pl.ds(0, narrow)
        arrivals = sum_sem(n, q)

        def pass_on(src, ssem):
            for d in range(2):
                send(src.at[d], crecv.at[m, g, d, :, q, :, lanes], ssem, cr_sem.at[arrivals, g], at_x(1 - 2 * d))

        def arrived():
            wait(crecv.at[m, g - 1, :, :, q, :, lanes], cr_sem.at[arrivals, g - 1])

        def begin():
            reuse(lambda: wait(c0.at[slot, :, :, :, :, old], c0_sem.at[slot]))
            c0[slot, :, :, q, :, keep] = prod[:, :, q, :, keep]
            pass_on(c0.at[slot, :, :, q, :, keep], c0_sem.at[slot])

        def middle():
            arrived()
            crecv[m, g - 1, :, :, q, :, lanes] += prod[:, :, q, :, keep]
            pass_on(crecv.at[m, g - 1, :, :, q, :, lanes], cs_sem.at[m // 4])

        def end():
            arrived()
            total = crecv[m, g - 1, :, :, q, :, lanes] + prod[:, :, q, :, keep]
            c_out[:, :, q, :, pl.ds(pl.multiple_of(first, size), size)] = total.astype(c_out.dtype)

        a = a_all[g, :, :, q]
        prod[:, :, q, :, keep] = dot(a, b_all[m, :, :, lanes]).reshape(a.shape[:-1] + (size,))
        when(g == 0, begin)
        when((g == 1) | (g == 2), middle)
        when(g == 3, end)

    def branch(cond, fn):
        pl.when(cond)(fn)

    def fixed(cond, fn):
        if cond:
            fn()

    def sum_loop(code, split, wide):
        n, g, q = code // 8, code // 2 % 4, code % 2
        if split:
            pl.when(n < SPLIT)(lambda: sum_stage(n, g, q, n, rest, n * width, width, branch, lambda fn: None, rest))
        if wide:
            pl.when(n >= SPLIT)(lambda: sum_stage(n, g, rest, n, rest, n * width, width, branch,
                                                  pl.when(n >= SLOTS), rest))

    def sum_narrow(n, g):
        m, half = chunk(n)
        old = rest if n - SLOTS < WIDE else pl.ds(0, narrow)
        sum_stage(n, g, rest, m, lanes_of(n), m * width + half * narrow, narrow, fixed, lambda fn: fn(), old)

    chunks = range(CHUNKS)
    queues = {"a": [(ev_own, (n,)) for n in chunks]}
    for hop in range(1, 5):
        queues["abcde"[hop]] = [(ev_long, (n, hop)) for n in chunks]
    for hop in range(1, 4):
        queues["efgh"[hop]] = [(ev_short, (n, hop)) for n in chunks]
    by_half = [(o, r) for o in range(2) for r in range(2)]
    by_row = [(o, r) for r in range(2) for o in range(2)]
    queues["i"] = [(ev_s1, p) for p in by_row]
    queues["j"] = [(ev_r1, p) for p in by_row]
    queues["k"] = [(ev_s2, p) for p in by_row]
    queues["l"] = [(ev_s2f, p) for p in by_row]
    queues["m"] = [(ev_r2, p) for p in by_row]
    groups = [(g, r) for g in range(4) for r in range(2)]
    queues["n"] = [(ev_ag, p) for p in groups]
    queues["o"] = [(ev_fw, p + (d,)) for p in groups for d in range(2)]
    for g in range(4):
        queues["pqrs"[g]] = [(None, (n, g, 0 if n < SPLIT else ALL)) for n in chunks]
        queues["tuvw"[g]] = [(None, (n, g, 1)) for n in range(SPLIT)]

    steps, before, complete, handed = [], [], set(), set()
    for letter in "".join(PROGRAM):
        fn, args = queues[letter].pop(0)
        if fn is not None:
            before.append((fn, args))
            continue
        n, g, q = args
        for r in (range(2) if q == ALL else (q,)):
            if (g, r) not in complete:
                complete.add((g, r))
                before.append((group_complete, (g, r)))
        if n not in handed:
            handed.add(n)
            before.append((handed_over, (n,)))
        if n >= WIDE:
            before.append((sum_narrow, (n, g)))
        else:
            steps.append((before, (n * 4 + g) * 2 + q % 2, q != ALL))
            before = []

    def run(todo):
        for fn, args in todo:
            fn(*args)

    def in_loop(first, last):
        part = steps[first:last]

        def body(k, carry):
            code = part[0][1]
            for i, (todo, this, _) in enumerate(part):
                code = jnp.where(k == first + i, this, code)
                if todo:
                    pl.when(k == first + i)(lambda: run(todo))
            sum_loop(code, any(s for _, _, s in part), any(not s for _, _, s in part))
            return carry

        lax.fori_loop(first, last, body, 0)

    for first in range(0, len(steps), LOOP):
        in_loop(first, min(first + LOOP, len(steps)))
    run(before)

    for i in range(BLOCKS // 4):
        wait(b_all.at[pl.ds(0, 4), pl.ds(0, 15)], zs_sem.at[i])
        wait(crecv.at[pl.ds(0, 4), pl.ds(0, 2)], cs_sem.at[i])
    wait(b_all.at[pl.ds(0, 5)], as_sem)
    for n in range(CHUNKS - SLOTS, CHUNKS):
        keep = rest if n < WIDE else pl.ds(0, narrow)
        wait(c0.at[n % SLOTS, :, :, :, :, keep], c0_sem.at[n % SLOTS])


def solution(mesh):
    def local_product(a_blk, b_blk):
        rows, cols = a_blk.shape
        width = cols // BLOCKS
        few = rows // 16
        dma = pltpu.SemaphoreType.DMA
        c_blk = pl.pallas_call(
            kernel,
            name="matmul_3d",
            out_shape=pltpu.VMEM((2, 4, 2, few, cols), jnp.bfloat16),
            in_specs=[pl.BlockSpec(memory_space=pl.ANY)] * 2,
            out_specs=pl.BlockSpec(memory_space=pltpu.VMEM),
            scratch_shapes=[
                pltpu.VMEM((2, 4, 2, few, cols), jnp.bfloat16),
                pltpu.VMEM((4, 2, 4, 2, few, cols), jnp.bfloat16),
                pltpu.VMEM((3, 2, 2, few, cols), jnp.bfloat16),
                pltpu.VMEM((2, 2, 2, few, cols // 2), jnp.bfloat16),
                pltpu.VMEM((2, 2, 2, few, cols // 2), jnp.bfloat16),
                pltpu.VMEM((BLOCKS, 2 * Z_N, rows, width), jnp.bfloat16),
                pltpu.VMEM((BLOCKS, 3, 2, 4, 2, few, width), jnp.float32),
                pltpu.VMEM((SLOTS, 2, 4, 2, few, width), jnp.float32),
                pltpu.VMEM((2, 4, 2, few, width), jnp.float32),
                dma((4,)), dma((Z_SEMS, 7)), dma((BLOCKS // 4,)), dma((CHUNKS,)),
                dma((3, 2, 2)), dma((2, 2)), dma((2, 2)), dma((3, 2)), dma((4, 2, 2)), dma((4, 2)), dma,
                dma((2 * SPLIT + C_SEMS, 3)), dma((BLOCKS // 4,)), dma((SLOTS,)),
            ],
            compiler_params=pltpu.CompilerParams(
                collective_id=0, has_side_effects=True, vmem_limit_bytes=61 * 1024 * 1024
            ),
        )(a_blk.reshape(2, 4, 2, few, cols), b_blk)
        return c_blk.reshape(rows, cols)

    block_spec = P(("row", "depth"), "col")
    return jax.shard_map(local_product, mesh=mesh, in_specs=(block_spec, block_spec), out_specs=block_spec, check_vma=False)
```

```python
import jax
import jax.numpy as jnp
from jax import lax
from jax.experimental import pallas as pl
from jax.experimental.pallas import tpu as pltpu
from jax.sharding import PartitionSpec as P

MESH = pl.DeviceIdType.MESH
X_N, Y_N, Z_N = 4, 4, 8
BLOCKS = 16
SLOTS = 8
LOOP = 8
WIDE = 14
SPLIT = 6
ALL = 2
Z_SEMS, C_SEMS = 5, 5

PROGRAM = (
    "aiaiaajfijbakjbiblkgcbknffjcdlnlohmamlcgmgoofeocmhnddkphbdnb",
    "egftceptoaoehptcopogntfdqfqnbduhaqqegucopotguuoqfheobaunrpth",
    "dvcavqovgueobnrdvpbsvchefsofracopgrqvdwwwbsgwrdwrasqhefrchws",
    "easpbpgsdfrbfcqehqascpgdrarbhqgdesfafbcpsehrgaqbcpdsbardgffh",
    "eqbccfhepscgpddrggdhqeheqehpspprqqqrsrrrssss",
)


def chunk(n):
    return (n, None) if n < WIDE else (WIDE + (n - WIDE) // 2, (n - WIDE) % 2)


CHUNKS = WIDE + 2 * (BLOCKS - WIDE)


def kernel(a_hbm, b_hbm, c_out, a_own, a_all, s1, rl1, rl2, b_all, crecv, c0, prod,
           ld_sem, zr_sem, zs_sem, dr_sem, s1_sem, r1_sem, r2_sem, s2_sem, ag_sem, fw_sem, as_sem,
           cr_sem, cs_sem, c0_sem):
    row, y, z = lax.axis_index("row"), lax.axis_index("col"), lax.axis_index("depth")
    x, c = row // 2, row % 2
    width = b_all.shape[3]
    narrow = width // 2
    cols = a_own.shape[4]
    part_cols = (pl.ds(0, cols // 2), pl.ds(cols // 2, cols // 2))
    rest = slice(None)

    def at_x(dx):
        return {"row": 2 * ((x + dx + X_N) % X_N) + c}

    def at_y(dy):
        return {"col": (y + dy + Y_N) % Y_N}

    step = 1 - 2 * c
    z_long = {"depth": (z + step + Z_N) % Z_N}
    z_short = {"depth": (z - step + Z_N) % Z_N}
    partner = {"row": 2 * x + 1 - c}

    def send(src, dst, ssem, rsem, dev):
        pltpu.make_async_remote_copy(src_ref=src, dst_ref=dst, send_sem=ssem, recv_sem=rsem,
                                     device_id=dev, device_id_type=MESH).start()

    def wait(ref, sem):
        pltpu.make_async_copy(ref, ref, sem).wait()

    e_own = (y - x + Y_N) % Y_N
    flip = e_own // 3
    j_own = e_own

    def b_local(m, sem):
        return pltpu.make_async_copy(b_hbm.at[:, pl.ds(pl.multiple_of(m * width, width), width)],
                                     b_all.at[m, c * Z_N + z], ld_sem.at[sem])

    def a_load(r):
        return pltpu.make_async_copy(a_hbm.at[:, :, r], a_own.at[:, :, r], ld_sem.at[2 + r])

    a_load(0).start()
    b_local(0, 0).start()
    a_load(1).start()
    barrier = pltpu.get_barrier_semaphore()
    for dev in (at_x(1), at_x(-1), at_y(1), at_y(-1), z_long, z_short, partner):
        pl.semaphore_signal(barrier, inc=1, device_id=dev, device_id_type=MESH)
    lax.fori_loop(1, BLOCKS, lambda m, _: (b_local(m, 1).start(), 0)[1], 0)

    def quarter_sem(e, o, r):
        return s1_sem.at[(e + 1) % 2 * (2 - e // 2), o, r]

    def by_e(e, o, r, j, part, fn):
        col_part = rest if part is None else part_cols[part]

        @pl.when(e == 0)
        def _():
            fn(a_all.at[3, o, j, r, :, col_part])

        @pl.when(e != 0)
        def _():
            fn(s1.at[(e + Y_N - 1) % Y_N, o, r, :, col_part])

    for o in range(2):
        for r in range(2):
            by_e(e_own, o, r, 0, None, lambda dst: pltpu.make_async_copy(
                a_hbm.at[(o + flip) % 2, 0, r], dst, quarter_sem(e_own, o, r)).start())
    pl.semaphore_wait(barrier, 7)
    loaded = set()

    def ev_s1(o, r):
        if r not in loaded:
            loaded.add(r)
            a_load(r).wait()
        h = (o + flip) % 2
        send(a_own.at[h, 2, r, :, part_cols[0]], rl1.at[0, o, r], as_sem, r1_sem.at[o, r], at_y(1))
        send(a_own.at[h, 2, r, :, part_cols[1]], rl1.at[1, o, r], as_sem, r1_sem.at[o, r], at_y(-1))
        sem = quarter_sem(e_own, o, r)
        by_e(e_own, o, r, 1, None, lambda dst: send(a_own.at[h, 1, r], dst, as_sem, sem, at_y(1)))
        by_e(e_own, o, r, 3, None, lambda dst: send(a_own.at[h, 3, r], dst, as_sem, sem, at_y(-1)))

    def ev_r1(o, r):
        wait(rl1.at[:, o, r], r1_sem.at[o, r])
        for d, dy in ((0, 1), (1, -1)):
            e = (y - dy - x + 2 * Y_N) % Y_N
            by_e(e, o, r, 2, d, lambda dst: send(rl1.at[d, o, r], dst, as_sem, quarter_sem(e, o, r), at_y(dy)))

    def ev_s2(o, r):
        wait(s1.at[pl.ds(0, 2), o, r], quarter_sem(1, o, r))
        g = 2 * o
        j = (y - x - 1 + 2 * Y_N) % Y_N
        send(s1.at[0, o, r], a_all.at[g, o, j, r], as_sem, s2_sem.at[g, r], at_x(1))
        j = (y - x + 1 + Y_N) % Y_N
        send(s1.at[2, o, r], a_all.at[g, 1 - o, j, r], as_sem, s2_sem.at[g, r], at_x(-1))

    def ev_s2f(o, r):
        wait(s1.at[1, o, r], quarter_sem(2, o, r))
        for d in range(2):
            send(s1.at[1, o, r, :, part_cols[d]], rl2.at[d, o, r], as_sem, r2_sem.at[o, r], at_x(1 - 2 * d))

    def ev_r2(o, r):
        wait(rl2.at[:, o, r], r2_sem.at[o, r])
        for d, dx in ((0, 1), (1, -1)):
            j = (y - x - dx + 2 * Y_N) % Y_N
            send(rl2.at[d, o, r], a_all.at[1, o, j, r, :, part_cols[d]], as_sem, s2_sem.at[1, r], at_x(dx))

    def ev_ag(g, r):
        if g == 3:
            for o in range(2):
                wait(a_all.at[g, o, j_own, r], quarter_sem(0, o, r))
        else:
            wait(a_all.at[g, :, j_own, r], s2_sem.at[g, r])
        for d in range(2):
            quarter = a_all.at[g, d, j_own, r]
            send(quarter, quarter, as_sem, ag_sem.at[g, d, r], at_y(1))
            send(quarter, quarter, as_sem, ag_sem.at[g, d, r], at_y(-1))

    def ev_fw(g, r, d):
        wait(a_all.at[0, 0, 0], ag_sem.at[g, d, r])
        for k, dy in ((0, 1), (1, -1)):
            j = (y - dy - x + 2 * Y_N) % Y_N
            part = a_all.at[g, d, j, r, :, part_cols[k]]
            send(part, part, as_sem, fw_sem.at[g, r], at_y(dy))

    def group_complete(g, r):
        wait(a_all.at[0, 0, 0], fw_sem.at[g, r])

    def block(hop):
        return c * Z_N + (z - hop * step + 2 * Z_N) % Z_N

    def lanes_of(n):
        half = chunk(n)[1]
        return rest if half is None else pl.ds(half * narrow, narrow)

    def piece(n, kb):
        return b_all.at[chunk(n)[0], kb, :, lanes_of(n)]

    def hand_over(n, kb):
        send(piece(n, kb), piece(n, kb), zs_sem.at[chunk(n)[0] // 4], dr_sem.at[n], partner)

    def forward_long(n, hop):
        p = piece(n, block(hop))
        send(p, p, zs_sem.at[chunk(n)[0] // 4], zr_sem.at[n % Z_SEMS, hop], z_long)

    def forward_short(n, hop):
        p = piece(n, block(-hop))
        send(p, p, zs_sem.at[chunk(n)[0] // 4], zr_sem.at[n % Z_SEMS, 4 + hop], z_short)

    def ev_own(n):
        if n == 0:
            b_local(0, 0).wait()
        elif n == 1:
            wait(b_all.at[0, pl.ds(0, BLOCKS - 1)], ld_sem.at[1])
        forward_long(n, 0)
        forward_short(n, 0)
        hand_over(n, block(0))

    def ev_long(n, hop):
        wait(piece(n, block(hop)), zr_sem.at[n % Z_SEMS, hop - 1])
        if hop < 4:
            forward_long(n, hop)
        hand_over(n, block(hop))

    def ev_short(n, hop):
        wait(piece(n, block(-hop)), zr_sem.at[n % Z_SEMS, 4 + hop - 1])
        if hop < 3:
            forward_short(n, hop)
        hand_over(n, block(-hop))

    def handed_over(n):
        wait(b_all.at[0, pl.ds(0, Z_N), :, lanes_of(n)], dr_sem.at[n])

    def dot(a, b):
        return jnp.dot(a.reshape(-1, cols), b.reshape(cols, -1), preferred_element_type=jnp.float32)

    def sum_sem(n, q):
        return 2 * SPLIT + (n - SPLIT) % C_SEMS if isinstance(q, slice) else 2 * n + q

    def sum_stage(n, g, q, m, lanes, first, size, when, reuse, old):
        slot = n % SLOTS
        keep = rest if isinstance(lanes, slice) else pl.ds(0, narrow)
        arrivals = sum_sem(n, q)

        def pass_on(src, ssem):
            for d in range(2):
                send(src.at[d], crecv.at[m, g, d, :, q, :, lanes], ssem, cr_sem.at[arrivals, g], at_x(1 - 2 * d))

        def arrived():
            wait(crecv.at[m, g - 1, :, :, q, :, lanes], cr_sem.at[arrivals, g - 1])

        def begin():
            reuse(lambda: wait(c0.at[slot, :, :, :, :, old], c0_sem.at[slot]))
            c0[slot, :, :, q, :, keep] = prod[:, :, q, :, keep]
            pass_on(c0.at[slot, :, :, q, :, keep], c0_sem.at[slot])

        def middle():
            arrived()
            crecv[m, g - 1, :, :, q, :, lanes] += prod[:, :, q, :, keep]
            pass_on(crecv.at[m, g - 1, :, :, q, :, lanes], cs_sem.at[m // 4])

        def end():
            arrived()
            total = crecv[m, g - 1, :, :, q, :, lanes] + prod[:, :, q, :, keep]
            c_out[:, :, q, :, pl.ds(pl.multiple_of(first, size), size)] = total.astype(c_out.dtype)

        a = a_all[g, :, :, q]
        prod[:, :, q, :, keep] = dot(a, b_all[m, :, :, lanes]).reshape(a.shape[:-1] + (size,))
        when(g == 0, begin)
        when((g == 1) | (g == 2), middle)
        when(g == 3, end)

    def branch(cond, fn):
        pl.when(cond)(fn)

    def fixed(cond, fn):
        if cond:
            fn()

    def sum_loop(code, split, wide):
        n, g, q = code // 8, code // 2 % 4, code % 2
        if split:
            pl.when(n < SPLIT)(lambda: sum_stage(n, g, q, n, rest, n * width, width, branch, lambda fn: None, rest))
        if wide:
            pl.when(n >= SPLIT)(lambda: sum_stage(n, g, rest, n, rest, n * width, width, branch,
                                                  pl.when(n >= SLOTS), rest))

    def sum_narrow(n, g):
        m, half = chunk(n)
        old = rest if n - SLOTS < WIDE else pl.ds(0, narrow)
        sum_stage(n, g, rest, m, lanes_of(n), m * width + half * narrow, narrow, fixed, lambda fn: fn(), old)

    chunks = range(CHUNKS)
    queues = {"a": [(ev_own, (n,)) for n in chunks]}
    for hop in range(1, 5):
        queues["abcde"[hop]] = [(ev_long, (n, hop)) for n in chunks]
    for hop in range(1, 4):
        queues["efgh"[hop]] = [(ev_short, (n, hop)) for n in chunks]
    by_half = [(o, r) for o in range(2) for r in range(2)]
    by_row = [(o, r) for r in range(2) for o in range(2)]
    queues["i"] = [(ev_s1, p) for p in by_row]
    queues["j"] = [(ev_r1, p) for p in by_row]
    queues["k"] = [(ev_s2, p) for p in by_row]
    queues["l"] = [(ev_s2f, p) for p in by_row]
    queues["m"] = [(ev_r2, p) for p in by_row]
    groups = [(g, r) for g in range(4) for r in range(2)]
    queues["n"] = [(ev_ag, p) for p in groups]
    queues["o"] = [(ev_fw, p + (d,)) for p in groups for d in range(2)]
    for g in range(4):
        queues["pqrs"[g]] = [(None, (n, g, 0 if n < SPLIT else ALL)) for n in chunks]
        queues["tuvw"[g]] = [(None, (n, g, 1)) for n in range(SPLIT)]

    steps, before, complete, handed = [], [], set(), set()
    for letter in "".join(PROGRAM):
        fn, args = queues[letter].pop(0)
        if fn is not None:
            before.append((fn, args))
            continue
        n, g, q = args
        for r in (range(2) if q == ALL else (q,)):
            if (g, r) not in complete:
                complete.add((g, r))
                before.append((group_complete, (g, r)))
        if n not in handed:
            handed.add(n)
            before.append((handed_over, (n,)))
        if n >= WIDE:
            before.append((sum_narrow, (n, g)))
        else:
            steps.append((before, (n * 4 + g) * 2 + q % 2, q != ALL))
            before = []

    def run(todo):
        for fn, args in todo:
            fn(*args)

    def in_loop(first, last):
        part = steps[first:last]

        def body(k, carry):
            code = part[0][1]
            for i, (todo, this, _) in enumerate(part):
                code = jnp.where(k == first + i, this, code)
                if todo:
                    pl.when(k == first + i)(lambda: run(todo))
            sum_loop(code, any(s for _, _, s in part), any(not s for _, _, s in part))
            return carry

        lax.fori_loop(first, last, body, 0)

    for first in range(0, len(steps), LOOP):
        in_loop(first, min(first + LOOP, len(steps)))
    run(before)

    for i in range(BLOCKS // 4):
        wait(b_all.at[pl.ds(0, 4), pl.ds(0, 15)], zs_sem.at[i])
        wait(crecv.at[pl.ds(0, 4), pl.ds(0, 2)], cs_sem.at[i])
    wait(b_all.at[pl.ds(0, 5)], as_sem)
    for n in range(CHUNKS - SLOTS, CHUNKS):
        keep = rest if n < WIDE else pl.ds(0, narrow)
        wait(c0.at[n % SLOTS, :, :, :, :, keep], c0_sem.at[n % SLOTS])


def solution(mesh):
    def local_product(a_blk, b_blk):
        rows, cols = a_blk.shape
        width = cols // BLOCKS
        few = rows // 16
        dma = pltpu.SemaphoreType.DMA
        c_blk = pl.pallas_call(
            kernel,
            name="matmul_3d",
            out_shape=pltpu.VMEM((2, 4, 2, few, cols), jnp.bfloat16),
            in_specs=[pl.BlockSpec(memory_space=pl.ANY)] * 2,
            out_specs=pl.BlockSpec(memory_space=pltpu.VMEM),
            scratch_shapes=[
                pltpu.VMEM((2, 4, 2, few, cols), jnp.bfloat16),
                pltpu.VMEM((4, 2, 4, 2, few, cols), jnp.bfloat16),
                pltpu.VMEM((3, 2, 2, few, cols), jnp.bfloat16),
                pltpu.VMEM((2, 2, 2, few, cols // 2), jnp.bfloat16),
                pltpu.VMEM((2, 2, 2, few, cols // 2), jnp.bfloat16),
                pltpu.VMEM((BLOCKS, 2 * Z_N, rows, width), jnp.bfloat16),
                pltpu.VMEM((BLOCKS, 3, 2, 4, 2, few, width), jnp.float32),
                pltpu.VMEM((SLOTS, 2, 4, 2, few, width), jnp.float32),
                pltpu.VMEM((2, 4, 2, few, width), jnp.float32),
                dma((4,)), dma((Z_SEMS, 7)), dma((BLOCKS // 4,)), dma((CHUNKS,)),
                dma((3, 2, 2)), dma((2, 2)), dma((2, 2)), dma((3, 2)), dma((4, 2, 2)), dma((4, 2)), dma,
                dma((2 * SPLIT + C_SEMS, 3)), dma((BLOCKS // 4,)), dma((SLOTS,)),
            ],
            compiler_params=pltpu.CompilerParams(
                collective_id=0, has_side_effects=True, vmem_limit_bytes=61 * 1024 * 1024
            ),
        )(a_blk.reshape(2, 4, 2, few, cols), b_blk)
        return c_blk.reshape(rows, cols)

    block_spec = P(("row", "depth"), "col")
    return jax.shard_map(local_product, mesh=mesh, in_specs=(block_spec, block_spec), out_specs=block_spec, check_vma=False)
```

```python
import jax
import jax.numpy as jnp
from jax import lax
from jax.experimental import pallas as pl
from jax.experimental.pallas import tpu as pltpu
from jax.sharding import PartitionSpec as P

MESH = pl.DeviceIdType.MESH
X_N, Y_N, Z_N = 4, 4, 8
BLOCKS = 16
SLOTS = 8
LOOP = 8
WIDE = 14
SPLIT = 6
ALL = 2
Z_SEMS, C_SEMS = 6, 5

PROGRAM = (
    "aiaiafbjfiajalgjkaikncjbbkgblmnchlmfclooddhcoodfmbnmgepdgetn",
    "kobehptcfehapoctotpondgfqfnqaqdquehbugptgououfqcoebohnuarpdt",
    "vcragohqeuobnvdpvbshafsroevfvoccpsqvbwgwwgfrdwdqawrwresharch",
    "espsfpbgsrdqbcafhgqesprdacrhbegffqsdbpshcarecgaqdbpdasbrhgef",
    "fcqefbhpcgsdgpcrdgqdhheehqeppsprqqqsrrrrssss",
)


def chunk(n):
    return (n, None) if n < WIDE else (WIDE + (n - WIDE) // 2, (n - WIDE) % 2)


CHUNKS = WIDE + 2 * (BLOCKS - WIDE)


def kernel(a_hbm, b_hbm, c_out, a_own, a_all, s1, rl1, rl2, b_all, crecv, c0, prod,
           ld_sem, zr_sem, zs_sem, dr_sem, s1_sem, r1_sem, r2_sem, s2_sem, ag_sem, fw_sem, as_sem,
           cr_sem, cs_sem, c0_sem):
    row, y, z = lax.axis_index("row"), lax.axis_index("col"), lax.axis_index("depth")
    x, c = row // 2, row % 2
    width = b_all.shape[3]
    narrow = width // 2
    cols = a_own.shape[4]
    part_cols = (pl.ds(0, cols // 2), pl.ds(cols // 2, cols // 2))
    rest = slice(None)

    def at_x(dx):
        return {"row": 2 * ((x + dx + X_N) % X_N) + c}

    def at_y(dy):
        return {"col": (y + dy + Y_N) % Y_N}

    step = 1 - 2 * c
    z_long = {"depth": (z + step + Z_N) % Z_N}
    z_short = {"depth": (z - step + Z_N) % Z_N}
    partner = {"row": 2 * x + 1 - c}

    def send(src, dst, ssem, rsem, dev):
        pltpu.make_async_remote_copy(src_ref=src, dst_ref=dst, send_sem=ssem, recv_sem=rsem,
                                     device_id=dev, device_id_type=MESH).start()

    def wait(ref, sem):
        pltpu.make_async_copy(ref, ref, sem).wait()

    e_own = (y - x + Y_N) % Y_N
    flip = e_own // 3
    j_own = e_own

    def b_local(m, sem):
        return pltpu.make_async_copy(b_hbm.at[:, pl.ds(pl.multiple_of(m * width, width), width)],
                                     b_all.at[m, c * Z_N + z], ld_sem.at[sem])

    def a_load(r):
        return pltpu.make_async_copy(a_hbm.at[:, :, r], a_own.at[:, :, r], ld_sem.at[2 + r])

    a_load(0).start()
    b_local(0, 0).start()
    a_load(1).start()
    barrier = pltpu.get_barrier_semaphore()
    for dev in (at_x(1), at_x(-1), at_y(1), at_y(-1), z_long, z_short, partner):
        pl.semaphore_signal(barrier, inc=1, device_id=dev, device_id_type=MESH)
    lax.fori_loop(1, BLOCKS, lambda m, _: (b_local(m, 1).start(), 0)[1], 0)

    def quarter_sem(e, o, r):
        return s1_sem.at[(e + 1) % 2 * (2 - e // 2), o, r]

    def by_e(e, o, r, j, part, fn):
        col_part = rest if part is None else part_cols[part]

        @pl.when(e == 0)
        def _():
            fn(a_all.at[3, o, j, r, :, col_part])

        @pl.when(e != 0)
        def _():
            fn(s1.at[(e + Y_N - 1) % Y_N, o, r, :, col_part])

    for o in range(2):
        for r in range(2):
            by_e(e_own, o, r, 0, None, lambda dst: pltpu.make_async_copy(
                a_hbm.at[(o + flip) % 2, 0, r], dst, quarter_sem(e_own, o, r)).start())
    pl.semaphore_wait(barrier, 7)
    loaded = set()

    def ev_s1(o, r):
        if r not in loaded:
            loaded.add(r)
            a_load(r).wait()
        h = (o + flip) % 2
        send(a_own.at[h, 2, r, :, part_cols[0]], rl1.at[0, o, r], as_sem, r1_sem.at[o, r], at_y(1))
        send(a_own.at[h, 2, r, :, part_cols[1]], rl1.at[1, o, r], as_sem, r1_sem.at[o, r], at_y(-1))
        sem = quarter_sem(e_own, o, r)
        by_e(e_own, o, r, 1, None, lambda dst: send(a_own.at[h, 1, r], dst, as_sem, sem, at_y(1)))
        by_e(e_own, o, r, 3, None, lambda dst: send(a_own.at[h, 3, r], dst, as_sem, sem, at_y(-1)))

    def ev_r1(o, r):
        wait(rl1.at[:, o, r], r1_sem.at[o, r])
        for d, dy in ((0, 1), (1, -1)):
            e = (y - dy - x + 2 * Y_N) % Y_N
            by_e(e, o, r, 2, d, lambda dst: send(rl1.at[d, o, r], dst, as_sem, quarter_sem(e, o, r), at_y(dy)))

    def ev_s2(o, r):
        wait(s1.at[pl.ds(0, 2), o, r], quarter_sem(1, o, r))
        g = 2 * o
        j = (y - x - 1 + 2 * Y_N) % Y_N
        send(s1.at[0, o, r], a_all.at[g, o, j, r], as_sem, s2_sem.at[g, r], at_x(1))
        j = (y - x + 1 + Y_N) % Y_N
        send(s1.at[2, o, r], a_all.at[g, 1 - o, j, r], as_sem, s2_sem.at[g, r], at_x(-1))

    def ev_s2f(o, r):
        wait(s1.at[1, o, r], quarter_sem(2, o, r))
        for d in range(2):
            send(s1.at[1, o, r, :, part_cols[d]], rl2.at[d, o, r], as_sem, r2_sem.at[o, r], at_x(1 - 2 * d))

    def ev_r2(o, r):
        wait(rl2.at[:, o, r], r2_sem.at[o, r])
        for d, dx in ((0, 1), (1, -1)):
            j = (y - x - dx + 2 * Y_N) % Y_N
            send(rl2.at[d, o, r], a_all.at[1, o, j, r, :, part_cols[d]], as_sem, s2_sem.at[1, r], at_x(dx))

    def ev_ag(g, r):
        if g == 3:
            for o in range(2):
                wait(a_all.at[g, o, j_own, r], quarter_sem(0, o, r))
        else:
            wait(a_all.at[g, :, j_own, r], s2_sem.at[g, r])
        for d in range(2):
            quarter = a_all.at[g, d, j_own, r]
            send(quarter, quarter, as_sem, ag_sem.at[g, d, r], at_y(1))
            send(quarter, quarter, as_sem, ag_sem.at[g, d, r], at_y(-1))

    def ev_fw(g, r, d):
        wait(a_all.at[0, 0, 0], ag_sem.at[g, d, r])
        for k, dy in ((0, 1), (1, -1)):
            j = (y - dy - x + 2 * Y_N) % Y_N
            part = a_all.at[g, d, j, r, :, part_cols[k]]
            send(part, part, as_sem, fw_sem.at[g, r], at_y(dy))

    def group_complete(g, r):
        wait(a_all.at[0, 0, 0], fw_sem.at[g, r])

    def block(hop):
        return c * Z_N + (z - hop * step + 2 * Z_N) % Z_N

    def lanes_of(n):
        half = chunk(n)[1]
        return rest if half is None else pl.ds(half * narrow, narrow)

    def piece(n, kb):
        return b_all.at[chunk(n)[0], kb, :, lanes_of(n)]

    def hand_over(n, kb):
        send(piece(n, kb), piece(n, kb), zs_sem.at[chunk(n)[0] // 4], dr_sem.at[n], partner)

    def forward_long(n, hop):
        p = piece(n, block(hop))
        send(p, p, zs_sem.at[chunk(n)[0] // 4], zr_sem.at[n % Z_SEMS, hop], z_long)

    def forward_short(n, hop):
        p = piece(n, block(-hop))
        send(p, p, zs_sem.at[chunk(n)[0] // 4], zr_sem.at[n % Z_SEMS, 4 + hop], z_short)

    def ev_own(n):
        if n == 0:
            b_local(0, 0).wait()
        elif n == 1:
            wait(b_all.at[0, pl.ds(0, BLOCKS - 1)], ld_sem.at[1])
        forward_long(n, 0)
        forward_short(n, 0)
        hand_over(n, block(0))

    def ev_long(n, hop):
        wait(piece(n, block(hop)), zr_sem.at[n % Z_SEMS, hop - 1])
        if hop < 4:
            forward_long(n, hop)
        hand_over(n, block(hop))

    def ev_short(n, hop):
        wait(piece(n, block(-hop)), zr_sem.at[n % Z_SEMS, 4 + hop - 1])
        if hop < 3:
            forward_short(n, hop)
        hand_over(n, block(-hop))

    def handed_over(n):
        wait(b_all.at[0, pl.ds(0, Z_N), :, lanes_of(n)], dr_sem.at[n])

    def dot(a, b):
        return jnp.dot(a.reshape(-1, cols), b.reshape(cols, -1), preferred_element_type=jnp.float32)

    def sum_sem(n, q):
        return 2 * SPLIT + (n - SPLIT) % C_SEMS if isinstance(q, slice) else 2 * n + q

    def sum_stage(n, g, q, m, lanes, first, size, when, reuse, old):
        slot = n % SLOTS
        keep = rest if isinstance(lanes, slice) else pl.ds(0, narrow)
        arrivals = sum_sem(n, q)

        def pass_on(src, ssem):
            for d in range(2):
                send(src.at[d], crecv.at[m, g, d, :, q, :, lanes], ssem, cr_sem.at[arrivals, g], at_x(1 - 2 * d))

        def arrived():
            wait(crecv.at[m, g - 1, :, :, q, :, lanes], cr_sem.at[arrivals, g - 1])

        def begin():
            reuse(lambda: wait(c0.at[slot, :, :, :, :, old], c0_sem.at[slot]))
            c0[slot, :, :, q, :, keep] = prod[:, :, q, :, keep]
            pass_on(c0.at[slot, :, :, q, :, keep], c0_sem.at[slot])

        def middle():
            arrived()
            crecv[m, g - 1, :, :, q, :, lanes] += prod[:, :, q, :, keep]
            pass_on(crecv.at[m, g - 1, :, :, q, :, lanes], cs_sem.at[m // 4])

        def end():
            arrived()
            total = crecv[m, g - 1, :, :, q, :, lanes] + prod[:, :, q, :, keep]
            c_out[:, :, q, :, pl.ds(pl.multiple_of(first, size), size)] = total.astype(c_out.dtype)

        a = a_all[g, :, :, q]
        prod[:, :, q, :, keep] = dot(a, b_all[m, :, :, lanes]).reshape(a.shape[:-1] + (size,))
        when(g == 0, begin)
        when((g == 1) | (g == 2), middle)
        when(g == 3, end)

    def branch(cond, fn):
        pl.when(cond)(fn)

    def fixed(cond, fn):
        if cond:
            fn()

    def sum_loop(code, split, wide):
        n, g, q = code // 8, code // 2 % 4, code % 2
        if split:
            pl.when(n < SPLIT)(lambda: sum_stage(n, g, q, n, rest, n * width, width, branch, lambda fn: None, rest))
        if wide:
            pl.when(n >= SPLIT)(lambda: sum_stage(n, g, rest, n, rest, n * width, width, branch,
                                                  pl.when(n >= SLOTS), rest))

    def sum_narrow(n, g):
        m, half = chunk(n)
        old = rest if n - SLOTS < WIDE else pl.ds(0, narrow)
        sum_stage(n, g, rest, m, lanes_of(n), m * width + half * narrow, narrow, fixed, lambda fn: fn(), old)

    chunks = range(CHUNKS)
    queues = {"a": [(ev_own, (n,)) for n in chunks]}
    for hop in range(1, 5):
        queues["abcde"[hop]] = [(ev_long, (n, hop)) for n in chunks]
    for hop in range(1, 4):
        queues["efgh"[hop]] = [(ev_short, (n, hop)) for n in chunks]
    by_half = [(o, r) for o in range(2) for r in range(2)]
    by_row = [(o, r) for r in range(2) for o in range(2)]
    queues["i"] = [(ev_s1, p) for p in by_row]
    queues["j"] = [(ev_r1, p) for p in by_row]
    queues["k"] = [(ev_s2, p) for p in by_row]
    queues["l"] = [(ev_s2f, p) for p in by_row]
    queues["m"] = [(ev_r2, p) for p in by_row]
    groups = [(g, r) for g in range(4) for r in range(2)]
    queues["n"] = [(ev_ag, p) for p in groups]
    queues["o"] = [(ev_fw, p + (d,)) for p in groups for d in range(2)]
    for g in range(4):
        queues["pqrs"[g]] = [(None, (n, g, 0 if n < SPLIT else ALL)) for n in chunks]
        queues["tuvw"[g]] = [(None, (n, g, 1)) for n in range(SPLIT)]

    steps, before, complete, handed = [], [], set(), set()
    for letter in "".join(PROGRAM):
        fn, args = queues[letter].pop(0)
        if fn is not None:
            before.append((fn, args))
            continue
        n, g, q = args
        for r in (range(2) if q == ALL else (q,)):
            if (g, r) not in complete:
                complete.add((g, r))
                before.append((group_complete, (g, r)))
        if n not in handed:
            handed.add(n)
            before.append((handed_over, (n,)))
        if n >= WIDE:
            before.append((sum_narrow, (n, g)))
        else:
            steps.append((before, (n * 4 + g) * 2 + q % 2, q != ALL))
            before = []

    def run(todo):
        for fn, args in todo:
            fn(*args)

    def in_loop(first, last):
        part = steps[first:last]

        def body(k, carry):
            code = part[0][1]
            for i, (todo, this, _) in enumerate(part):
                code = jnp.where(k == first + i, this, code)
                if todo:
                    pl.when(k == first + i)(lambda: run(todo))
            sum_loop(code, any(s for _, _, s in part), any(not s for _, _, s in part))
            return carry

        lax.fori_loop(first, last, body, 0)

    for first in range(0, len(steps), LOOP):
        in_loop(first, min(first + LOOP, len(steps)))
    run(before)

    for i in range(BLOCKS // 4):
        wait(b_all.at[pl.ds(0, 4), pl.ds(0, 15)], zs_sem.at[i])
        wait(crecv.at[pl.ds(0, 4), pl.ds(0, 2)], cs_sem.at[i])
    wait(b_all.at[pl.ds(0, 5)], as_sem)
    for n in range(CHUNKS - SLOTS, CHUNKS):
        keep = rest if n < WIDE else pl.ds(0, narrow)
        wait(c0.at[n % SLOTS, :, :, :, :, keep], c0_sem.at[n % SLOTS])


def solution(mesh):
    def local_product(a_blk, b_blk):
        rows, cols = a_blk.shape
        width = cols // BLOCKS
        few = rows // 16
        dma = pltpu.SemaphoreType.DMA
        c_blk = pl.pallas_call(
            kernel,
            name="matmul_3d",
            out_shape=pltpu.VMEM((2, 4, 2, few, cols), jnp.bfloat16),
            in_specs=[pl.BlockSpec(memory_space=pl.ANY)] * 2,
            out_specs=pl.BlockSpec(memory_space=pltpu.VMEM),
            scratch_shapes=[
                pltpu.VMEM((2, 4, 2, few, cols), jnp.bfloat16),
                pltpu.VMEM((4, 2, 4, 2, few, cols), jnp.bfloat16),
                pltpu.VMEM((3, 2, 2, few, cols), jnp.bfloat16),
                pltpu.VMEM((2, 2, 2, few, cols // 2), jnp.bfloat16),
                pltpu.VMEM((2, 2, 2, few, cols // 2), jnp.bfloat16),
                pltpu.VMEM((BLOCKS, 2 * Z_N, rows, width), jnp.bfloat16),
                pltpu.VMEM((BLOCKS, 3, 2, 4, 2, few, width), jnp.float32),
                pltpu.VMEM((SLOTS, 2, 4, 2, few, width), jnp.float32),
                pltpu.VMEM((2, 4, 2, few, width), jnp.float32),
                dma((4,)), dma((Z_SEMS, 7)), dma((BLOCKS // 4,)), dma((CHUNKS,)),
                dma((3, 2, 2)), dma((2, 2)), dma((2, 2)), dma((3, 2)), dma((4, 2, 2)), dma((4, 2)), dma,
                dma((2 * SPLIT + C_SEMS, 3)), dma((BLOCKS // 4,)), dma((SLOTS,)),
            ],
            compiler_params=pltpu.CompilerParams(
                collective_id=0, has_side_effects=True, vmem_limit_bytes=61 * 1024 * 1024
            ),
        )(a_blk.reshape(2, 4, 2, few, cols), b_blk)
        return c_blk.reshape(rows, cols)

    block_spec = P(("row", "depth"), "col")
    return jax.shard_map(local_product, mesh=mesh, in_specs=(block_spec, block_spec), out_specs=block_spec, check_vma=False)
```

```python
import jax
import jax.numpy as jnp
from jax import lax
from jax.experimental import pallas as pl
from jax.experimental.pallas import tpu as pltpu
from jax.sharding import PartitionSpec as P

MESH = pl.DeviceIdType.MESH
X_N, Y_N, Z_N = 4, 4, 8
BLOCKS = 16
SLOTS = 8
LOOP = 8
WIDE = 15
SPLIT = 6
ALL = 2
Z_SEMS, C_SEMS = 5, 3

PROGRAM = (
    "aiaiafjafiabjbkjiknbbjckllgclbnfdmmocofdcgnldgkmchhgemoefdoa",
    "hpeophonpdttgeqnbqoapehtoftcapqqbootnndqgfuufcueubhurgdptaro",
    "carooehorngpufqvbdsssoaqcshbvegaovrrpwwwdscfrsbvefhbqfgdspwv",
    "craqehwgdvacpshrebgwqbdpfsccrhgeaqdpdshfrbeqagapfsbrhcebqfcg",
    "pdcsdfrhgeqdgehpehprspqqsqrrrsss",
)


def chunk(n):
    return (n, None) if n < WIDE else (WIDE + (n - WIDE) // 2, (n - WIDE) % 2)


CHUNKS = WIDE + 2 * (BLOCKS - WIDE)


def kernel(a_hbm, b_hbm, c_out, a_own, a_all, s1, rl1, rl2, b_all, crecv, c0, prod,
           ld_sem, zr_sem, zs_sem, dr_sem, s1_sem, r1_sem, r2_sem, s2_sem, ag_sem, fw_sem, as_sem,
           cr_sem, cs_sem, c0_sem):
    row, y, z = lax.axis_index("row"), lax.axis_index("col"), lax.axis_index("depth")
    x, c = row // 2, row % 2
    width = b_all.shape[3]
    narrow = width // 2
    cols = a_own.shape[4]
    part_cols = (pl.ds(0, cols // 2), pl.ds(cols // 2, cols // 2))
    rest = slice(None)

    def at_x(dx):
        return {"row": 2 * ((x + dx + X_N) % X_N) + c}

    def at_y(dy):
        return {"col": (y + dy + Y_N) % Y_N}

    step = 1 - 2 * c
    z_long = {"depth": (z + step + Z_N) % Z_N}
    z_short = {"depth": (z - step + Z_N) % Z_N}
    partner = {"row": 2 * x + 1 - c}

    def send(src, dst, ssem, rsem, dev):
        pltpu.make_async_remote_copy(src_ref=src, dst_ref=dst, send_sem=ssem, recv_sem=rsem,
                                     device_id=dev, device_id_type=MESH).start()

    def wait(ref, sem):
        pltpu.make_async_copy(ref, ref, sem).wait()

    e_own = (y - x + Y_N) % Y_N
    flip = e_own // 3
    j_own = e_own

    def b_local(m, sem):
        return pltpu.make_async_copy(b_hbm.at[:, pl.ds(pl.multiple_of(m * width, width), width)],
                                     b_all.at[m, c * Z_N + z], ld_sem.at[sem])

    def a_load(r):
        return pltpu.make_async_copy(a_hbm.at[:, :, r], a_own.at[:, :, r], ld_sem.at[2 + r])

    a_load(0).start()
    b_local(0, 0).start()
    a_load(1).start()
    barrier = pltpu.get_barrier_semaphore()
    for dev in (at_x(1), at_x(-1), at_y(1), at_y(-1), z_long, z_short, partner):
        pl.semaphore_signal(barrier, inc=1, device_id=dev, device_id_type=MESH)
    lax.fori_loop(1, BLOCKS, lambda m, _: (b_local(m, 1).start(), 0)[1], 0)

    def quarter_sem(e, o, r):
        return s1_sem.at[(e + 1) % 2 * (2 - e // 2), o, r]

    def by_e(e, o, r, j, part, fn):
        col_part = rest if part is None else part_cols[part]

        @pl.when(e == 0)
        def _():
            fn(a_all.at[3, o, j, r, :, col_part])

        @pl.when(e != 0)
        def _():
            fn(s1.at[(e + Y_N - 1) % Y_N, o, r, :, col_part])

    for o in range(2):
        for r in range(2):
            by_e(e_own, o, r, 0, None, lambda dst: pltpu.make_async_copy(
                a_hbm.at[(o + flip) % 2, 0, r], dst, quarter_sem(e_own, o, r)).start())
    pl.semaphore_wait(barrier, 7)
    loaded = set()

    def ev_s1(o, r):
        if r not in loaded:
            loaded.add(r)
            a_load(r).wait()
        h = (o + flip) % 2
        send(a_own.at[h, 2, r, :, part_cols[0]], rl1.at[0, o, r], as_sem, r1_sem.at[o, r], at_y(1))
        send(a_own.at[h, 2, r, :, part_cols[1]], rl1.at[1, o, r], as_sem, r1_sem.at[o, r], at_y(-1))
        sem = quarter_sem(e_own, o, r)
        by_e(e_own, o, r, 1, None, lambda dst: send(a_own.at[h, 1, r], dst, as_sem, sem, at_y(1)))
        by_e(e_own, o, r, 3, None, lambda dst: send(a_own.at[h, 3, r], dst, as_sem, sem, at_y(-1)))

    def ev_r1(o, r):
        wait(rl1.at[:, o, r], r1_sem.at[o, r])
        for d, dy in ((0, 1), (1, -1)):
            e = (y - dy - x + 2 * Y_N) % Y_N
            by_e(e, o, r, 2, d, lambda dst: send(rl1.at[d, o, r], dst, as_sem, quarter_sem(e, o, r), at_y(dy)))

    def ev_s2(o, r):
        wait(s1.at[pl.ds(0, 2), o, r], quarter_sem(1, o, r))
        g = 2 * o
        j = (y - x - 1 + 2 * Y_N) % Y_N
        send(s1.at[0, o, r], a_all.at[g, o, j, r], as_sem, s2_sem.at[g, r], at_x(1))
        j = (y - x + 1 + Y_N) % Y_N
        send(s1.at[2, o, r], a_all.at[g, 1 - o, j, r], as_sem, s2_sem.at[g, r], at_x(-1))

    def ev_s2f(o, r):
        wait(s1.at[1, o, r], quarter_sem(2, o, r))
        for d in range(2):
            send(s1.at[1, o, r, :, part_cols[d]], rl2.at[d, o, r], as_sem, r2_sem.at[o, r], at_x(1 - 2 * d))

    def ev_r2(o, r):
        wait(rl2.at[:, o, r], r2_sem.at[o, r])
        for d, dx in ((0, 1), (1, -1)):
            j = (y - x - dx + 2 * Y_N) % Y_N
            send(rl2.at[d, o, r], a_all.at[1, o, j, r, :, part_cols[d]], as_sem, s2_sem.at[1, r], at_x(dx))

    def ev_ag(g, r):
        if g == 3:
            for o in range(2):
                wait(a_all.at[g, o, j_own, r], quarter_sem(0, o, r))
        else:
            wait(a_all.at[g, :, j_own, r], s2_sem.at[g, r])
        for d in range(2):
            quarter = a_all.at[g, d, j_own, r]
            send(quarter, quarter, as_sem, ag_sem.at[g, d, r], at_y(1))
            send(quarter, quarter, as_sem, ag_sem.at[g, d, r], at_y(-1))

    def ev_fw(g, r, d):
        wait(a_all.at[0, 0, 0], ag_sem.at[g, d, r])
        for k, dy in ((0, 1), (1, -1)):
            j = (y - dy - x + 2 * Y_N) % Y_N
            part = a_all.at[g, d, j, r, :, part_cols[k]]
            send(part, part, as_sem, fw_sem.at[g, r], at_y(dy))

    def group_complete(g, r):
        wait(a_all.at[0, 0, 0], fw_sem.at[g, r])

    def block(hop):
        return c * Z_N + (z - hop * step + 2 * Z_N) % Z_N

    def lanes_of(n):
        half = chunk(n)[1]
        return rest if half is None else pl.ds(half * narrow, narrow)

    def piece(n, kb):
        return b_all.at[chunk(n)[0], kb, :, lanes_of(n)]

    def hand_over(n, kb):
        send(piece(n, kb), piece(n, kb), zs_sem.at[chunk(n)[0] // 4], dr_sem.at[n], partner)

    def forward_long(n, hop):
        p = piece(n, block(hop))
        send(p, p, zs_sem.at[chunk(n)[0] // 4], zr_sem.at[n % Z_SEMS, hop], z_long)

    def forward_short(n, hop):
        p = piece(n, block(-hop))
        send(p, p, zs_sem.at[chunk(n)[0] // 4], zr_sem.at[n % Z_SEMS, 4 + hop], z_short)

    def ev_own(n):
        if n == 0:
            b_local(0, 0).wait()
        elif n == 1:
            wait(b_all.at[0, pl.ds(0, BLOCKS - 1)], ld_sem.at[1])
        forward_long(n, 0)
        forward_short(n, 0)
        hand_over(n, block(0))

    def ev_long(n, hop):
        wait(piece(n, block(hop)), zr_sem.at[n % Z_SEMS, hop - 1])
        if hop < 4:
            forward_long(n, hop)
        hand_over(n, block(hop))

    def ev_short(n, hop):
        wait(piece(n, block(-hop)), zr_sem.at[n % Z_SEMS, 4 + hop - 1])
        if hop < 3:
            forward_short(n, hop)
        hand_over(n, block(-hop))

    def handed_over(n):
        wait(b_all.at[0, pl.ds(0, Z_N), :, lanes_of(n)], dr_sem.at[n])

    def dot(a, b):
        return jnp.dot(a.reshape(-1, cols), b.reshape(cols, -1), preferred_element_type=jnp.float32)

    def sum_sem(n, q):
        return 2 * SPLIT + (n - SPLIT) % C_SEMS if isinstance(q, slice) else 2 * n + q

    def sum_stage(n, g, q, m, lanes, first, size, when, reuse, old):
        slot = n % SLOTS
        keep = rest if isinstance(lanes, slice) else pl.ds(0, narrow)
        arrivals = sum_sem(n, q)

        def pass_on(src, ssem):
            for d in range(2):
                send(src.at[d], crecv.at[m, g, d, :, q, :, lanes], ssem, cr_sem.at[arrivals, g], at_x(1 - 2 * d))

        def arrived():
            wait(crecv.at[m, g - 1, :, :, q, :, lanes], cr_sem.at[arrivals, g - 1])

        def begin():
            reuse(lambda: wait(c0.at[slot, :, :, :, :, old], c0_sem.at[slot]))
            c0[slot, :, :, q, :, keep] = prod[:, :, q, :, keep]
            pass_on(c0.at[slot, :, :, q, :, keep], c0_sem.at[slot])

        def middle():
            arrived()
            crecv[m, g - 1, :, :, q, :, lanes] += prod[:, :, q, :, keep]
            pass_on(crecv.at[m, g - 1, :, :, q, :, lanes], cs_sem.at[m // 4])

        def end():
            arrived()
            total = crecv[m, g - 1, :, :, q, :, lanes] + prod[:, :, q, :, keep]
            c_out[:, :, q, :, pl.ds(pl.multiple_of(first, size), size)] = total.astype(c_out.dtype)

        a = a_all[g, :, :, q]
        prod[:, :, q, :, keep] = dot(a, b_all[m, :, :, lanes]).reshape(a.shape[:-1] + (size,))
        when(g == 0, begin)
        when((g == 1) | (g == 2), middle)
        when(g == 3, end)

    def branch(cond, fn):
        pl.when(cond)(fn)

    def fixed(cond, fn):
        if cond:
            fn()

    def sum_loop(code, split, wide):
        n, g, q = code // 8, code // 2 % 4, code % 2
        if split:
            pl.when(n < SPLIT)(lambda: sum_stage(n, g, q, n, rest, n * width, width, branch, lambda fn: None, rest))
        if wide:
            pl.when(n >= SPLIT)(lambda: sum_stage(n, g, rest, n, rest, n * width, width, branch,
                                                  pl.when(n >= SLOTS), rest))

    def sum_narrow(n, g):
        m, half = chunk(n)
        old = rest if n - SLOTS < WIDE else pl.ds(0, narrow)
        sum_stage(n, g, rest, m, lanes_of(n), m * width + half * narrow, narrow, fixed, lambda fn: fn(), old)

    chunks = range(CHUNKS)
    queues = {"a": [(ev_own, (n,)) for n in chunks]}
    for hop in range(1, 5):
        queues["abcde"[hop]] = [(ev_long, (n, hop)) for n in chunks]
    for hop in range(1, 4):
        queues["efgh"[hop]] = [(ev_short, (n, hop)) for n in chunks]
    by_half = [(o, r) for o in range(2) for r in range(2)]
    by_row = [(o, r) for r in range(2) for o in range(2)]
    queues["i"] = [(ev_s1, p) for p in by_row]
    queues["j"] = [(ev_r1, p) for p in by_row]
    queues["k"] = [(ev_s2, p) for p in by_row]
    queues["l"] = [(ev_s2f, p) for p in by_row]
    queues["m"] = [(ev_r2, p) for p in by_row]
    groups = [(g, r) for g in range(4) for r in range(2)]
    queues["n"] = [(ev_ag, p) for p in groups]
    queues["o"] = [(ev_fw, p + (d,)) for p in groups for d in range(2)]
    for g in range(4):
        queues["pqrs"[g]] = [(None, (n, g, 0 if n < SPLIT else ALL)) for n in chunks]
        queues["tuvw"[g]] = [(None, (n, g, 1)) for n in range(SPLIT)]

    steps, before, complete, handed = [], [], set(), set()
    for letter in "".join(PROGRAM):
        fn, args = queues[letter].pop(0)
        if fn is not None:
            before.append((fn, args))
            continue
        n, g, q = args
        for r in (range(2) if q == ALL else (q,)):
            if (g, r) not in complete:
                complete.add((g, r))
                before.append((group_complete, (g, r)))
        if n not in handed:
            handed.add(n)
            before.append((handed_over, (n,)))
        if n >= WIDE:
            before.append((sum_narrow, (n, g)))
        else:
            steps.append((before, (n * 4 + g) * 2 + q % 2, q != ALL))
            before = []

    def run(todo):
        for fn, args in todo:
            fn(*args)

    def in_loop(first, last):
        part = steps[first:last]

        def body(k, carry):
            code = part[0][1]
            for i, (todo, this, _) in enumerate(part):
                code = jnp.where(k == first + i, this, code)
                if todo:
                    pl.when(k == first + i)(lambda: run(todo))
            sum_loop(code, any(s for _, _, s in part), any(not s for _, _, s in part))
            return carry

        lax.fori_loop(first, last, body, 0)

    for first in range(0, len(steps), LOOP):
        in_loop(first, min(first + LOOP, len(steps)))
    run(before)

    for i in range(BLOCKS // 4):
        wait(b_all.at[pl.ds(0, 4), pl.ds(0, 15)], zs_sem.at[i])
        wait(crecv.at[pl.ds(0, 4), pl.ds(0, 2)], cs_sem.at[i])
    wait(b_all.at[pl.ds(0, 5)], as_sem)
    for n in range(CHUNKS - SLOTS, CHUNKS):
        keep = rest if n < WIDE else pl.ds(0, narrow)
        wait(c0.at[n % SLOTS, :, :, :, :, keep], c0_sem.at[n % SLOTS])


def solution(mesh):
    def local_product(a_blk, b_blk):
        rows, cols = a_blk.shape
        width = cols // BLOCKS
        few = rows // 16
        dma = pltpu.SemaphoreType.DMA
        c_blk = pl.pallas_call(
            kernel,
            name="matmul_3d",
            out_shape=pltpu.VMEM((2, 4, 2, few, cols), jnp.bfloat16),
            in_specs=[pl.BlockSpec(memory_space=pl.ANY)] * 2,
            out_specs=pl.BlockSpec(memory_space=pltpu.VMEM),
            scratch_shapes=[
                pltpu.VMEM((2, 4, 2, few, cols), jnp.bfloat16),
                pltpu.VMEM((4, 2, 4, 2, few, cols), jnp.bfloat16),
                pltpu.VMEM((3, 2, 2, few, cols), jnp.bfloat16),
                pltpu.VMEM((2, 2, 2, few, cols // 2), jnp.bfloat16),
                pltpu.VMEM((2, 2, 2, few, cols // 2), jnp.bfloat16),
                pltpu.VMEM((BLOCKS, 2 * Z_N, rows, width), jnp.bfloat16),
                pltpu.VMEM((BLOCKS, 3, 2, 4, 2, few, width), jnp.float32),
                pltpu.VMEM((SLOTS, 2, 4, 2, few, width), jnp.float32),
                pltpu.VMEM((2, 4, 2, few, width), jnp.float32),
                dma((4,)), dma((Z_SEMS, 7)), dma((BLOCKS // 4,)), dma((CHUNKS,)),
                dma((3, 2, 2)), dma((2, 2)), dma((2, 2)), dma((3, 2)), dma((4, 2, 2)), dma((4, 2)), dma,
                dma((2 * SPLIT + C_SEMS, 3)), dma((BLOCKS // 4,)), dma((SLOTS,)),
            ],
            compiler_params=pltpu.CompilerParams(
                collective_id=0, has_side_effects=True, vmem_limit_bytes=61 * 1024 * 1024
            ),
        )(a_blk.reshape(2, 4, 2, few, cols), b_blk)
        return c_blk.reshape(rows, cols)

    block_spec = P(("row", "depth"), "col")
    return jax.shard_map(local_product, mesh=mesh, in_specs=(block_spec, block_spec), out_specs=block_spec, check_vma=False)
```

```python
import jax
import jax.numpy as jnp
from jax import lax
from jax.experimental import pallas as pl
from jax.experimental.pallas import tpu as pltpu
from jax.sharding import PartitionSpec as P

MESH = pl.DeviceIdType.MESH
X_N, Y_N, Z_N = 4, 4, 8
BLOCKS = 16
SLOTS = 8
LOOP = 8
WIDE = 15
SPLIT = 4
ALL = 2
Z_SEMS, C_SEMS = 4, 3

PROGRAM = (
    "aiaaijbfbijfbjkfgcialgcnjckldbmndhohaomlldckmeoefbmgoendpfng",
    "apthotgpkcotheabotopdfnqbqcuhfauneucqopdgqoagobuqonherdranbp",
    "orfhfcvvoebqcrpodgvgofrarssssdhwweqwvcaepbhgssdpbawrhfqcecpg",
    "sbqffrdqhdcgaersgephrdfsbpaaheqscpgqabrdbhbqfcrecfgpdsrgfdsc",
    "ehqehgdpspherpqqsqrrrsss",
)


def chunk(n):
    return (n, None) if n < WIDE else (WIDE + (n - WIDE) // 2, (n - WIDE) % 2)


CHUNKS = WIDE + 2 * (BLOCKS - WIDE)


def kernel(a_hbm, b_hbm, c_out, a_own, a_all, s1, rl1, rl2, b_all, crecv, c0, prod,
           ld_sem, zr_sem, zs_sem, dr_sem, s1_sem, r1_sem, r2_sem, s2_sem, ag_sem, fw_sem, as_sem,
           cr_sem, cs_sem, c0_sem):
    row, y, z = lax.axis_index("row"), lax.axis_index("col"), lax.axis_index("depth")
    x, c = row // 2, row % 2
    width = b_all.shape[3]
    narrow = width // 2
    cols = a_own.shape[4]
    part_cols = (pl.ds(0, cols // 2), pl.ds(cols // 2, cols // 2))
    rest = slice(None)

    def at_x(dx):
        return {"row": 2 * ((x + dx + X_N) % X_N) + c}

    def at_y(dy):
        return {"col": (y + dy + Y_N) % Y_N}

    step = 1 - 2 * c
    z_long = {"depth": (z + step + Z_N) % Z_N}
    z_short = {"depth": (z - step + Z_N) % Z_N}
    partner = {"row": 2 * x + 1 - c}

    def send(src, dst, ssem, rsem, dev):
        pltpu.make_async_remote_copy(src_ref=src, dst_ref=dst, send_sem=ssem, recv_sem=rsem,
                                     device_id=dev, device_id_type=MESH).start()

    def wait(ref, sem):
        pltpu.make_async_copy(ref, ref, sem).wait()

    e_own = (y - x + Y_N) % Y_N
    flip = e_own // 3
    j_own = e_own

    def b_local(m, sem):
        return pltpu.make_async_copy(b_hbm.at[:, pl.ds(pl.multiple_of(m * width, width), width)],
                                     b_all.at[m, c * Z_N + z], ld_sem.at[sem])

    def a_load(r):
        return pltpu.make_async_copy(a_hbm.at[:, :, r], a_own.at[:, :, r], ld_sem.at[2 + r])

    a_load(0).start()
    b_local(0, 0).start()
    a_load(1).start()
    barrier = pltpu.get_barrier_semaphore()
    for dev in (at_x(1), at_x(-1), at_y(1), at_y(-1), z_long, z_short, partner):
        pl.semaphore_signal(barrier, inc=1, device_id=dev, device_id_type=MESH)
    lax.fori_loop(1, BLOCKS, lambda m, _: (b_local(m, 1).start(), 0)[1], 0)

    def quarter_sem(e, o, r):
        return s1_sem.at[(e + 1) % 2 * (2 - e // 2), o, r]

    def by_e(e, o, r, j, part, fn):
        col_part = rest if part is None else part_cols[part]

        @pl.when(e == 0)
        def _():
            fn(a_all.at[3, o, j, r, :, col_part])

        @pl.when(e != 0)
        def _():
            fn(s1.at[(e + Y_N - 1) % Y_N, o, r, :, col_part])

    for o in range(2):
        for r in range(2):
            by_e(e_own, o, r, 0, None, lambda dst: pltpu.make_async_copy(
                a_hbm.at[(o + flip) % 2, 0, r], dst, quarter_sem(e_own, o, r)).start())
    pl.semaphore_wait(barrier, 7)
    loaded = set()

    def ev_s1(o, r):
        if r not in loaded:
            loaded.add(r)
            a_load(r).wait()
        h = (o + flip) % 2
        send(a_own.at[h, 2, r, :, part_cols[0]], rl1.at[0, o, r], as_sem, r1_sem.at[o, r], at_y(1))
        send(a_own.at[h, 2, r, :, part_cols[1]], rl1.at[1, o, r], as_sem, r1_sem.at[o, r], at_y(-1))
        sem = quarter_sem(e_own, o, r)
        by_e(e_own, o, r, 1, None, lambda dst: send(a_own.at[h, 1, r], dst, as_sem, sem, at_y(1)))
        by_e(e_own, o, r, 3, None, lambda dst: send(a_own.at[h, 3, r], dst, as_sem, sem, at_y(-1)))

    def ev_r1(o, r):
        wait(rl1.at[:, o, r], r1_sem.at[o, r])
        for d, dy in ((0, 1), (1, -1)):
            e = (y - dy - x + 2 * Y_N) % Y_N
            by_e(e, o, r, 2, d, lambda dst: send(rl1.at[d, o, r], dst, as_sem, quarter_sem(e, o, r), at_y(dy)))

    def ev_s2(o, r):
        wait(s1.at[pl.ds(0, 2), o, r], quarter_sem(1, o, r))
        g = 2 * o
        j = (y - x - 1 + 2 * Y_N) % Y_N
        send(s1.at[0, o, r], a_all.at[g, o, j, r], as_sem, s2_sem.at[g, r], at_x(1))
        j = (y - x + 1 + Y_N) % Y_N
        send(s1.at[2, o, r], a_all.at[g, 1 - o, j, r], as_sem, s2_sem.at[g, r], at_x(-1))

    def ev_s2f(o, r):
        wait(s1.at[1, o, r], quarter_sem(2, o, r))
        for d in range(2):
            send(s1.at[1, o, r, :, part_cols[d]], rl2.at[d, o, r], as_sem, r2_sem.at[o, r], at_x(1 - 2 * d))

    def ev_r2(o, r):
        wait(rl2.at[:, o, r], r2_sem.at[o, r])
        for d, dx in ((0, 1), (1, -1)):
            j = (y - x - dx + 2 * Y_N) % Y_N
            send(rl2.at[d, o, r], a_all.at[1, o, j, r, :, part_cols[d]], as_sem, s2_sem.at[1, r], at_x(dx))

    def ev_ag(g, r):
        if g == 3:
            for o in range(2):
                wait(a_all.at[g, o, j_own, r], quarter_sem(0, o, r))
        else:
            wait(a_all.at[g, :, j_own, r], s2_sem.at[g, r])
        for d in range(2):
            quarter = a_all.at[g, d, j_own, r]
            send(quarter, quarter, as_sem, ag_sem.at[g, d, r], at_y(1))
            send(quarter, quarter, as_sem, ag_sem.at[g, d, r], at_y(-1))

    def ev_fw(g, r, d):
        wait(a_all.at[0, 0, 0], ag_sem.at[g, d, r])
        for k, dy in ((0, 1), (1, -1)):
            j = (y - dy - x + 2 * Y_N) % Y_N
            part = a_all.at[g, d, j, r, :, part_cols[k]]
            send(part, part, as_sem, fw_sem.at[g, r], at_y(dy))

    def group_complete(g, r):
        wait(a_all.at[0, 0, 0], fw_sem.at[g, r])

    def block(hop):
        return c * Z_N + (z - hop * step + 2 * Z_N) % Z_N

    def lanes_of(n):
        half = chunk(n)[1]
        return rest if half is None else pl.ds(half * narrow, narrow)

    def piece(n, kb):
        return b_all.at[chunk(n)[0], kb, :, lanes_of(n)]

    def hand_over(n, kb):
        send(piece(n, kb), piece(n, kb), zs_sem.at[chunk(n)[0] // 4], dr_sem.at[n], partner)

    def forward_long(n, hop):
        p = piece(n, block(hop))
        send(p, p, zs_sem.at[chunk(n)[0] // 4], zr_sem.at[n % Z_SEMS, hop], z_long)

    def forward_short(n, hop):
        p = piece(n, block(-hop))
        send(p, p, zs_sem.at[chunk(n)[0] // 4], zr_sem.at[n % Z_SEMS, 4 + hop], z_short)

    def ev_own(n):
        if n == 0:
            b_local(0, 0).wait()
        elif n == 1:
            wait(b_all.at[0, pl.ds(0, BLOCKS - 1)], ld_sem.at[1])
        forward_long(n, 0)
        forward_short(n, 0)
        hand_over(n, block(0))

    def ev_long(n, hop):
        wait(piece(n, block(hop)), zr_sem.at[n % Z_SEMS, hop - 1])
        if hop < 4:
            forward_long(n, hop)
        hand_over(n, block(hop))

    def ev_short(n, hop):
        wait(piece(n, block(-hop)), zr_sem.at[n % Z_SEMS, 4 + hop - 1])
        if hop < 3:
            forward_short(n, hop)
        hand_over(n, block(-hop))

    def handed_over(n):
        wait(b_all.at[0, pl.ds(0, Z_N), :, lanes_of(n)], dr_sem.at[n])

    def dot(a, b):
        return jnp.dot(a.reshape(-1, cols), b.reshape(cols, -1), preferred_element_type=jnp.float32)

    def sum_sem(n, q):
        return 2 * SPLIT + (n - SPLIT) % C_SEMS if isinstance(q, slice) else 2 * n + q

    def sum_stage(n, g, q, m, lanes, first, size, when, reuse, old):
        slot = n % SLOTS
        keep = rest if isinstance(lanes, slice) else pl.ds(0, narrow)
        arrivals = sum_sem(n, q)

        def pass_on(src, ssem):
            for d in range(2):
                send(src.at[d], crecv.at[m, g, d, :, q, :, lanes], ssem, cr_sem.at[arrivals, g], at_x(1 - 2 * d))

        def arrived():
            wait(crecv.at[m, g - 1, :, :, q, :, lanes], cr_sem.at[arrivals, g - 1])

        def begin():
            reuse(lambda: wait(c0.at[slot, :, :, :, :, old], c0_sem.at[slot]))
            c0[slot, :, :, q, :, keep] = prod[:, :, q, :, keep]
            pass_on(c0.at[slot, :, :, q, :, keep], c0_sem.at[slot])

        def middle():
            arrived()
            crecv[m, g - 1, :, :, q, :, lanes] += prod[:, :, q, :, keep]
            pass_on(crecv.at[m, g - 1, :, :, q, :, lanes], cs_sem.at[m // 4])

        def end():
            arrived()
            total = crecv[m, g - 1, :, :, q, :, lanes] + prod[:, :, q, :, keep]
            c_out[:, :, q, :, pl.ds(pl.multiple_of(first, size), size)] = total.astype(c_out.dtype)

        a = a_all[g, :, :, q]
        prod[:, :, q, :, keep] = dot(a, b_all[m, :, :, lanes]).reshape(a.shape[:-1] + (size,))
        when(g == 0, begin)
        when((g == 1) | (g == 2), middle)
        when(g == 3, end)

    def branch(cond, fn):
        pl.when(cond)(fn)

    def fixed(cond, fn):
        if cond:
            fn()

    def sum_loop(code, split, wide):
        n, g, q = code // 8, code // 2 % 4, code % 2
        if split:
            pl.when(n < SPLIT)(lambda: sum_stage(n, g, q, n, rest, n * width, width, branch, lambda fn: None, rest))
        if wide:
            pl.when(n >= SPLIT)(lambda: sum_stage(n, g, rest, n, rest, n * width, width, branch,
                                                  pl.when(n >= SLOTS), rest))

    def sum_narrow(n, g):
        m, half = chunk(n)
        old = rest if n - SLOTS < WIDE else pl.ds(0, narrow)
        sum_stage(n, g, rest, m, lanes_of(n), m * width + half * narrow, narrow, fixed, lambda fn: fn(), old)

    chunks = range(CHUNKS)
    queues = {"a": [(ev_own, (n,)) for n in chunks]}
    for hop in range(1, 5):
        queues["abcde"[hop]] = [(ev_long, (n, hop)) for n in chunks]
    for hop in range(1, 4):
        queues["efgh"[hop]] = [(ev_short, (n, hop)) for n in chunks]
    by_half = [(o, r) for o in range(2) for r in range(2)]
    by_row = [(o, r) for r in range(2) for o in range(2)]
    queues["i"] = [(ev_s1, p) for p in by_half]
    queues["j"] = [(ev_r1, p) for p in by_half]
    queues["k"] = [(ev_s2, p) for p in by_half]
    queues["l"] = [(ev_s2f, p) for p in by_row]
    queues["m"] = [(ev_r2, p) for p in by_row]
    groups = [(g, r) for g in range(4) for r in range(2)]
    queues["n"] = [(ev_ag, p) for p in groups]
    queues["o"] = [(ev_fw, p + (d,)) for p in groups for d in range(2)]
    for g in range(4):
        queues["pqrs"[g]] = [(None, (n, g, 0 if n < SPLIT else ALL)) for n in chunks]
        queues["tuvw"[g]] = [(None, (n, g, 1)) for n in range(SPLIT)]

    steps, before, complete, handed = [], [], set(), set()
    for letter in "".join(PROGRAM):
        fn, args = queues[letter].pop(0)
        if fn is not None:
            before.append((fn, args))
            continue
        n, g, q = args
        for r in (range(2) if q == ALL else (q,)):
            if (g, r) not in complete:
                complete.add((g, r))
                before.append((group_complete, (g, r)))
        if n not in handed:
            handed.add(n)
            before.append((handed_over, (n,)))
        if n >= WIDE:
            before.append((sum_narrow, (n, g)))
        else:
            steps.append((before, (n * 4 + g) * 2 + q % 2, q != ALL))
            before = []

    def run(todo):
        for fn, args in todo:
            fn(*args)

    def in_loop(first, last):
        part = steps[first:last]

        def body(k, carry):
            code = part[0][1]
            for i, (todo, this, _) in enumerate(part):
                code = jnp.where(k == first + i, this, code)
                if todo:
                    pl.when(k == first + i)(lambda: run(todo))
            sum_loop(code, any(s for _, _, s in part), any(not s for _, _, s in part))
            return carry

        lax.fori_loop(first, last, body, 0)

    for first in range(0, len(steps), LOOP):
        in_loop(first, min(first + LOOP, len(steps)))
    run(before)

    for i in range(BLOCKS // 4):
        wait(b_all.at[pl.ds(0, 4), pl.ds(0, 15)], zs_sem.at[i])
        wait(crecv.at[pl.ds(0, 4), pl.ds(0, 2)], cs_sem.at[i])
    wait(b_all.at[pl.ds(0, 5)], as_sem)
    for n in range(CHUNKS - SLOTS, CHUNKS):
        keep = rest if n < WIDE else pl.ds(0, narrow)
        wait(c0.at[n % SLOTS, :, :, :, :, keep], c0_sem.at[n % SLOTS])


def solution(mesh):
    def local_product(a_blk, b_blk):
        rows, cols = a_blk.shape
        width = cols // BLOCKS
        few = rows // 16
        dma = pltpu.SemaphoreType.DMA
        c_blk = pl.pallas_call(
            kernel,
            name="matmul_3d",
            out_shape=pltpu.VMEM((2, 4, 2, few, cols), jnp.bfloat16),
            in_specs=[pl.BlockSpec(memory_space=pl.ANY)] * 2,
            out_specs=pl.BlockSpec(memory_space=pltpu.VMEM),
            scratch_shapes=[
                pltpu.VMEM((2, 4, 2, few, cols), jnp.bfloat16),
                pltpu.VMEM((4, 2, 4, 2, few, cols), jnp.bfloat16),
                pltpu.VMEM((3, 2, 2, few, cols), jnp.bfloat16),
                pltpu.VMEM((2, 2, 2, few, cols // 2), jnp.bfloat16),
                pltpu.VMEM((2, 2, 2, few, cols // 2), jnp.bfloat16),
                pltpu.VMEM((BLOCKS, 2 * Z_N, rows, width), jnp.bfloat16),
                pltpu.VMEM((BLOCKS, 3, 2, 4, 2, few, width), jnp.float32),
                pltpu.VMEM((SLOTS, 2, 4, 2, few, width), jnp.float32),
                pltpu.VMEM((2, 4, 2, few, width), jnp.float32),
                dma((4,)), dma((Z_SEMS, 7)), dma((BLOCKS // 4,)), dma((CHUNKS,)),
                dma((3, 2, 2)), dma((2, 2)), dma((2, 2)), dma((3, 2)), dma((4, 2, 2)), dma((4, 2)), dma,
                dma((2 * SPLIT + C_SEMS, 3)), dma((BLOCKS // 4,)), dma((SLOTS,)),
            ],
            compiler_params=pltpu.CompilerParams(
                collective_id=0, has_side_effects=True, vmem_limit_bytes=61 * 1024 * 1024
            ),
        )(a_blk.reshape(2, 4, 2, few, cols), b_blk)
        return c_blk.reshape(rows, cols)

    block_spec = P(("row", "depth"), "col")
    return jax.shard_map(local_product, mesh=mesh, in_specs=(block_spec, block_spec), out_specs=block_spec, check_vma=False)
```

```python
import jax
import jax.numpy as jnp
from jax import lax
from jax.experimental import pallas as pl
from jax.experimental.pallas import tpu as pltpu
from jax.sharding import PartitionSpec as P

MESH = pl.DeviceIdType.MESH
X_N, Y_N, Z_N = 4, 4, 8
BLOCKS = 16
SLOTS = 8
LOOP = 8
WIDE = 14
SPLIT = 6
ALL = 2
Z_SEMS, C_SEMS = 4, 5

PROGRAM = (
    "aiaifjibfajakbcjlifgkcbklnbahjnddlmcomlgfooeamoncdhmgkbdtneh",
    "ogpfepctbehopaotgdtopcnqbqffnqquehduaoptogeuguocqhfbounardhp",
    "tvrcoagqbveourndpbssavvhesocvfcopfqvbfwwwwdrgqgwdrracwaehsre",
    "hspsbpdsgfrbcaqaeqhspgdrcffrhqbebsdgapscrgaechfqdpbshdargfeb",
    "cqeffbhpcgdpcrdsghgeqdqehheppprsqqqsrrrrssss",
)


def chunk(n):
    return (n, None) if n < WIDE else (WIDE + (n - WIDE) // 2, (n - WIDE) % 2)


CHUNKS = WIDE + 2 * (BLOCKS - WIDE)


def kernel(a_hbm, b_hbm, c_out, a_own, a_all, s1, rl1, rl2, b_all, crecv, c0, prod,
           ld_sem, zr_sem, zs_sem, dr_sem, s1_sem, r1_sem, r2_sem, s2_sem, ag_sem, fw_sem, as_sem,
           cr_sem, cs_sem, c0_sem):
    row, y, z = lax.axis_index("row"), lax.axis_index("col"), lax.axis_index("depth")
    x, c = row // 2, row % 2
    width = b_all.shape[3]
    narrow = width // 2
    cols = a_own.shape[4]
    part_cols = (pl.ds(0, cols // 2), pl.ds(cols // 2, cols // 2))
    rest = slice(None)

    def at_x(dx):
        return {"row": 2 * ((x + dx + X_N) % X_N) + c}

    def at_y(dy):
        return {"col": (y + dy + Y_N) % Y_N}

    step = 1 - 2 * c
    z_long = {"depth": (z + step + Z_N) % Z_N}
    z_short = {"depth": (z - step + Z_N) % Z_N}
    partner = {"row": 2 * x + 1 - c}

    def send(src, dst, ssem, rsem, dev):
        pltpu.make_async_remote_copy(src_ref=src, dst_ref=dst, send_sem=ssem, recv_sem=rsem,
                                     device_id=dev, device_id_type=MESH).start()

    def wait(ref, sem):
        pltpu.make_async_copy(ref, ref, sem).wait()

    e_own = (y - x + Y_N) % Y_N
    flip = e_own // 3
    j_own = e_own

    def b_local(m, sem):
        return pltpu.make_async_copy(b_hbm.at[:, pl.ds(pl.multiple_of(m * width, width), width)],
                                     b_all.at[m, c * Z_N + z], ld_sem.at[sem])

    def a_load(r):
        return pltpu.make_async_copy(a_hbm.at[:, :, r], a_own.at[:, :, r], ld_sem.at[2 + r])

    a_load(0).start()
    b_local(0, 0).start()
    a_load(1).start()
    barrier = pltpu.get_barrier_semaphore()
    for dev in (at_x(1), at_x(-1), at_y(1), at_y(-1), z_long, z_short, partner):
        pl.semaphore_signal(barrier, inc=1, device_id=dev, device_id_type=MESH)
    lax.fori_loop(1, BLOCKS, lambda m, _: (b_local(m, 1).start(), 0)[1], 0)

    def quarter_sem(e, o, r):
        return s1_sem.at[(e + 1) % 2 * (2 - e // 2), o, r]

    def by_e(e, o, r, j, part, fn):
        col_part = rest if part is None else part_cols[part]

        @pl.when(e == 0)
        def _():
            fn(a_all.at[3, o, j, r, :, col_part])

        @pl.when(e != 0)
        def _():
            fn(s1.at[(e + Y_N - 1) % Y_N, o, r, :, col_part])

    for o in range(2):
        for r in range(2):
            by_e(e_own, o, r, 0, None, lambda dst: pltpu.make_async_copy(
                a_hbm.at[(o + flip) % 2, 0, r], dst, quarter_sem(e_own, o, r)).start())
    pl.semaphore_wait(barrier, 7)
    loaded = set()

    def ev_s1(o, r):
        if r not in loaded:
            loaded.add(r)
            a_load(r).wait()
        h = (o + flip) % 2
        send(a_own.at[h, 2, r, :, part_cols[0]], rl1.at[0, o, r], as_sem, r1_sem.at[o, r], at_y(1))
        send(a_own.at[h, 2, r, :, part_cols[1]], rl1.at[1, o, r], as_sem, r1_sem.at[o, r], at_y(-1))
        sem = quarter_sem(e_own, o, r)
        by_e(e_own, o, r, 1, None, lambda dst: send(a_own.at[h, 1, r], dst, as_sem, sem, at_y(1)))
        by_e(e_own, o, r, 3, None, lambda dst: send(a_own.at[h, 3, r], dst, as_sem, sem, at_y(-1)))

    def ev_r1(o, r):
        wait(rl1.at[:, o, r], r1_sem.at[o, r])
        for d, dy in ((0, 1), (1, -1)):
            e = (y - dy - x + 2 * Y_N) % Y_N
            by_e(e, o, r, 2, d, lambda dst: send(rl1.at[d, o, r], dst, as_sem, quarter_sem(e, o, r), at_y(dy)))

    def ev_s2(o, r):
        wait(s1.at[pl.ds(0, 2), o, r], quarter_sem(1, o, r))
        g = 2 * o
        j = (y - x - 1 + 2 * Y_N) % Y_N
        send(s1.at[0, o, r], a_all.at[g, o, j, r], as_sem, s2_sem.at[g, r], at_x(1))
        j = (y - x + 1 + Y_N) % Y_N
        send(s1.at[2, o, r], a_all.at[g, 1 - o, j, r], as_sem, s2_sem.at[g, r], at_x(-1))

    def ev_s2f(o, r):
        wait(s1.at[1, o, r], quarter_sem(2, o, r))
        for d in range(2):
            send(s1.at[1, o, r, :, part_cols[d]], rl2.at[d, o, r], as_sem, r2_sem.at[o, r], at_x(1 - 2 * d))

    def ev_r2(o, r):
        wait(rl2.at[:, o, r], r2_sem.at[o, r])
        for d, dx in ((0, 1), (1, -1)):
            j = (y - x - dx + 2 * Y_N) % Y_N
            send(rl2.at[d, o, r], a_all.at[1, o, j, r, :, part_cols[d]], as_sem, s2_sem.at[1, r], at_x(dx))

    def ev_ag(g, r):
        if g == 3:
            for o in range(2):
                wait(a_all.at[g, o, j_own, r], quarter_sem(0, o, r))
        else:
            wait(a_all.at[g, :, j_own, r], s2_sem.at[g, r])
        for d in range(2):
            quarter = a_all.at[g, d, j_own, r]
            send(quarter, quarter, as_sem, ag_sem.at[g, d, r], at_y(1))
            send(quarter, quarter, as_sem, ag_sem.at[g, d, r], at_y(-1))

    def ev_fw(g, r, d):
        wait(a_all.at[0, 0, 0], ag_sem.at[g, d, r])
        for k, dy in ((0, 1), (1, -1)):
            j = (y - dy - x + 2 * Y_N) % Y_N
            part = a_all.at[g, d, j, r, :, part_cols[k]]
            send(part, part, as_sem, fw_sem.at[g, r], at_y(dy))

    def group_complete(g, r):
        wait(a_all.at[0, 0, 0], fw_sem.at[g, r])

    def block(hop):
        return c * Z_N + (z - hop * step + 2 * Z_N) % Z_N

    def lanes_of(n):
        half = chunk(n)[1]
        return rest if half is None else pl.ds(half * narrow, narrow)

    def piece(n, kb):
        return b_all.at[chunk(n)[0], kb, :, lanes_of(n)]

    def hand_over(n, kb):
        send(piece(n, kb), piece(n, kb), zs_sem.at[chunk(n)[0] // 4], dr_sem.at[n], partner)

    def forward_long(n, hop):
        p = piece(n, block(hop))
        send(p, p, zs_sem.at[chunk(n)[0] // 4], zr_sem.at[n % Z_SEMS, hop], z_long)

    def forward_short(n, hop):
        p = piece(n, block(-hop))
        send(p, p, zs_sem.at[chunk(n)[0] // 4], zr_sem.at[n % Z_SEMS, 4 + hop], z_short)

    def ev_own(n):
        if n == 0:
            b_local(0, 0).wait()
        elif n == 1:
            wait(b_all.at[0, pl.ds(0, BLOCKS - 1)], ld_sem.at[1])
        forward_long(n, 0)
        forward_short(n, 0)
        hand_over(n, block(0))

    def ev_long(n, hop):
        wait(piece(n, block(hop)), zr_sem.at[n % Z_SEMS, hop - 1])
        if hop < 4:
            forward_long(n, hop)
        hand_over(n, block(hop))

    def ev_short(n, hop):
        wait(piece(n, block(-hop)), zr_sem.at[n % Z_SEMS, 4 + hop - 1])
        if hop < 3:
            forward_short(n, hop)
        hand_over(n, block(-hop))

    def handed_over(n):
        wait(b_all.at[0, pl.ds(0, Z_N), :, lanes_of(n)], dr_sem.at[n])

    def dot(a, b):
        return jnp.dot(a.reshape(-1, cols), b.reshape(cols, -1), preferred_element_type=jnp.float32)

    def sum_sem(n, q):
        return 2 * SPLIT + (n - SPLIT) % C_SEMS if isinstance(q, slice) else 2 * n + q

    def sum_stage(n, g, q, m, lanes, first, size, when, reuse, old):
        slot = n % SLOTS
        keep = rest if isinstance(lanes, slice) else pl.ds(0, narrow)
        arrivals = sum_sem(n, q)

        def pass_on(src, ssem):
            for d in range(2):
                send(src.at[d], crecv.at[m, g, d, :, q, :, lanes], ssem, cr_sem.at[arrivals, g], at_x(1 - 2 * d))

        def arrived():
            wait(crecv.at[m, g - 1, :, :, q, :, lanes], cr_sem.at[arrivals, g - 1])

        def begin():
            reuse(lambda: wait(c0.at[slot, :, :, :, :, old], c0_sem.at[slot]))
            c0[slot, :, :, q, :, keep] = prod[:, :, q, :, keep]
            pass_on(c0.at[slot, :, :, q, :, keep], c0_sem.at[slot])

        def middle():
            arrived()
            crecv[m, g - 1, :, :, q, :, lanes] += prod[:, :, q, :, keep]
            pass_on(crecv.at[m, g - 1, :, :, q, :, lanes], cs_sem.at[m // 4])

        def end():
            arrived()
            total = crecv[m, g - 1, :, :, q, :, lanes] + prod[:, :, q, :, keep]
            c_out[:, :, q, :, pl.ds(pl.multiple_of(first, size), size)] = total.astype(c_out.dtype)

        a = a_all[g, :, :, q]
        prod[:, :, q, :, keep] = dot(a, b_all[m, :, :, lanes]).reshape(a.shape[:-1] + (size,))
        when(g == 0, begin)
        when((g == 1) | (g == 2), middle)
        when(g == 3, end)

    def branch(cond, fn):
        pl.when(cond)(fn)

    def fixed(cond, fn):
        if cond:
            fn()

    def sum_loop(code, split, wide):
        n, g, q = code // 8, code // 2 % 4, code % 2
        if split:
            pl.when(n < SPLIT)(lambda: sum_stage(n, g, q, n, rest, n * width, width, branch, lambda fn: None, rest))
        if wide:
            pl.when(n >= SPLIT)(lambda: sum_stage(n, g, rest, n, rest, n * width, width, branch,
                                                  pl.when(n >= SLOTS), rest))

    def sum_narrow(n, g):
        m, half = chunk(n)
        old = rest if n - SLOTS < WIDE else pl.ds(0, narrow)
        sum_stage(n, g, rest, m, lanes_of(n), m * width + half * narrow, narrow, fixed, lambda fn: fn(), old)

    chunks = range(CHUNKS)
    queues = {"a": [(ev_own, (n,)) for n in chunks]}
    for hop in range(1, 5):
        queues["abcde"[hop]] = [(ev_long, (n, hop)) for n in chunks]
    for hop in range(1, 4):
        queues["efgh"[hop]] = [(ev_short, (n, hop)) for n in chunks]
    by_half = [(o, r) for o in range(2) for r in range(2)]
    by_row = [(o, r) for r in range(2) for o in range(2)]
    queues["i"] = [(ev_s1, p) for p in by_row]
    queues["j"] = [(ev_r1, p) for p in by_row]
    queues["k"] = [(ev_s2, p) for p in by_row]
    queues["l"] = [(ev_s2f, p) for p in by_row]
    queues["m"] = [(ev_r2, p) for p in by_row]
    groups = [(g, r) for g in range(4) for r in range(2)]
    queues["n"] = [(ev_ag, p) for p in groups]
    queues["o"] = [(ev_fw, p + (d,)) for p in groups for d in range(2)]
    for g in range(4):
        queues["pqrs"[g]] = [(None, (n, g, 0 if n < SPLIT else ALL)) for n in chunks]
        queues["tuvw"[g]] = [(None, (n, g, 1)) for n in range(SPLIT)]

    steps, before, complete, handed = [], [], set(), set()
    for letter in "".join(PROGRAM):
        fn, args = queues[letter].pop(0)
        if fn is not None:
            before.append((fn, args))
            continue
        n, g, q = args
        for r in (range(2) if q == ALL else (q,)):
            if (g, r) not in complete:
                complete.add((g, r))
                before.append((group_complete, (g, r)))
        if n not in handed:
            handed.add(n)
            before.append((handed_over, (n,)))
        if n >= WIDE:
            before.append((sum_narrow, (n, g)))
        else:
            steps.append((before, (n * 4 + g) * 2 + q % 2, q != ALL))
            before = []

    def run(todo):
        for fn, args in todo:
            fn(*args)

    def in_loop(first, last):
        part = steps[first:last]

        def body(k, carry):
            code = part[0][1]
            for i, (todo, this, _) in enumerate(part):
                code = jnp.where(k == first + i, this, code)
                if todo:
                    pl.when(k == first + i)(lambda: run(todo))
            sum_loop(code, any(s for _, _, s in part), any(not s for _, _, s in part))
            return carry

        lax.fori_loop(first, last, body, 0)

    for first in range(0, len(steps), LOOP):
        in_loop(first, min(first + LOOP, len(steps)))
    run(before)

    for i in range(BLOCKS // 4):
        wait(b_all.at[pl.ds(0, 4), pl.ds(0, 15)], zs_sem.at[i])
        wait(crecv.at[pl.ds(0, 4), pl.ds(0, 2)], cs_sem.at[i])
    wait(b_all.at[pl.ds(0, 5)], as_sem)
    for n in range(CHUNKS - SLOTS, CHUNKS):
        keep = rest if n < WIDE else pl.ds(0, narrow)
        wait(c0.at[n % SLOTS, :, :, :, :, keep], c0_sem.at[n % SLOTS])


def solution(mesh):
    def local_product(a_blk, b_blk):
        rows, cols = a_blk.shape
        width = cols // BLOCKS
        few = rows // 16
        dma = pltpu.SemaphoreType.DMA
        c_blk = pl.pallas_call(
            kernel,
            name="matmul_3d",
            out_shape=pltpu.VMEM((2, 4, 2, few, cols), jnp.bfloat16),
            in_specs=[pl.BlockSpec(memory_space=pl.ANY)] * 2,
            out_specs=pl.BlockSpec(memory_space=pltpu.VMEM),
            scratch_shapes=[
                pltpu.VMEM((2, 4, 2, few, cols), jnp.bfloat16),
                pltpu.VMEM((4, 2, 4, 2, few, cols), jnp.bfloat16),
                pltpu.VMEM((3, 2, 2, few, cols), jnp.bfloat16),
                pltpu.VMEM((2, 2, 2, few, cols // 2), jnp.bfloat16),
                pltpu.VMEM((2, 2, 2, few, cols // 2), jnp.bfloat16),
                pltpu.VMEM((BLOCKS, 2 * Z_N, rows, width), jnp.bfloat16),
                pltpu.VMEM((BLOCKS, 3, 2, 4, 2, few, width), jnp.float32),
                pltpu.VMEM((SLOTS, 2, 4, 2, few, width), jnp.float32),
                pltpu.VMEM((2, 4, 2, few, width), jnp.float32),
                dma((4,)), dma((Z_SEMS, 7)), dma((BLOCKS // 4,)), dma((CHUNKS,)),
                dma((3, 2, 2)), dma((2, 2)), dma((2, 2)), dma((3, 2)), dma((4, 2, 2)), dma((4, 2)), dma,
                dma((2 * SPLIT + C_SEMS, 3)), dma((BLOCKS // 4,)), dma((SLOTS,)),
            ],
            compiler_params=pltpu.CompilerParams(
                collective_id=0, has_side_effects=True, vmem_limit_bytes=61 * 1024 * 1024
            ),
        )(a_blk.reshape(2, 4, 2, few, cols), b_blk)
        return c_blk.reshape(rows, cols)

    block_spec = P(("row", "depth"), "col")
    return jax.shard_map(local_product, mesh=mesh, in_specs=(block_spec, block_spec), out_specs=block_spec, check_vma=False)
```

```python
import jax
import jax.numpy as jnp
from jax import lax
from jax.experimental import pallas as pl
from jax.experimental.pallas import tpu as pltpu
from jax.sharding import PartitionSpec as P

MESH = pl.DeviceIdType.MESH
X_N, Y_N, Z_N = 4, 4, 8
BLOCKS = 16
SLOTS = 8
LOOP = 8
WIDE = 13
SPLIT = 6
ALL = 2
Z_SEMS, C_SEMS = 5, 5

PROGRAM = (
    "aiaiabjiafjkbjflcaikbbnckmjdlcgnlfcdekfohdaommgolbgonemtdghp",
    "noehbcptfahoetpoctonndpgqfqdfaquheqbuopgteguooucqfbahounhrpd",
    "tvvcoagqueorndbvpbsafvsherrovfocpqcsbgwwwwdwrgsqdfahcvarhesr",
    "ewpsgbpsfdrqbchqgeaasfpdrarhcbfebqbgsfpdsacgchrcfgeaqdbhpdds",
    "garebcehffqhebpfcpgpdcsgrdgqheqhdheqpesprpqrsqqrsrrrssss",
)


def chunk(n):
    return (n, None) if n < WIDE else (WIDE + (n - WIDE) // 2, (n - WIDE) % 2)


CHUNKS = WIDE + 2 * (BLOCKS - WIDE)


def kernel(a_hbm, b_hbm, c_out, a_own, a_all, s1, rl1, rl2, b_all, crecv, c0, prod,
           ld_sem, zr_sem, zs_sem, dr_sem, s1_sem, r1_sem, r2_sem, s2_sem, ag_sem, fw_sem, as_sem,
           cr_sem, cs_sem, c0_sem):
    row, y, z = lax.axis_index("row"), lax.axis_index("col"), lax.axis_index("depth")
    x, c = row // 2, row % 2
    width = b_all.shape[3]
    narrow = width // 2
    cols = a_own.shape[4]
    part_cols = (pl.ds(0, cols // 2), pl.ds(cols // 2, cols // 2))
    rest = slice(None)

    def at_x(dx):
        return {"row": 2 * ((x + dx + X_N) % X_N) + c}

    def at_y(dy):
        return {"col": (y + dy + Y_N) % Y_N}

    step = 1 - 2 * c
    z_long = {"depth": (z + step + Z_N) % Z_N}
    z_short = {"depth": (z - step + Z_N) % Z_N}
    partner = {"row": 2 * x + 1 - c}

    def send(src, dst, ssem, rsem, dev):
        pltpu.make_async_remote_copy(src_ref=src, dst_ref=dst, send_sem=ssem, recv_sem=rsem,
                                     device_id=dev, device_id_type=MESH).start()

    def wait(ref, sem):
        pltpu.make_async_copy(ref, ref, sem).wait()

    e_own = (y - x + Y_N) % Y_N
    flip = e_own // 3
    j_own = e_own

    def b_local(m, sem):
        return pltpu.make_async_copy(b_hbm.at[:, pl.ds(pl.multiple_of(m * width, width), width)],
                                     b_all.at[m, c * Z_N + z], ld_sem.at[sem])

    def a_load(r):
        return pltpu.make_async_copy(a_hbm.at[:, :, r], a_own.at[:, :, r], ld_sem.at[2 + r])

    a_load(0).start()
    b_local(0, 0).start()
    a_load(1).start()
    barrier = pltpu.get_barrier_semaphore()
    for dev in (at_x(1), at_x(-1), at_y(1), at_y(-1), z_long, z_short, partner):
        pl.semaphore_signal(barrier, inc=1, device_id=dev, device_id_type=MESH)
    lax.fori_loop(1, BLOCKS, lambda m, _: (b_local(m, 1).start(), 0)[1], 0)

    def quarter_sem(e, o, r):
        return s1_sem.at[(e + 1) % 2 * (2 - e // 2), o, r]

    def by_e(e, o, r, j, part, fn):
        col_part = rest if part is None else part_cols[part]

        @pl.when(e == 0)
        def _():
            fn(a_all.at[3, o, j, r, :, col_part])

        @pl.when(e != 0)
        def _():
            fn(s1.at[(e + Y_N - 1) % Y_N, o, r, :, col_part])

    for o in range(2):
        for r in range(2):
            by_e(e_own, o, r, 0, None, lambda dst: pltpu.make_async_copy(
                a_hbm.at[(o + flip) % 2, 0, r], dst, quarter_sem(e_own, o, r)).start())
    pl.semaphore_wait(barrier, 7)
    loaded = set()

    def ev_s1(o, r):
        if r not in loaded:
            loaded.add(r)
            a_load(r).wait()
        h = (o + flip) % 2
        send(a_own.at[h, 2, r, :, part_cols[0]], rl1.at[0, o, r], as_sem, r1_sem.at[o, r], at_y(1))
        send(a_own.at[h, 2, r, :, part_cols[1]], rl1.at[1, o, r], as_sem, r1_sem.at[o, r], at_y(-1))
        sem = quarter_sem(e_own, o, r)
        by_e(e_own, o, r, 1, None, lambda dst: send(a_own.at[h, 1, r], dst, as_sem, sem, at_y(1)))
        by_e(e_own, o, r, 3, None, lambda dst: send(a_own.at[h, 3, r], dst, as_sem, sem, at_y(-1)))

    def ev_r1(o, r):
        wait(rl1.at[:, o, r], r1_sem.at[o, r])
        for d, dy in ((0, 1), (1, -1)):
            e = (y - dy - x + 2 * Y_N) % Y_N
            by_e(e, o, r, 2, d, lambda dst: send(rl1.at[d, o, r], dst, as_sem, quarter_sem(e, o, r), at_y(dy)))

    def ev_s2(o, r):
        wait(s1.at[pl.ds(0, 2), o, r], quarter_sem(1, o, r))
        g = 2 * o
        j = (y - x - 1 + 2 * Y_N) % Y_N
        send(s1.at[0, o, r], a_all.at[g, o, j, r], as_sem, s2_sem.at[g, r], at_x(1))
        j = (y - x + 1 + Y_N) % Y_N
        send(s1.at[2, o, r], a_all.at[g, 1 - o, j, r], as_sem, s2_sem.at[g, r], at_x(-1))

    def ev_s2f(o, r):
        wait(s1.at[1, o, r], quarter_sem(2, o, r))
        for d in range(2):
            send(s1.at[1, o, r, :, part_cols[d]], rl2.at[d, o, r], as_sem, r2_sem.at[o, r], at_x(1 - 2 * d))

    def ev_r2(o, r):
        wait(rl2.at[:, o, r], r2_sem.at[o, r])
        for d, dx in ((0, 1), (1, -1)):
            j = (y - x - dx + 2 * Y_N) % Y_N
            send(rl2.at[d, o, r], a_all.at[1, o, j, r, :, part_cols[d]], as_sem, s2_sem.at[1, r], at_x(dx))

    def ev_ag(g, r):
        if g == 3:
            for o in range(2):
                wait(a_all.at[g, o, j_own, r], quarter_sem(0, o, r))
        else:
            wait(a_all.at[g, :, j_own, r], s2_sem.at[g, r])
        for d in range(2):
            quarter = a_all.at[g, d, j_own, r]
            send(quarter, quarter, as_sem, ag_sem.at[g, d, r], at_y(1))
            send(quarter, quarter, as_sem, ag_sem.at[g, d, r], at_y(-1))

    def ev_fw(g, r, d):
        wait(a_all.at[0, 0, 0], ag_sem.at[g, d, r])
        for k, dy in ((0, 1), (1, -1)):
            j = (y - dy - x + 2 * Y_N) % Y_N
            part = a_all.at[g, d, j, r, :, part_cols[k]]
            send(part, part, as_sem, fw_sem.at[g, r], at_y(dy))

    def group_complete(g, r):
        wait(a_all.at[0, 0, 0], fw_sem.at[g, r])

    def block(hop):
        return c * Z_N + (z - hop * step + 2 * Z_N) % Z_N

    def lanes_of(n):
        half = chunk(n)[1]
        return rest if half is None else pl.ds(half * narrow, narrow)

    def piece(n, kb):
        return b_all.at[chunk(n)[0], kb, :, lanes_of(n)]

    def hand_over(n, kb):
        send(piece(n, kb), piece(n, kb), zs_sem.at[chunk(n)[0] // 4], dr_sem.at[n], partner)

    def forward_long(n, hop):
        p = piece(n, block(hop))
        send(p, p, zs_sem.at[chunk(n)[0] // 4], zr_sem.at[n % Z_SEMS, hop], z_long)

    def forward_short(n, hop):
        p = piece(n, block(-hop))
        send(p, p, zs_sem.at[chunk(n)[0] // 4], zr_sem.at[n % Z_SEMS, 4 + hop], z_short)

    def ev_own(n):
        if n == 0:
            b_local(0, 0).wait()
        elif n == 1:
            wait(b_all.at[0, pl.ds(0, BLOCKS - 1)], ld_sem.at[1])
        forward_long(n, 0)
        forward_short(n, 0)
        hand_over(n, block(0))

    def ev_long(n, hop):
        wait(piece(n, block(hop)), zr_sem.at[n % Z_SEMS, hop - 1])
        if hop < 4:
            forward_long(n, hop)
        hand_over(n, block(hop))

    def ev_short(n, hop):
        wait(piece(n, block(-hop)), zr_sem.at[n % Z_SEMS, 4 + hop - 1])
        if hop < 3:
            forward_short(n, hop)
        hand_over(n, block(-hop))

    def handed_over(n):
        wait(b_all.at[0, pl.ds(0, Z_N), :, lanes_of(n)], dr_sem.at[n])

    def dot(a, b):
        return jnp.dot(a.reshape(-1, cols), b.reshape(cols, -1), preferred_element_type=jnp.float32)

    def sum_sem(n, q):
        return 2 * SPLIT + (n - SPLIT) % C_SEMS if isinstance(q, slice) else 2 * n + q

    def sum_stage(n, g, q, m, lanes, first, size, when, reuse, old):
        slot = n % SLOTS
        keep = rest if isinstance(lanes, slice) else pl.ds(0, narrow)
        arrivals = sum_sem(n, q)

        def pass_on(src, ssem):
            for d in range(2):
                send(src.at[d], crecv.at[m, g, d, :, q, :, lanes], ssem, cr_sem.at[arrivals, g], at_x(1 - 2 * d))

        def arrived():
            wait(crecv.at[m, g - 1, :, :, q, :, lanes], cr_sem.at[arrivals, g - 1])

        def begin():
            reuse(lambda: wait(c0.at[slot, :, :, :, :, old], c0_sem.at[slot]))
            c0[slot, :, :, q, :, keep] = prod[:, :, q, :, keep]
            pass_on(c0.at[slot, :, :, q, :, keep], c0_sem.at[slot])

        def middle():
            arrived()
            crecv[m, g - 1, :, :, q, :, lanes] += prod[:, :, q, :, keep]
            pass_on(crecv.at[m, g - 1, :, :, q, :, lanes], cs_sem.at[m // 4])

        def end():
            arrived()
            total = crecv[m, g - 1, :, :, q, :, lanes] + prod[:, :, q, :, keep]
            c_out[:, :, q, :, pl.ds(pl.multiple_of(first, size), size)] = total.astype(c_out.dtype)

        a = a_all[g, :, :, q]
        prod[:, :, q, :, keep] = dot(a, b_all[m, :, :, lanes]).reshape(a.shape[:-1] + (size,))
        when(g == 0, begin)
        when((g == 1) | (g == 2), middle)
        when(g == 3, end)

    def branch(cond, fn):
        pl.when(cond)(fn)

    def fixed(cond, fn):
        if cond:
            fn()

    def sum_loop(code, split, wide):
        n, g, q = code // 8, code // 2 % 4, code % 2
        if split:
            pl.when(n < SPLIT)(lambda: sum_stage(n, g, q, n, rest, n * width, width, branch, lambda fn: None, rest))
        if wide:
            pl.when(n >= SPLIT)(lambda: sum_stage(n, g, rest, n, rest, n * width, width, branch,
                                                  pl.when(n >= SLOTS), rest))

    def sum_narrow(n, g):
        m, half = chunk(n)
        old = rest if n - SLOTS < WIDE else pl.ds(0, narrow)
        sum_stage(n, g, rest, m, lanes_of(n), m * width + half * narrow, narrow, fixed, lambda fn: fn(), old)

    chunks = range(CHUNKS)
    queues = {"a": [(ev_own, (n,)) for n in chunks]}
    for hop in range(1, 5):
        queues["abcde"[hop]] = [(ev_long, (n, hop)) for n in chunks]
    for hop in range(1, 4):
        queues["efgh"[hop]] = [(ev_short, (n, hop)) for n in chunks]
    by_half = [(o, r) for o in range(2) for r in range(2)]
    by_row = [(o, r) for r in range(2) for o in range(2)]
    queues["i"] = [(ev_s1, p) for p in by_row]
    queues["j"] = [(ev_r1, p) for p in by_row]
    queues["k"] = [(ev_s2, p) for p in by_row]
    queues["l"] = [(ev_s2f, p) for p in by_row]
    queues["m"] = [(ev_r2, p) for p in by_row]
    groups = [(g, r) for g in range(4) for r in range(2)]
    queues["n"] = [(ev_ag, p) for p in groups]
    queues["o"] = [(ev_fw, p + (d,)) for p in groups for d in range(2)]
    for g in range(4):
        queues["pqrs"[g]] = [(None, (n, g, 0 if n < SPLIT else ALL)) for n in chunks]
        queues["tuvw"[g]] = [(None, (n, g, 1)) for n in range(SPLIT)]

    steps, before, complete, handed = [], [], set(), set()
    for letter in "".join(PROGRAM):
        fn, args = queues[letter].pop(0)
        if fn is not None:
            before.append((fn, args))
            continue
        n, g, q = args
        for r in (range(2) if q == ALL else (q,)):
            if (g, r) not in complete:
                complete.add((g, r))
                before.append((group_complete, (g, r)))
        if n not in handed:
            handed.add(n)
            before.append((handed_over, (n,)))
        if n >= WIDE:
            before.append((sum_narrow, (n, g)))
        else:
            steps.append((before, (n * 4 + g) * 2 + q % 2, q != ALL))
            before = []

    def run(todo):
        for fn, args in todo:
            fn(*args)

    def in_loop(first, last):
        part = steps[first:last]

        def body(k, carry):
            code = part[0][1]
            for i, (todo, this, _) in enumerate(part):
                code = jnp.where(k == first + i, this, code)
                if todo:
                    pl.when(k == first + i)(lambda: run(todo))
            sum_loop(code, any(s for _, _, s in part), any(not s for _, _, s in part))
            return carry

        lax.fori_loop(first, last, body, 0)

    for first in range(0, len(steps), LOOP):
        in_loop(first, min(first + LOOP, len(steps)))
    run(before)

    for i in range(BLOCKS // 4):
        wait(b_all.at[pl.ds(0, 4), pl.ds(0, 15)], zs_sem.at[i])
        wait(crecv.at[pl.ds(0, 4), pl.ds(0, 2)], cs_sem.at[i])
    wait(b_all.at[pl.ds(0, 5)], as_sem)
    for n in range(CHUNKS - SLOTS, CHUNKS):
        keep = rest if n < WIDE else pl.ds(0, narrow)
        wait(c0.at[n % SLOTS, :, :, :, :, keep], c0_sem.at[n % SLOTS])


def solution(mesh):
    def local_product(a_blk, b_blk):
        rows, cols = a_blk.shape
        width = cols // BLOCKS
        few = rows // 16
        dma = pltpu.SemaphoreType.DMA
        c_blk = pl.pallas_call(
            kernel,
            name="matmul_3d",
            out_shape=pltpu.VMEM((2, 4, 2, few, cols), jnp.bfloat16),
            in_specs=[pl.BlockSpec(memory_space=pl.ANY)] * 2,
            out_specs=pl.BlockSpec(memory_space=pltpu.VMEM),
            scratch_shapes=[
                pltpu.VMEM((2, 4, 2, few, cols), jnp.bfloat16),
                pltpu.VMEM((4, 2, 4, 2, few, cols), jnp.bfloat16),
                pltpu.VMEM((3, 2, 2, few, cols), jnp.bfloat16),
                pltpu.VMEM((2, 2, 2, few, cols // 2), jnp.bfloat16),
                pltpu.VMEM((2, 2, 2, few, cols // 2), jnp.bfloat16),
                pltpu.VMEM((BLOCKS, 2 * Z_N, rows, width), jnp.bfloat16),
                pltpu.VMEM((BLOCKS, 3, 2, 4, 2, few, width), jnp.float32),
                pltpu.VMEM((SLOTS, 2, 4, 2, few, width), jnp.float32),
                pltpu.VMEM((2, 4, 2, few, width), jnp.float32),
                dma((4,)), dma((Z_SEMS, 7)), dma((BLOCKS // 4,)), dma((CHUNKS,)),
                dma((3, 2, 2)), dma((2, 2)), dma((2, 2)), dma((3, 2)), dma((4, 2, 2)), dma((4, 2)), dma,
                dma((2 * SPLIT + C_SEMS, 3)), dma((BLOCKS // 4,)), dma((SLOTS,)),
            ],
            compiler_params=pltpu.CompilerParams(
                collective_id=0, has_side_effects=True, vmem_limit_bytes=61 * 1024 * 1024
            ),
        )(a_blk.reshape(2, 4, 2, few, cols), b_blk)
        return c_blk.reshape(rows, cols)

    block_spec = P(("row", "depth"), "col")
    return jax.shard_map(local_product, mesh=mesh, in_specs=(block_spec, block_spec), out_specs=block_spec, check_vma=False)
```

```python
import jax
import jax.numpy as jnp
from jax import lax
from jax.experimental import pallas as pl
from jax.experimental.pallas import tpu as pltpu
from jax.sharding import PartitionSpec as P

MESH = pl.DeviceIdType.MESH
X_N, Y_N, Z_N = 4, 4, 8
BLOCKS = 16
SLOTS = 8
LOOP = 8
WIDE = 15
SPLIT = 4
ALL = 2
Z_SEMS, C_SEMS = 4, 3

PROGRAM = (
    "aiiaabjfbiajkjgbifclnfkcljblgcnmmddchlamefkoonhkddoebmgegfpo",
    "anophecothabttopgdtponbqfqcqfhunauecupudgqoaaoobqohegnrndrbp",
    "vrvcffqoehbvcroopgrodgrssasdsfwwhwhcevqasepgsbwpdbraqehfccpq",
    "bgfsdrfqdhcegrasegphdrsbfpaaheqscpqgarbdbhqfcfrecbgpdrdscgfh",
    "seqhdegpspehrpqsqqrrrsss",
)


def chunk(n):
    return (n, None) if n < WIDE else (WIDE + (n - WIDE) // 2, (n - WIDE) % 2)


CHUNKS = WIDE + 2 * (BLOCKS - WIDE)


def kernel(a_hbm, b_hbm, c_out, a_own, a_all, s1, rl1, rl2, b_all, crecv, c0, prod,
           ld_sem, zr_sem, zs_sem, dr_sem, s1_sem, r1_sem, r2_sem, s2_sem, ag_sem, fw_sem, as_sem,
           cr_sem, cs_sem, c0_sem):
    row, y, z = lax.axis_index("row"), lax.axis_index("col"), lax.axis_index("depth")
    x, c = row // 2, row % 2
    width = b_all.shape[3]
    narrow = width // 2
    cols = a_own.shape[4]
    part_cols = (pl.ds(0, cols // 2), pl.ds(cols // 2, cols // 2))
    rest = slice(None)

    def at_x(dx):
        return {"row": 2 * ((x + dx + X_N) % X_N) + c}

    def at_y(dy):
        return {"col": (y + dy + Y_N) % Y_N}

    step = 1 - 2 * c
    z_long = {"depth": (z + step + Z_N) % Z_N}
    z_short = {"depth": (z - step + Z_N) % Z_N}
    partner = {"row": 2 * x + 1 - c}

    def send(src, dst, ssem, rsem, dev):
        pltpu.make_async_remote_copy(src_ref=src, dst_ref=dst, send_sem=ssem, recv_sem=rsem,
                                     device_id=dev, device_id_type=MESH).start()

    def wait(ref, sem):
        pltpu.make_async_copy(ref, ref, sem).wait()

    e_own = (y - x + Y_N) % Y_N
    flip = e_own // 3
    j_own = e_own

    def b_local(m, sem):
        return pltpu.make_async_copy(b_hbm.at[:, pl.ds(pl.multiple_of(m * width, width), width)],
                                     b_all.at[m, c * Z_N + z], ld_sem.at[sem])

    def a_load(r):
        return pltpu.make_async_copy(a_hbm.at[:, :, r], a_own.at[:, :, r], ld_sem.at[2 + r])

    a_load(0).start()
    b_local(0, 0).start()
    a_load(1).start()
    barrier = pltpu.get_barrier_semaphore()
    for dev in (at_x(1), at_x(-1), at_y(1), at_y(-1), z_long, z_short, partner):
        pl.semaphore_signal(barrier, inc=1, device_id=dev, device_id_type=MESH)
    lax.fori_loop(1, BLOCKS, lambda m, _: (b_local(m, 1).start(), 0)[1], 0)

    def quarter_sem(e, o, r):
        return s1_sem.at[(e + 1) % 2 * (2 - e // 2), o, r]

    def by_e(e, o, r, j, part, fn):
        col_part = rest if part is None else part_cols[part]

        @pl.when(e == 0)
        def _():
            fn(a_all.at[3, o, j, r, :, col_part])

        @pl.when(e != 0)
        def _():
            fn(s1.at[(e + Y_N - 1) % Y_N, o, r, :, col_part])

    for o in range(2):
        for r in range(2):
            by_e(e_own, o, r, 0, None, lambda dst: pltpu.make_async_copy(
                a_hbm.at[(o + flip) % 2, 0, r], dst, quarter_sem(e_own, o, r)).start())
    pl.semaphore_wait(barrier, 7)
    loaded = set()

    def ev_s1(o, r):
        if r not in loaded:
            loaded.add(r)
            a_load(r).wait()
        h = (o + flip) % 2
        send(a_own.at[h, 2, r, :, part_cols[0]], rl1.at[0, o, r], as_sem, r1_sem.at[o, r], at_y(1))
        send(a_own.at[h, 2, r, :, part_cols[1]], rl1.at[1, o, r], as_sem, r1_sem.at[o, r], at_y(-1))
        sem = quarter_sem(e_own, o, r)
        by_e(e_own, o, r, 1, None, lambda dst: send(a_own.at[h, 1, r], dst, as_sem, sem, at_y(1)))
        by_e(e_own, o, r, 3, None, lambda dst: send(a_own.at[h, 3, r], dst, as_sem, sem, at_y(-1)))

    def ev_r1(o, r):
        wait(rl1.at[:, o, r], r1_sem.at[o, r])
        for d, dy in ((0, 1), (1, -1)):
            e = (y - dy - x + 2 * Y_N) % Y_N
            by_e(e, o, r, 2, d, lambda dst: send(rl1.at[d, o, r], dst, as_sem, quarter_sem(e, o, r), at_y(dy)))

    def ev_s2(o, r):
        wait(s1.at[pl.ds(0, 2), o, r], quarter_sem(1, o, r))
        g = 2 * o
        j = (y - x - 1 + 2 * Y_N) % Y_N
        send(s1.at[0, o, r], a_all.at[g, o, j, r], as_sem, s2_sem.at[g, r], at_x(1))
        j = (y - x + 1 + Y_N) % Y_N
        send(s1.at[2, o, r], a_all.at[g, 1 - o, j, r], as_sem, s2_sem.at[g, r], at_x(-1))

    def ev_s2f(o, r):
        wait(s1.at[1, o, r], quarter_sem(2, o, r))
        for d in range(2):
            send(s1.at[1, o, r, :, part_cols[d]], rl2.at[d, o, r], as_sem, r2_sem.at[o, r], at_x(1 - 2 * d))

    def ev_r2(o, r):
        wait(rl2.at[:, o, r], r2_sem.at[o, r])
        for d, dx in ((0, 1), (1, -1)):
            j = (y - x - dx + 2 * Y_N) % Y_N
            send(rl2.at[d, o, r], a_all.at[1, o, j, r, :, part_cols[d]], as_sem, s2_sem.at[1, r], at_x(dx))

    def ev_ag(g, r):
        if g == 3:
            for o in range(2):
                wait(a_all.at[g, o, j_own, r], quarter_sem(0, o, r))
        else:
            wait(a_all.at[g, :, j_own, r], s2_sem.at[g, r])
        for d in range(2):
            quarter = a_all.at[g, d, j_own, r]
            send(quarter, quarter, as_sem, ag_sem.at[g, d, r], at_y(1))
            send(quarter, quarter, as_sem, ag_sem.at[g, d, r], at_y(-1))

    def ev_fw(g, r, d):
        wait(a_all.at[0, 0, 0], ag_sem.at[g, d, r])
        for k, dy in ((0, 1), (1, -1)):
            j = (y - dy - x + 2 * Y_N) % Y_N
            part = a_all.at[g, d, j, r, :, part_cols[k]]
            send(part, part, as_sem, fw_sem.at[g, r], at_y(dy))

    def group_complete(g, r):
        wait(a_all.at[0, 0, 0], fw_sem.at[g, r])

    def block(hop):
        return c * Z_N + (z - hop * step + 2 * Z_N) % Z_N

    def lanes_of(n):
        half = chunk(n)[1]
        return rest if half is None else pl.ds(half * narrow, narrow)

    def piece(n, kb):
        return b_all.at[chunk(n)[0], kb, :, lanes_of(n)]

    def hand_over(n, kb):
        send(piece(n, kb), piece(n, kb), zs_sem.at[chunk(n)[0] // 4], dr_sem.at[n], partner)

    def forward_long(n, hop):
        p = piece(n, block(hop))
        send(p, p, zs_sem.at[chunk(n)[0] // 4], zr_sem.at[n % Z_SEMS, hop], z_long)

    def forward_short(n, hop):
        p = piece(n, block(-hop))
        send(p, p, zs_sem.at[chunk(n)[0] // 4], zr_sem.at[n % Z_SEMS, 4 + hop], z_short)

    def ev_own(n):
        if n == 0:
            b_local(0, 0).wait()
        elif n == 1:
            wait(b_all.at[0, pl.ds(0, BLOCKS - 1)], ld_sem.at[1])
        forward_long(n, 0)
        forward_short(n, 0)
        hand_over(n, block(0))

    def ev_long(n, hop):
        wait(piece(n, block(hop)), zr_sem.at[n % Z_SEMS, hop - 1])
        if hop < 4:
            forward_long(n, hop)
        hand_over(n, block(hop))

    def ev_short(n, hop):
        wait(piece(n, block(-hop)), zr_sem.at[n % Z_SEMS, 4 + hop - 1])
        if hop < 3:
            forward_short(n, hop)
        hand_over(n, block(-hop))

    def handed_over(n):
        wait(b_all.at[0, pl.ds(0, Z_N), :, lanes_of(n)], dr_sem.at[n])

    def dot(a, b):
        return jnp.dot(a.reshape(-1, cols), b.reshape(cols, -1), preferred_element_type=jnp.float32)

    def sum_sem(n, q):
        return 2 * SPLIT + (n - SPLIT) % C_SEMS if isinstance(q, slice) else 2 * n + q

    def sum_stage(n, g, q, m, lanes, first, size, when, reuse, old):
        slot = n % SLOTS
        keep = rest if isinstance(lanes, slice) else pl.ds(0, narrow)
        arrivals = sum_sem(n, q)

        def pass_on(src, ssem):
            for d in range(2):
                send(src.at[d], crecv.at[m, g, d, :, q, :, lanes], ssem, cr_sem.at[arrivals, g], at_x(1 - 2 * d))

        def arrived():
            wait(crecv.at[m, g - 1, :, :, q, :, lanes], cr_sem.at[arrivals, g - 1])

        def begin():
            reuse(lambda: wait(c0.at[slot, :, :, :, :, old], c0_sem.at[slot]))
            c0[slot, :, :, q, :, keep] = prod[:, :, q, :, keep]
            pass_on(c0.at[slot, :, :, q, :, keep], c0_sem.at[slot])

        def middle():
            arrived()
            crecv[m, g - 1, :, :, q, :, lanes] += prod[:, :, q, :, keep]
            pass_on(crecv.at[m, g - 1, :, :, q, :, lanes], cs_sem.at[m // 4])

        def end():
            arrived()
            total = crecv[m, g - 1, :, :, q, :, lanes] + prod[:, :, q, :, keep]
            c_out[:, :, q, :, pl.ds(pl.multiple_of(first, size), size)] = total.astype(c_out.dtype)

        a = a_all[g, :, :, q]
        prod[:, :, q, :, keep] = dot(a, b_all[m, :, :, lanes]).reshape(a.shape[:-1] + (size,))
        when(g == 0, begin)
        when((g == 1) | (g == 2), middle)
        when(g == 3, end)

    def branch(cond, fn):
        pl.when(cond)(fn)

    def fixed(cond, fn):
        if cond:
            fn()

    def sum_loop(code, split, wide):
        n, g, q = code // 8, code // 2 % 4, code % 2
        if split:
            pl.when(n < SPLIT)(lambda: sum_stage(n, g, q, n, rest, n * width, width, branch, lambda fn: None, rest))
        if wide:
            pl.when(n >= SPLIT)(lambda: sum_stage(n, g, rest, n, rest, n * width, width, branch,
                                                  pl.when(n >= SLOTS), rest))

    def sum_narrow(n, g):
        m, half = chunk(n)
        old = rest if n - SLOTS < WIDE else pl.ds(0, narrow)
        sum_stage(n, g, rest, m, lanes_of(n), m * width + half * narrow, narrow, fixed, lambda fn: fn(), old)

    chunks = range(CHUNKS)
    queues = {"a": [(ev_own, (n,)) for n in chunks]}
    for hop in range(1, 5):
        queues["abcde"[hop]] = [(ev_long, (n, hop)) for n in chunks]
    for hop in range(1, 4):
        queues["efgh"[hop]] = [(ev_short, (n, hop)) for n in chunks]
    by_half = [(o, r) for o in range(2) for r in range(2)]
    by_row = [(o, r) for r in range(2) for o in range(2)]
    queues["i"] = [(ev_s1, p) for p in by_half]
    queues["j"] = [(ev_r1, p) for p in by_half]
    queues["k"] = [(ev_s2, p) for p in by_half]
    queues["l"] = [(ev_s2f, p) for p in by_row]
    queues["m"] = [(ev_r2, p) for p in by_row]
    groups = [(g, r) for g in range(4) for r in range(2)]
    queues["n"] = [(ev_ag, p) for p in groups]
    queues["o"] = [(ev_fw, p + (d,)) for p in groups for d in range(2)]
    for g in range(4):
        queues["pqrs"[g]] = [(None, (n, g, 0 if n < SPLIT else ALL)) for n in chunks]
        queues["tuvw"[g]] = [(None, (n, g, 1)) for n in range(SPLIT)]

    steps, before, complete, handed = [], [], set(), set()
    for letter in "".join(PROGRAM):
        fn, args = queues[letter].pop(0)
        if fn is not None:
            before.append((fn, args))
            continue
        n, g, q = args
        for r in (range(2) if q == ALL else (q,)):
            if (g, r) not in complete:
                complete.add((g, r))
                before.append((group_complete, (g, r)))
        if n not in handed:
            handed.add(n)
            before.append((handed_over, (n,)))
        if n >= WIDE:
            before.append((sum_narrow, (n, g)))
        else:
            steps.append((before, (n * 4 + g) * 2 + q % 2, q != ALL))
            before = []

    def run(todo):
        for fn, args in todo:
            fn(*args)

    def in_loop(first, last):
        part = steps[first:last]

        def body(k, carry):
            code = part[0][1]
            for i, (todo, this, _) in enumerate(part):
                code = jnp.where(k == first + i, this, code)
                if todo:
                    pl.when(k == first + i)(lambda: run(todo))
            sum_loop(code, any(s for _, _, s in part), any(not s for _, _, s in part))
            return carry

        lax.fori_loop(first, last, body, 0)

    for first in range(0, len(steps), LOOP):
        in_loop(first, min(first + LOOP, len(steps)))
    run(before)

    for i in range(BLOCKS // 4):
        wait(b_all.at[pl.ds(0, 4), pl.ds(0, 15)], zs_sem.at[i])
        wait(crecv.at[pl.ds(0, 4), pl.ds(0, 2)], cs_sem.at[i])
    wait(b_all.at[pl.ds(0, 5)], as_sem)
    for n in range(CHUNKS - SLOTS, CHUNKS):
        keep = rest if n < WIDE else pl.ds(0, narrow)
        wait(c0.at[n % SLOTS, :, :, :, :, keep], c0_sem.at[n % SLOTS])


def solution(mesh):
    def local_product(a_blk, b_blk):
        rows, cols = a_blk.shape
        width = cols // BLOCKS
        few = rows // 16
        dma = pltpu.SemaphoreType.DMA
        c_blk = pl.pallas_call(
            kernel,
            name="matmul_3d",
            out_shape=pltpu.VMEM((2, 4, 2, few, cols), jnp.bfloat16),
            in_specs=[pl.BlockSpec(memory_space=pl.ANY)] * 2,
            out_specs=pl.BlockSpec(memory_space=pltpu.VMEM),
            scratch_shapes=[
                pltpu.VMEM((2, 4, 2, few, cols), jnp.bfloat16),
                pltpu.VMEM((4, 2, 4, 2, few, cols), jnp.bfloat16),
                pltpu.VMEM((3, 2, 2, few, cols), jnp.bfloat16),
                pltpu.VMEM((2, 2, 2, few, cols // 2), jnp.bfloat16),
                pltpu.VMEM((2, 2, 2, few, cols // 2), jnp.bfloat16),
                pltpu.VMEM((BLOCKS, 2 * Z_N, rows, width), jnp.bfloat16),
                pltpu.VMEM((BLOCKS, 3, 2, 4, 2, few, width), jnp.float32),
                pltpu.VMEM((SLOTS, 2, 4, 2, few, width), jnp.float32),
                pltpu.VMEM((2, 4, 2, few, width), jnp.float32),
                dma((4,)), dma((Z_SEMS, 7)), dma((BLOCKS // 4,)), dma((CHUNKS,)),
                dma((3, 2, 2)), dma((2, 2)), dma((2, 2)), dma((3, 2)), dma((4, 2, 2)), dma((4, 2)), dma,
                dma((2 * SPLIT + C_SEMS, 3)), dma((BLOCKS // 4,)), dma((SLOTS,)),
            ],
            compiler_params=pltpu.CompilerParams(
                collective_id=0, has_side_effects=True, vmem_limit_bytes=61 * 1024 * 1024
            ),
        )(a_blk.reshape(2, 4, 2, few, cols), b_blk)
        return c_blk.reshape(rows, cols)

    block_spec = P(("row", "depth"), "col")
    return jax.shard_map(local_product, mesh=mesh, in_specs=(block_spec, block_spec), out_specs=block_spec, check_vma=False)
```

```python
import jax
import jax.numpy as jnp
from jax import lax
from jax.experimental import pallas as pl
from jax.experimental.pallas import tpu as pltpu
from jax.sharding import PartitionSpec as P

MESH = pl.DeviceIdType.MESH
X_N, Y_N, Z_N = 4, 4, 8
BLOCKS = 16
SLOTS = 8
LOOP = 8
WIDE = 16
SPLIT = 4
ALL = 2
Z_SEMS, C_SEMS = 5, 3

PROGRAM = (
    "aiaiabjiajbaicbjffklkcbjnlkgfdlmdnlmocfmchbomggoedeodnpgkfat",
    "ancheohhpetbtootgppondbqfqqhcaeuungpudoucbfaoqheoqondpgfrfrc",
    "vnbvoheaqoprdvgcovrbroaressgswdwwfwhcsqhasepgbsdpbrfhaqcecpq",
    "gbfsdrqdchfregsapedhgraspbaehfqspqcbrgdcqfhebfrdgpsrcsehgqdp",
    "hserpqsqrrss",
)


def chunk(n):
    return (n, None) if n < WIDE else (WIDE + (n - WIDE) // 2, (n - WIDE) % 2)


CHUNKS = WIDE + 2 * (BLOCKS - WIDE)


def kernel(a_hbm, b_hbm, c_out, a_own, a_all, s1, rl1, rl2, b_all, crecv, c0, prod,
           ld_sem, zr_sem, zs_sem, dr_sem, s1_sem, r1_sem, r2_sem, s2_sem, ag_sem, fw_sem, as_sem,
           cr_sem, cs_sem, c0_sem):
    row, y, z = lax.axis_index("row"), lax.axis_index("col"), lax.axis_index("depth")
    x, c = row // 2, row % 2
    width = b_all.shape[3]
    narrow = width // 2
    cols = a_own.shape[4]
    part_cols = (pl.ds(0, cols // 2), pl.ds(cols // 2, cols // 2))
    rest = slice(None)

    def at_x(dx):
        return {"row": 2 * ((x + dx + X_N) % X_N) + c}

    def at_y(dy):
        return {"col": (y + dy + Y_N) % Y_N}

    step = 1 - 2 * c
    z_long = {"depth": (z + step + Z_N) % Z_N}
    z_short = {"depth": (z - step + Z_N) % Z_N}
    partner = {"row": 2 * x + 1 - c}

    def send(src, dst, ssem, rsem, dev):
        pltpu.make_async_remote_copy(src_ref=src, dst_ref=dst, send_sem=ssem, recv_sem=rsem,
                                     device_id=dev, device_id_type=MESH).start()

    def wait(ref, sem):
        pltpu.make_async_copy(ref, ref, sem).wait()

    e_own = (y - x + Y_N) % Y_N
    flip = e_own // 3
    j_own = e_own

    def b_local(m, sem):
        return pltpu.make_async_copy(b_hbm.at[:, pl.ds(pl.multiple_of(m * width, width), width)],
                                     b_all.at[m, c * Z_N + z], ld_sem.at[sem])

    def a_load(r):
        return pltpu.make_async_copy(a_hbm.at[:, :, r], a_own.at[:, :, r], ld_sem.at[2 + r])

    a_load(0).start()
    b_local(0, 0).start()
    a_load(1).start()
    barrier = pltpu.get_barrier_semaphore()
    for dev in (at_x(1), at_x(-1), at_y(1), at_y(-1), z_long, z_short, partner):
        pl.semaphore_signal(barrier, inc=1, device_id=dev, device_id_type=MESH)
    lax.fori_loop(1, BLOCKS, lambda m, _: (b_local(m, 1).start(), 0)[1], 0)

    def quarter_sem(e, o, r):
        return s1_sem.at[(e + 1) % 2 * (2 - e // 2), o, r]

    def by_e(e, o, r, j, part, fn):
        col_part = rest if part is None else part_cols[part]

        @pl.when(e == 0)
        def _():
            fn(a_all.at[3, o, j, r, :, col_part])

        @pl.when(e != 0)
        def _():
            fn(s1.at[(e + Y_N - 1) % Y_N, o, r, :, col_part])

    for o in range(2):
        for r in range(2):
            by_e(e_own, o, r, 0, None, lambda dst: pltpu.make_async_copy(
                a_hbm.at[(o + flip) % 2, 0, r], dst, quarter_sem(e_own, o, r)).start())
    pl.semaphore_wait(barrier, 7)
    loaded = set()

    def ev_s1(o, r):
        if r not in loaded:
            loaded.add(r)
            a_load(r).wait()
        h = (o + flip) % 2
        send(a_own.at[h, 2, r, :, part_cols[0]], rl1.at[0, o, r], as_sem, r1_sem.at[o, r], at_y(1))
        send(a_own.at[h, 2, r, :, part_cols[1]], rl1.at[1, o, r], as_sem, r1_sem.at[o, r], at_y(-1))
        sem = quarter_sem(e_own, o, r)
        by_e(e_own, o, r, 1, None, lambda dst: send(a_own.at[h, 1, r], dst, as_sem, sem, at_y(1)))
        by_e(e_own, o, r, 3, None, lambda dst: send(a_own.at[h, 3, r], dst, as_sem, sem, at_y(-1)))

    def ev_r1(o, r):
        wait(rl1.at[:, o, r], r1_sem.at[o, r])
        for d, dy in ((0, 1), (1, -1)):
            e = (y - dy - x + 2 * Y_N) % Y_N
            by_e(e, o, r, 2, d, lambda dst: send(rl1.at[d, o, r], dst, as_sem, quarter_sem(e, o, r), at_y(dy)))

    def ev_s2(o, r):
        wait(s1.at[pl.ds(0, 2), o, r], quarter_sem(1, o, r))
        g = 2 * o
        j = (y - x - 1 + 2 * Y_N) % Y_N
        send(s1.at[0, o, r], a_all.at[g, o, j, r], as_sem, s2_sem.at[g, r], at_x(1))
        j = (y - x + 1 + Y_N) % Y_N
        send(s1.at[2, o, r], a_all.at[g, 1 - o, j, r], as_sem, s2_sem.at[g, r], at_x(-1))

    def ev_s2f(o, r):
        wait(s1.at[1, o, r], quarter_sem(2, o, r))
        for d in range(2):
            send(s1.at[1, o, r, :, part_cols[d]], rl2.at[d, o, r], as_sem, r2_sem.at[o, r], at_x(1 - 2 * d))

    def ev_r2(o, r):
        wait(rl2.at[:, o, r], r2_sem.at[o, r])
        for d, dx in ((0, 1), (1, -1)):
            j = (y - x - dx + 2 * Y_N) % Y_N
            send(rl2.at[d, o, r], a_all.at[1, o, j, r, :, part_cols[d]], as_sem, s2_sem.at[1, r], at_x(dx))

    def ev_ag(g, r):
        if g == 3:
            for o in range(2):
                wait(a_all.at[g, o, j_own, r], quarter_sem(0, o, r))
        else:
            wait(a_all.at[g, :, j_own, r], s2_sem.at[g, r])
        for d in range(2):
            quarter = a_all.at[g, d, j_own, r]
            send(quarter, quarter, as_sem, ag_sem.at[g, d, r], at_y(1))
            send(quarter, quarter, as_sem, ag_sem.at[g, d, r], at_y(-1))

    def ev_fw(g, r, d):
        wait(a_all.at[0, 0, 0], ag_sem.at[g, d, r])
        for k, dy in ((0, 1), (1, -1)):
            j = (y - dy - x + 2 * Y_N) % Y_N
            part = a_all.at[g, d, j, r, :, part_cols[k]]
            send(part, part, as_sem, fw_sem.at[g, r], at_y(dy))

    def group_complete(g, r):
        wait(a_all.at[0, 0, 0], fw_sem.at[g, r])

    def block(hop):
        return c * Z_N + (z - hop * step + 2 * Z_N) % Z_N

    def lanes_of(n):
        half = chunk(n)[1]
        return rest if half is None else pl.ds(half * narrow, narrow)

    def piece(n, kb):
        return b_all.at[chunk(n)[0], kb, :, lanes_of(n)]

    def hand_over(n, kb):
        send(piece(n, kb), piece(n, kb), zs_sem.at[chunk(n)[0] // 4], dr_sem.at[n], partner)

    def forward_long(n, hop):
        p = piece(n, block(hop))
        send(p, p, zs_sem.at[chunk(n)[0] // 4], zr_sem.at[n % Z_SEMS, hop], z_long)

    def forward_short(n, hop):
        p = piece(n, block(-hop))
        send(p, p, zs_sem.at[chunk(n)[0] // 4], zr_sem.at[n % Z_SEMS, 4 + hop], z_short)

    def ev_own(n):
        if n == 0:
            b_local(0, 0).wait()
        elif n == 1:
            wait(b_all.at[0, pl.ds(0, BLOCKS - 1)], ld_sem.at[1])
        forward_long(n, 0)
        forward_short(n, 0)
        hand_over(n, block(0))

    def ev_long(n, hop):
        wait(piece(n, block(hop)), zr_sem.at[n % Z_SEMS, hop - 1])
        if hop < 4:
            forward_long(n, hop)
        hand_over(n, block(hop))

    def ev_short(n, hop):
        wait(piece(n, block(-hop)), zr_sem.at[n % Z_SEMS, 4 + hop - 1])
        if hop < 3:
            forward_short(n, hop)
        hand_over(n, block(-hop))

    def handed_over(n):
        wait(b_all.at[0, pl.ds(0, Z_N), :, lanes_of(n)], dr_sem.at[n])

    def dot(a, b):
        return jnp.dot(a.reshape(-1, cols), b.reshape(cols, -1), preferred_element_type=jnp.float32)

    def sum_sem(n, q):
        return 2 * SPLIT + (n - SPLIT) % C_SEMS if isinstance(q, slice) else 2 * n + q

    def sum_stage(n, g, q, m, lanes, first, size, when, reuse, old):
        slot = n % SLOTS
        keep = rest if isinstance(lanes, slice) else pl.ds(0, narrow)
        arrivals = sum_sem(n, q)

        def pass_on(src, ssem):
            for d in range(2):
                send(src.at[d], crecv.at[m, g, d, :, q, :, lanes], ssem, cr_sem.at[arrivals, g], at_x(1 - 2 * d))

        def arrived():
            wait(crecv.at[m, g - 1, :, :, q, :, lanes], cr_sem.at[arrivals, g - 1])

        def begin():
            reuse(lambda: wait(c0.at[slot, :, :, :, :, old], c0_sem.at[slot]))
            c0[slot, :, :, q, :, keep] = prod[:, :, q, :, keep]
            pass_on(c0.at[slot, :, :, q, :, keep], c0_sem.at[slot])

        def middle():
            arrived()
            crecv[m, g - 1, :, :, q, :, lanes] += prod[:, :, q, :, keep]
            pass_on(crecv.at[m, g - 1, :, :, q, :, lanes], cs_sem.at[m // 4])

        def end():
            arrived()
            total = crecv[m, g - 1, :, :, q, :, lanes] + prod[:, :, q, :, keep]
            c_out[:, :, q, :, pl.ds(pl.multiple_of(first, size), size)] = total.astype(c_out.dtype)

        a = a_all[g, :, :, q]
        prod[:, :, q, :, keep] = dot(a, b_all[m, :, :, lanes]).reshape(a.shape[:-1] + (size,))
        when(g == 0, begin)
        when((g == 1) | (g == 2), middle)
        when(g == 3, end)

    def branch(cond, fn):
        pl.when(cond)(fn)

    def fixed(cond, fn):
        if cond:
            fn()

    def sum_loop(code, split, wide):
        n, g, q = code // 8, code // 2 % 4, code % 2
        if split:
            pl.when(n < SPLIT)(lambda: sum_stage(n, g, q, n, rest, n * width, width, branch, lambda fn: None, rest))
        if wide:
            pl.when(n >= SPLIT)(lambda: sum_stage(n, g, rest, n, rest, n * width, width, branch,
                                                  pl.when(n >= SLOTS), rest))

    def sum_narrow(n, g):
        m, half = chunk(n)
        old = rest if n - SLOTS < WIDE else pl.ds(0, narrow)
        sum_stage(n, g, rest, m, lanes_of(n), m * width + half * narrow, narrow, fixed, lambda fn: fn(), old)

    chunks = range(CHUNKS)
    queues = {"a": [(ev_own, (n,)) for n in chunks]}
    for hop in range(1, 5):
        queues["abcde"[hop]] = [(ev_long, (n, hop)) for n in chunks]
    for hop in range(1, 4):
        queues["efgh"[hop]] = [(ev_short, (n, hop)) for n in chunks]
    by_half = [(o, r) for o in range(2) for r in range(2)]
    by_row = [(o, r) for r in range(2) for o in range(2)]
    queues["i"] = [(ev_s1, p) for p in by_half]
    queues["j"] = [(ev_r1, p) for p in by_half]
    queues["k"] = [(ev_s2, p) for p in by_half]
    queues["l"] = [(ev_s2f, p) for p in by_row]
    queues["m"] = [(ev_r2, p) for p in by_row]
    groups = [(g, r) for g in range(4) for r in range(2)]
    queues["n"] = [(ev_ag, p) for p in groups]
    queues["o"] = [(ev_fw, p + (d,)) for p in groups for d in range(2)]
    for g in range(4):
        queues["pqrs"[g]] = [(None, (n, g, 0 if n < SPLIT else ALL)) for n in chunks]
        queues["tuvw"[g]] = [(None, (n, g, 1)) for n in range(SPLIT)]

    steps, before, complete, handed = [], [], set(), set()
    for letter in "".join(PROGRAM):
        fn, args = queues[letter].pop(0)
        if fn is not None:
            before.append((fn, args))
            continue
        n, g, q = args
        for r in (range(2) if q == ALL else (q,)):
            if (g, r) not in complete:
                complete.add((g, r))
                before.append((group_complete, (g, r)))
        if n not in handed:
            handed.add(n)
            before.append((handed_over, (n,)))
        if n >= WIDE:
            before.append((sum_narrow, (n, g)))
        else:
            steps.append((before, (n * 4 + g) * 2 + q % 2, q != ALL))
            before = []

    def run(todo):
        for fn, args in todo:
            fn(*args)

    def in_loop(first, last):
        part = steps[first:last]

        def body(k, carry):
            code = part[0][1]
            for i, (todo, this, _) in enumerate(part):
                code = jnp.where(k == first + i, this, code)
                if todo:
                    pl.when(k == first + i)(lambda: run(todo))
            sum_loop(code, any(s for _, _, s in part), any(not s for _, _, s in part))
            return carry

        lax.fori_loop(first, last, body, 0)

    for first in range(0, len(steps), LOOP):
        in_loop(first, min(first + LOOP, len(steps)))
    run(before)

    for i in range(BLOCKS // 4):
        wait(b_all.at[pl.ds(0, 4), pl.ds(0, 15)], zs_sem.at[i])
        wait(crecv.at[pl.ds(0, 4), pl.ds(0, 2)], cs_sem.at[i])
    wait(b_all.at[pl.ds(0, 5)], as_sem)
    for n in range(CHUNKS - SLOTS, CHUNKS):
        keep = rest if n < WIDE else pl.ds(0, narrow)
        wait(c0.at[n % SLOTS, :, :, :, :, keep], c0_sem.at[n % SLOTS])


def solution(mesh):
    def local_product(a_blk, b_blk):
        rows, cols = a_blk.shape
        width = cols // BLOCKS
        few = rows // 16
        dma = pltpu.SemaphoreType.DMA
        c_blk = pl.pallas_call(
            kernel,
            name="matmul_3d",
            out_shape=pltpu.VMEM((2, 4, 2, few, cols), jnp.bfloat16),
            in_specs=[pl.BlockSpec(memory_space=pl.ANY)] * 2,
            out_specs=pl.BlockSpec(memory_space=pltpu.VMEM),
            scratch_shapes=[
                pltpu.VMEM((2, 4, 2, few, cols), jnp.bfloat16),
                pltpu.VMEM((4, 2, 4, 2, few, cols), jnp.bfloat16),
                pltpu.VMEM((3, 2, 2, few, cols), jnp.bfloat16),
                pltpu.VMEM((2, 2, 2, few, cols // 2), jnp.bfloat16),
                pltpu.VMEM((2, 2, 2, few, cols // 2), jnp.bfloat16),
                pltpu.VMEM((BLOCKS, 2 * Z_N, rows, width), jnp.bfloat16),
                pltpu.VMEM((BLOCKS, 3, 2, 4, 2, few, width), jnp.float32),
                pltpu.VMEM((SLOTS, 2, 4, 2, few, width), jnp.float32),
                pltpu.VMEM((2, 4, 2, few, width), jnp.float32),
                dma((4,)), dma((Z_SEMS, 7)), dma((BLOCKS // 4,)), dma((CHUNKS,)),
                dma((3, 2, 2)), dma((2, 2)), dma((2, 2)), dma((3, 2)), dma((4, 2, 2)), dma((4, 2)), dma,
                dma((2 * SPLIT + C_SEMS, 3)), dma((BLOCKS // 4,)), dma((SLOTS,)),
            ],
            compiler_params=pltpu.CompilerParams(
                collective_id=0, has_side_effects=True, vmem_limit_bytes=61 * 1024 * 1024
            ),
        )(a_blk.reshape(2, 4, 2, few, cols), b_blk)
        return c_blk.reshape(rows, cols)

    block_spec = P(("row", "depth"), "col")
    return jax.shard_map(local_product, mesh=mesh, in_specs=(block_spec, block_spec), out_specs=block_spec, check_vma=False)
```

```python
import jax
import jax.numpy as jnp
from jax import lax
from jax.experimental import pallas as pl
from jax.experimental.pallas import tpu as pltpu
from jax.sharding import PartitionSpec as P

MESH = pl.DeviceIdType.MESH
X_N, Y_N, Z_N = 4, 4, 8
BLOCKS = 16
SLOTS = 8
LOOP = 8
WIDE = 15
SPLIT = 4
ALL = 2
Z_SEMS, C_SEMS = 4, 3

PROGRAM = (
    "aiaiajbjibffcbijkkafgjnclcbdnlhdllamkmcogogfmdomekohnbdehgpt",
    "feanohpctpebotaodpotgnfqbnqqcehfuaupdugoqoacnuobgqeoahrrpdno",
    "rcrbhbvffeoqrcvvdpgoovfssdsgsrehawwcweqahpwgsbsdpbraqcehfcpq",
    "bgfsrdqdfchregsaegprhdsbfpaaheqscpqgarbdbhqffrcecbgpdrdsgfch",
    "seqehdgpspehrpqsqqrrrsss",
)


def chunk(n):
    return (n, None) if n < WIDE else (WIDE + (n - WIDE) // 2, (n - WIDE) % 2)


CHUNKS = WIDE + 2 * (BLOCKS - WIDE)


def kernel(a_hbm, b_hbm, c_out, a_own, a_all, s1, rl1, rl2, b_all, crecv, c0, prod,
           ld_sem, zr_sem, zs_sem, dr_sem, s1_sem, r1_sem, r2_sem, s2_sem, ag_sem, fw_sem, as_sem,
           cr_sem, cs_sem, c0_sem):
    row, y, z = lax.axis_index("row"), lax.axis_index("col"), lax.axis_index("depth")
    x, c = row // 2, row % 2
    width = b_all.shape[3]
    narrow = width // 2
    cols = a_own.shape[4]
    part_cols = (pl.ds(0, cols // 2), pl.ds(cols // 2, cols // 2))
    rest = slice(None)

    def at_x(dx):
        return {"row": 2 * ((x + dx + X_N) % X_N) + c}

    def at_y(dy):
        return {"col": (y + dy + Y_N) % Y_N}

    step = 1 - 2 * c
    z_long = {"depth": (z + step + Z_N) % Z_N}
    z_short = {"depth": (z - step + Z_N) % Z_N}
    partner = {"row": 2 * x + 1 - c}

    def send(src, dst, ssem, rsem, dev):
        pltpu.make_async_remote_copy(src_ref=src, dst_ref=dst, send_sem=ssem, recv_sem=rsem,
                                     device_id=dev, device_id_type=MESH).start()

    def wait(ref, sem):
        pltpu.make_async_copy(ref, ref, sem).wait()

    e_own = (y - x + Y_N) % Y_N
    flip = e_own // 3
    j_own = e_own

    def b_local(m, sem):
        return pltpu.make_async_copy(b_hbm.at[:, pl.ds(pl.multiple_of(m * width, width), width)],
                                     b_all.at[m, c * Z_N + z], ld_sem.at[sem])

    def a_load(r):
        return pltpu.make_async_copy(a_hbm.at[:, :, r], a_own.at[:, :, r], ld_sem.at[2 + r])

    a_load(0).start()
    b_local(0, 0).start()
    a_load(1).start()
    barrier = pltpu.get_barrier_semaphore()
    for dev in (at_x(1), at_x(-1), at_y(1), at_y(-1), z_long, z_short, partner):
        pl.semaphore_signal(barrier, inc=1, device_id=dev, device_id_type=MESH)
    lax.fori_loop(1, BLOCKS, lambda m, _: (b_local(m, 1).start(), 0)[1], 0)

    def quarter_sem(e, o, r):
        return s1_sem.at[(e + 1) % 2 * (2 - e // 2), o, r]

    def by_e(e, o, r, j, part, fn):
        col_part = rest if part is None else part_cols[part]

        @pl.when(e == 0)
        def _():
            fn(a_all.at[3, o, j, r, :, col_part])

        @pl.when(e != 0)
        def _():
            fn(s1.at[(e + Y_N - 1) % Y_N, o, r, :, col_part])

    for o in range(2):
        for r in range(2):
            by_e(e_own, o, r, 0, None, lambda dst: pltpu.make_async_copy(
                a_hbm.at[(o + flip) % 2, 0, r], dst, quarter_sem(e_own, o, r)).start())
    pl.semaphore_wait(barrier, 7)
    loaded = set()

    def ev_s1(o, r):
        if r not in loaded:
            loaded.add(r)
            a_load(r).wait()
        h = (o + flip) % 2
        send(a_own.at[h, 2, r, :, part_cols[0]], rl1.at[0, o, r], as_sem, r1_sem.at[o, r], at_y(1))
        send(a_own.at[h, 2, r, :, part_cols[1]], rl1.at[1, o, r], as_sem, r1_sem.at[o, r], at_y(-1))
        sem = quarter_sem(e_own, o, r)
        by_e(e_own, o, r, 1, None, lambda dst: send(a_own.at[h, 1, r], dst, as_sem, sem, at_y(1)))
        by_e(e_own, o, r, 3, None, lambda dst: send(a_own.at[h, 3, r], dst, as_sem, sem, at_y(-1)))

    def ev_r1(o, r):
        wait(rl1.at[:, o, r], r1_sem.at[o, r])
        for d, dy in ((0, 1), (1, -1)):
            e = (y - dy - x + 2 * Y_N) % Y_N
            by_e(e, o, r, 2, d, lambda dst: send(rl1.at[d, o, r], dst, as_sem, quarter_sem(e, o, r), at_y(dy)))

    def ev_s2(o, r):
        wait(s1.at[pl.ds(0, 2), o, r], quarter_sem(1, o, r))
        g = 2 * o
        j = (y - x - 1 + 2 * Y_N) % Y_N
        send(s1.at[0, o, r], a_all.at[g, o, j, r], as_sem, s2_sem.at[g, r], at_x(1))
        j = (y - x + 1 + Y_N) % Y_N
        send(s1.at[2, o, r], a_all.at[g, 1 - o, j, r], as_sem, s2_sem.at[g, r], at_x(-1))

    def ev_s2f(o, r):
        wait(s1.at[1, o, r], quarter_sem(2, o, r))
        for d in range(2):
            send(s1.at[1, o, r, :, part_cols[d]], rl2.at[d, o, r], as_sem, r2_sem.at[o, r], at_x(1 - 2 * d))

    def ev_r2(o, r):
        wait(rl2.at[:, o, r], r2_sem.at[o, r])
        for d, dx in ((0, 1), (1, -1)):
            j = (y - x - dx + 2 * Y_N) % Y_N
            send(rl2.at[d, o, r], a_all.at[1, o, j, r, :, part_cols[d]], as_sem, s2_sem.at[1, r], at_x(dx))

    def ev_ag(g, r):
        if g == 3:
            for o in range(2):
                wait(a_all.at[g, o, j_own, r], quarter_sem(0, o, r))
        else:
            wait(a_all.at[g, :, j_own, r], s2_sem.at[g, r])
        for d in range(2):
            quarter = a_all.at[g, d, j_own, r]
            send(quarter, quarter, as_sem, ag_sem.at[g, d, r], at_y(1))
            send(quarter, quarter, as_sem, ag_sem.at[g, d, r], at_y(-1))

    def ev_fw(g, r, d):
        wait(a_all.at[0, 0, 0], ag_sem.at[g, d, r])
        for k, dy in ((0, 1), (1, -1)):
            j = (y - dy - x + 2 * Y_N) % Y_N
            part = a_all.at[g, d, j, r, :, part_cols[k]]
            send(part, part, as_sem, fw_sem.at[g, r], at_y(dy))

    def group_complete(g, r):
        wait(a_all.at[0, 0, 0], fw_sem.at[g, r])

    def block(hop):
        return c * Z_N + (z - hop * step + 2 * Z_N) % Z_N

    def lanes_of(n):
        half = chunk(n)[1]
        return rest if half is None else pl.ds(half * narrow, narrow)

    def piece(n, kb):
        return b_all.at[chunk(n)[0], kb, :, lanes_of(n)]

    def hand_over(n, kb):
        send(piece(n, kb), piece(n, kb), zs_sem.at[chunk(n)[0] // 4], dr_sem.at[n], partner)

    def forward_long(n, hop):
        p = piece(n, block(hop))
        send(p, p, zs_sem.at[chunk(n)[0] // 4], zr_sem.at[n % Z_SEMS, hop], z_long)

    def forward_short(n, hop):
        p = piece(n, block(-hop))
        send(p, p, zs_sem.at[chunk(n)[0] // 4], zr_sem.at[n % Z_SEMS, 4 + hop], z_short)

    def ev_own(n):
        if n == 0:
            b_local(0, 0).wait()
        elif n == 1:
            wait(b_all.at[0, pl.ds(0, BLOCKS - 1)], ld_sem.at[1])
        forward_long(n, 0)
        forward_short(n, 0)
        hand_over(n, block(0))

    def ev_long(n, hop):
        wait(piece(n, block(hop)), zr_sem.at[n % Z_SEMS, hop - 1])
        if hop < 4:
            forward_long(n, hop)
        hand_over(n, block(hop))

    def ev_short(n, hop):
        wait(piece(n, block(-hop)), zr_sem.at[n % Z_SEMS, 4 + hop - 1])
        if hop < 3:
            forward_short(n, hop)
        hand_over(n, block(-hop))

    def handed_over(n):
        wait(b_all.at[0, pl.ds(0, Z_N), :, lanes_of(n)], dr_sem.at[n])

    def dot(a, b):
        return jnp.dot(a.reshape(-1, cols), b.reshape(cols, -1), preferred_element_type=jnp.float32)

    def sum_sem(n, q):
        return 2 * SPLIT + (n - SPLIT) % C_SEMS if isinstance(q, slice) else 2 * n + q

    def sum_stage(n, g, q, m, lanes, first, size, when, reuse, old):
        slot = n % SLOTS
        keep = rest if isinstance(lanes, slice) else pl.ds(0, narrow)
        arrivals = sum_sem(n, q)

        def pass_on(src, ssem):
            for d in range(2):
                send(src.at[d], crecv.at[m, g, d, :, q, :, lanes], ssem, cr_sem.at[arrivals, g], at_x(1 - 2 * d))

        def arrived():
            wait(crecv.at[m, g - 1, :, :, q, :, lanes], cr_sem.at[arrivals, g - 1])

        def begin():
            reuse(lambda: wait(c0.at[slot, :, :, :, :, old], c0_sem.at[slot]))
            c0[slot, :, :, q, :, keep] = prod[:, :, q, :, keep]
            pass_on(c0.at[slot, :, :, q, :, keep], c0_sem.at[slot])

        def middle():
            arrived()
            crecv[m, g - 1, :, :, q, :, lanes] += prod[:, :, q, :, keep]
            pass_on(crecv.at[m, g - 1, :, :, q, :, lanes], cs_sem.at[m // 4])

        def end():
            arrived()
            total = crecv[m, g - 1, :, :, q, :, lanes] + prod[:, :, q, :, keep]
            c_out[:, :, q, :, pl.ds(pl.multiple_of(first, size), size)] = total.astype(c_out.dtype)

        a = a_all[g, :, :, q]
        prod[:, :, q, :, keep] = dot(a, b_all[m, :, :, lanes]).reshape(a.shape[:-1] + (size,))
        when(g == 0, begin)
        when((g == 1) | (g == 2), middle)
        when(g == 3, end)

    def branch(cond, fn):
        pl.when(cond)(fn)

    def fixed(cond, fn):
        if cond:
            fn()

    def sum_loop(code, split, wide):
        n, g, q = code // 8, code // 2 % 4, code % 2
        if split:
            pl.when(n < SPLIT)(lambda: sum_stage(n, g, q, n, rest, n * width, width, branch, lambda fn: None, rest))
        if wide:
            pl.when(n >= SPLIT)(lambda: sum_stage(n, g, rest, n, rest, n * width, width, branch,
                                                  pl.when(n >= SLOTS), rest))

    def sum_narrow(n, g):
        m, half = chunk(n)
        old = rest if n - SLOTS < WIDE else pl.ds(0, narrow)
        sum_stage(n, g, rest, m, lanes_of(n), m * width + half * narrow, narrow, fixed, lambda fn: fn(), old)

    chunks = range(CHUNKS)
    queues = {"a": [(ev_own, (n,)) for n in chunks]}
    for hop in range(1, 5):
        queues["abcde"[hop]] = [(ev_long, (n, hop)) for n in chunks]
    for hop in range(1, 4):
        queues["efgh"[hop]] = [(ev_short, (n, hop)) for n in chunks]
    by_half = [(o, r) for o in range(2) for r in range(2)]
    by_row = [(o, r) for r in range(2) for o in range(2)]
    queues["i"] = [(ev_s1, p) for p in by_half]
    queues["j"] = [(ev_r1, p) for p in by_half]
    queues["k"] = [(ev_s2, p) for p in by_half]
    queues["l"] = [(ev_s2f, p) for p in by_row]
    queues["m"] = [(ev_r2, p) for p in by_row]
    groups = [(g, r) for g in range(4) for r in range(2)]
    queues["n"] = [(ev_ag, p) for p in groups]
    queues["o"] = [(ev_fw, p + (d,)) for p in groups for d in range(2)]
    for g in range(4):
        queues["pqrs"[g]] = [(None, (n, g, 0 if n < SPLIT else ALL)) for n in chunks]
        queues["tuvw"[g]] = [(None, (n, g, 1)) for n in range(SPLIT)]

    steps, before, complete, handed = [], [], set(), set()
    for letter in "".join(PROGRAM):
        fn, args = queues[letter].pop(0)
        if fn is not None:
            before.append((fn, args))
            continue
        n, g, q = args
        for r in (range(2) if q == ALL else (q,)):
            if (g, r) not in complete:
                complete.add((g, r))
                before.append((group_complete, (g, r)))
        if n not in handed:
            handed.add(n)
            before.append((handed_over, (n,)))
        if n >= WIDE:
            before.append((sum_narrow, (n, g)))
        else:
            steps.append((before, (n * 4 + g) * 2 + q % 2, q != ALL))
            before = []

    def run(todo):
        for fn, args in todo:
            fn(*args)

    def in_loop(first, last):
        part = steps[first:last]

        def body(k, carry):
            code = part[0][1]
            for i, (todo, this, _) in enumerate(part):
                code = jnp.where(k == first + i, this, code)
                if todo:
                    pl.when(k == first + i)(lambda: run(todo))
            sum_loop(code, any(s for _, _, s in part), any(not s for _, _, s in part))
            return carry

        lax.fori_loop(first, last, body, 0)

    for first in range(0, len(steps), LOOP):
        in_loop(first, min(first + LOOP, len(steps)))
    run(before)

    for i in range(BLOCKS // 4):
        wait(b_all.at[pl.ds(0, 4), pl.ds(0, 15)], zs_sem.at[i])
        wait(crecv.at[pl.ds(0, 4), pl.ds(0, 2)], cs_sem.at[i])
    wait(b_all.at[pl.ds(0, 5)], as_sem)
    for n in range(CHUNKS - SLOTS, CHUNKS):
        keep = rest if n < WIDE else pl.ds(0, narrow)
        wait(c0.at[n % SLOTS, :, :, :, :, keep], c0_sem.at[n % SLOTS])


def solution(mesh):
    def local_product(a_blk, b_blk):
        rows, cols = a_blk.shape
        width = cols // BLOCKS
        few = rows // 16
        dma = pltpu.SemaphoreType.DMA
        c_blk = pl.pallas_call(
            kernel,
            name="matmul_3d",
            out_shape=pltpu.VMEM((2, 4, 2, few, cols), jnp.bfloat16),
            in_specs=[pl.BlockSpec(memory_space=pl.ANY)] * 2,
            out_specs=pl.BlockSpec(memory_space=pltpu.VMEM),
            scratch_shapes=[
                pltpu.VMEM((2, 4, 2, few, cols), jnp.bfloat16),
                pltpu.VMEM((4, 2, 4, 2, few, cols), jnp.bfloat16),
                pltpu.VMEM((3, 2, 2, few, cols), jnp.bfloat16),
                pltpu.VMEM((2, 2, 2, few, cols // 2), jnp.bfloat16),
                pltpu.VMEM((2, 2, 2, few, cols // 2), jnp.bfloat16),
                pltpu.VMEM((BLOCKS, 2 * Z_N, rows, width), jnp.bfloat16),
                pltpu.VMEM((BLOCKS, 3, 2, 4, 2, few, width), jnp.float32),
                pltpu.VMEM((SLOTS, 2, 4, 2, few, width), jnp.float32),
                pltpu.VMEM((2, 4, 2, few, width), jnp.float32),
                dma((4,)), dma((Z_SEMS, 7)), dma((BLOCKS // 4,)), dma((CHUNKS,)),
                dma((3, 2, 2)), dma((2, 2)), dma((2, 2)), dma((3, 2)), dma((4, 2, 2)), dma((4, 2)), dma,
                dma((2 * SPLIT + C_SEMS, 3)), dma((BLOCKS // 4,)), dma((SLOTS,)),
            ],
            compiler_params=pltpu.CompilerParams(
                collective_id=0, has_side_effects=True, vmem_limit_bytes=61 * 1024 * 1024
            ),
        )(a_blk.reshape(2, 4, 2, few, cols), b_blk)
        return c_blk.reshape(rows, cols)

    block_spec = P(("row", "depth"), "col")
    return jax.shard_map(local_product, mesh=mesh, in_specs=(block_spec, block_spec), out_specs=block_spec, check_vma=False)
```

```python
import jax
import jax.numpy as jnp
from jax import lax
from jax.experimental import pallas as pl
from jax.experimental.pallas import tpu as pltpu
from jax.sharding import PartitionSpec as P

MESH = pl.DeviceIdType.MESH
X_N, Y_N, Z_N = 4, 4, 8
BLOCKS = 16
SLOTS = 8
LOOP = 8
WIDE = 15
SPLIT = 4
ALL = 2
Z_SEMS, C_SEMS = 4, 3

PROGRAM = (
    "aiiajaafibfbjikbfcbjkgjlgnlalmlhcdknfcomcmomdhogeodbnpngedet",
    "fhatkeohcpaoptobtdgponnbqfaqqhceuucopfqgduuaobaqoongdehrrnpb",
    "rrcvbfqfehcovopgoodrvgcsdssrwhfawsqeashevpsbgpdbwwrfahceqcpq",
    "bsgfdrfqhdecgrasgpehrdsbpfhaeqscapgbqadrhqbffcbrecgpdrcsgfds",
    "heqdhegpspherpqsqqrrrsss",
)


def chunk(n):
    return (n, None) if n < WIDE else (WIDE + (n - WIDE) // 2, (n - WIDE) % 2)


CHUNKS = WIDE + 2 * (BLOCKS - WIDE)


def kernel(a_hbm, b_hbm, c_out, a_own, a_all, s1, rl1, rl2, b_all, crecv, c0, prod,
           ld_sem, zr_sem, zs_sem, dr_sem, s1_sem, r1_sem, r2_sem, s2_sem, ag_sem, fw_sem, as_sem,
           cr_sem, cs_sem, c0_sem):
    row, y, z = lax.axis_index("row"), lax.axis_index("col"), lax.axis_index("depth")
    x, c = row // 2, row % 2
    width = b_all.shape[3]
    narrow = width // 2
    cols = a_own.shape[4]
    part_cols = (pl.ds(0, cols // 2), pl.ds(cols // 2, cols // 2))
    rest = slice(None)

    def at_x(dx):
        return {"row": 2 * ((x + dx + X_N) % X_N) + c}

    def at_y(dy):
        return {"col": (y + dy + Y_N) % Y_N}

    step = 1 - 2 * c
    z_long = {"depth": (z + step + Z_N) % Z_N}
    z_short = {"depth": (z - step + Z_N) % Z_N}
    partner = {"row": 2 * x + 1 - c}

    def send(src, dst, ssem, rsem, dev):
        pltpu.make_async_remote_copy(src_ref=src, dst_ref=dst, send_sem=ssem, recv_sem=rsem,
                                     device_id=dev, device_id_type=MESH).start()

    def wait(ref, sem):
        pltpu.make_async_copy(ref, ref, sem).wait()

    e_own = (y - x + Y_N) % Y_N
    flip = e_own // 3
    j_own = e_own

    def b_local(m, sem):
        return pltpu.make_async_copy(b_hbm.at[:, pl.ds(pl.multiple_of(m * width, width), width)],
                                     b_all.at[m, c * Z_N + z], ld_sem.at[sem])

    def a_load(r):
        return pltpu.make_async_copy(a_hbm.at[:, :, r], a_own.at[:, :, r], ld_sem.at[2 + r])

    a_load(0).start()
    b_local(0, 0).start()
    a_load(1).start()
    barrier = pltpu.get_barrier_semaphore()
    for dev in (at_x(1), at_x(-1), at_y(1), at_y(-1), z_long, z_short, partner):
        pl.semaphore_signal(barrier, inc=1, device_id=dev, device_id_type=MESH)
    lax.fori_loop(1, BLOCKS, lambda m, _: (b_local(m, 1).start(), 0)[1], 0)

    def quarter_sem(e, o, r):
        return s1_sem.at[(e + 1) % 2 * (2 - e // 2), o, r]

    def by_e(e, o, r, j, part, fn):
        col_part = rest if part is None else part_cols[part]

        @pl.when(e == 0)
        def _():
            fn(a_all.at[3, o, j, r, :, col_part])

        @pl.when(e != 0)
        def _():
            fn(s1.at[(e + Y_N - 1) % Y_N, o, r, :, col_part])

    for o in range(2):
        for r in range(2):
            by_e(e_own, o, r, 0, None, lambda dst: pltpu.make_async_copy(
                a_hbm.at[(o + flip) % 2, 0, r], dst, quarter_sem(e_own, o, r)).start())
    pl.semaphore_wait(barrier, 7)
    loaded = set()

    def ev_s1(o, r):
        if r not in loaded:
            loaded.add(r)
            a_load(r).wait()
        h = (o + flip) % 2
        send(a_own.at[h, 2, r, :, part_cols[0]], rl1.at[0, o, r], as_sem, r1_sem.at[o, r], at_y(1))
        send(a_own.at[h, 2, r, :, part_cols[1]], rl1.at[1, o, r], as_sem, r1_sem.at[o, r], at_y(-1))
        sem = quarter_sem(e_own, o, r)
        by_e(e_own, o, r, 1, None, lambda dst: send(a_own.at[h, 1, r], dst, as_sem, sem, at_y(1)))
        by_e(e_own, o, r, 3, None, lambda dst: send(a_own.at[h, 3, r], dst, as_sem, sem, at_y(-1)))

    def ev_r1(o, r):
        wait(rl1.at[:, o, r], r1_sem.at[o, r])
        for d, dy in ((0, 1), (1, -1)):
            e = (y - dy - x + 2 * Y_N) % Y_N
            by_e(e, o, r, 2, d, lambda dst: send(rl1.at[d, o, r], dst, as_sem, quarter_sem(e, o, r), at_y(dy)))

    def ev_s2(o, r):
        wait(s1.at[pl.ds(0, 2), o, r], quarter_sem(1, o, r))
        g = 2 * o
        j = (y - x - 1 + 2 * Y_N) % Y_N
        send(s1.at[0, o, r], a_all.at[g, o, j, r], as_sem, s2_sem.at[g, r], at_x(1))
        j = (y - x + 1 + Y_N) % Y_N
        send(s1.at[2, o, r], a_all.at[g, 1 - o, j, r], as_sem, s2_sem.at[g, r], at_x(-1))

    def ev_s2f(o, r):
        wait(s1.at[1, o, r], quarter_sem(2, o, r))
        for d in range(2):
            send(s1.at[1, o, r, :, part_cols[d]], rl2.at[d, o, r], as_sem, r2_sem.at[o, r], at_x(1 - 2 * d))

    def ev_r2(o, r):
        wait(rl2.at[:, o, r], r2_sem.at[o, r])
        for d, dx in ((0, 1), (1, -1)):
            j = (y - x - dx + 2 * Y_N) % Y_N
            send(rl2.at[d, o, r], a_all.at[1, o, j, r, :, part_cols[d]], as_sem, s2_sem.at[1, r], at_x(dx))

    def ev_ag(g, r):
        if g == 3:
            for o in range(2):
                wait(a_all.at[g, o, j_own, r], quarter_sem(0, o, r))
        else:
            wait(a_all.at[g, :, j_own, r], s2_sem.at[g, r])
        for d in range(2):
            quarter = a_all.at[g, d, j_own, r]
            send(quarter, quarter, as_sem, ag_sem.at[g, d, r], at_y(1))
            send(quarter, quarter, as_sem, ag_sem.at[g, d, r], at_y(-1))

    def ev_fw(g, r, d):
        wait(a_all.at[0, 0, 0], ag_sem.at[g, d, r])
        for k, dy in ((0, 1), (1, -1)):
            j = (y - dy - x + 2 * Y_N) % Y_N
            part = a_all.at[g, d, j, r, :, part_cols[k]]
            send(part, part, as_sem, fw_sem.at[g, r], at_y(dy))

    def group_complete(g, r):
        wait(a_all.at[0, 0, 0], fw_sem.at[g, r])

    def block(hop):
        return c * Z_N + (z - hop * step + 2 * Z_N) % Z_N

    def lanes_of(n):
        half = chunk(n)[1]
        return rest if half is None else pl.ds(half * narrow, narrow)

    def piece(n, kb):
        return b_all.at[chunk(n)[0], kb, :, lanes_of(n)]

    def hand_over(n, kb):
        send(piece(n, kb), piece(n, kb), zs_sem.at[chunk(n)[0] // 4], dr_sem.at[n], partner)

    def forward_long(n, hop):
        p = piece(n, block(hop))
        send(p, p, zs_sem.at[chunk(n)[0] // 4], zr_sem.at[n % Z_SEMS, hop], z_long)

    def forward_short(n, hop):
        p = piece(n, block(-hop))
        send(p, p, zs_sem.at[chunk(n)[0] // 4], zr_sem.at[n % Z_SEMS, 4 + hop], z_short)

    def ev_own(n):
        if n == 0:
            b_local(0, 0).wait()
        elif n == 1:
            wait(b_all.at[0, pl.ds(0, BLOCKS - 1)], ld_sem.at[1])
        forward_long(n, 0)
        forward_short(n, 0)
        hand_over(n, block(0))

    def ev_long(n, hop):
        wait(piece(n, block(hop)), zr_sem.at[n % Z_SEMS, hop - 1])
        if hop < 4:
            forward_long(n, hop)
        hand_over(n, block(hop))

    def ev_short(n, hop):
        wait(piece(n, block(-hop)), zr_sem.at[n % Z_SEMS, 4 + hop - 1])
        if hop < 3:
            forward_short(n, hop)
        hand_over(n, block(-hop))

    def handed_over(n):
        wait(b_all.at[0, pl.ds(0, Z_N), :, lanes_of(n)], dr_sem.at[n])

    def dot(a, b):
        return jnp.dot(a.reshape(-1, cols), b.reshape(cols, -1), preferred_element_type=jnp.float32)

    def sum_sem(n, q):
        return 2 * SPLIT + (n - SPLIT) % C_SEMS if isinstance(q, slice) else 2 * n + q

    def sum_stage(n, g, q, m, lanes, first, size, when, reuse, old):
        slot = n % SLOTS
        keep = rest if isinstance(lanes, slice) else pl.ds(0, narrow)
        arrivals = sum_sem(n, q)

        def pass_on(src, ssem):
            for d in range(2):
                send(src.at[d], crecv.at[m, g, d, :, q, :, lanes], ssem, cr_sem.at[arrivals, g], at_x(1 - 2 * d))

        def arrived():
            wait(crecv.at[m, g - 1, :, :, q, :, lanes], cr_sem.at[arrivals, g - 1])

        def begin():
            reuse(lambda: wait(c0.at[slot, :, :, :, :, old], c0_sem.at[slot]))
            c0[slot, :, :, q, :, keep] = prod[:, :, q, :, keep]
            pass_on(c0.at[slot, :, :, q, :, keep], c0_sem.at[slot])

        def middle():
            arrived()
            crecv[m, g - 1, :, :, q, :, lanes] += prod[:, :, q, :, keep]
            pass_on(crecv.at[m, g - 1, :, :, q, :, lanes], cs_sem.at[m // 4])

        def end():
            arrived()
            total = crecv[m, g - 1, :, :, q, :, lanes] + prod[:, :, q, :, keep]
            c_out[:, :, q, :, pl.ds(pl.multiple_of(first, size), size)] = total.astype(c_out.dtype)

        a = a_all[g, :, :, q]
        prod[:, :, q, :, keep] = dot(a, b_all[m, :, :, lanes]).reshape(a.shape[:-1] + (size,))
        when(g == 0, begin)
        when((g == 1) | (g == 2), middle)
        when(g == 3, end)

    def branch(cond, fn):
        pl.when(cond)(fn)

    def fixed(cond, fn):
        if cond:
            fn()

    def sum_loop(code, split, wide):
        n, g, q = code // 8, code // 2 % 4, code % 2
        if split:
            pl.when(n < SPLIT)(lambda: sum_stage(n, g, q, n, rest, n * width, width, branch, lambda fn: None, rest))
        if wide:
            pl.when(n >= SPLIT)(lambda: sum_stage(n, g, rest, n, rest, n * width, width, branch,
                                                  pl.when(n >= SLOTS), rest))

    def sum_narrow(n, g):
        m, half = chunk(n)
        old = rest if n - SLOTS < WIDE else pl.ds(0, narrow)
        sum_stage(n, g, rest, m, lanes_of(n), m * width + half * narrow, narrow, fixed, lambda fn: fn(), old)

    chunks = range(CHUNKS)
    queues = {"a": [(ev_own, (n,)) for n in chunks]}
    for hop in range(1, 5):
        queues["abcde"[hop]] = [(ev_long, (n, hop)) for n in chunks]
    for hop in range(1, 4):
        queues["efgh"[hop]] = [(ev_short, (n, hop)) for n in chunks]
    by_half = [(o, r) for o in range(2) for r in range(2)]
    by_row = [(o, r) for r in range(2) for o in range(2)]
    queues["i"] = [(ev_s1, p) for p in by_half]
    queues["j"] = [(ev_r1, p) for p in by_half]
    queues["k"] = [(ev_s2, p) for p in by_half]
    queues["l"] = [(ev_s2f, p) for p in by_row]
    queues["m"] = [(ev_r2, p) for p in by_row]
    groups = [(g, r) for g in range(4) for r in range(2)]
    queues["n"] = [(ev_ag, p) for p in groups]
    queues["o"] = [(ev_fw, p + (d,)) for p in groups for d in range(2)]
    for g in range(4):
        queues["pqrs"[g]] = [(None, (n, g, 0 if n < SPLIT else ALL)) for n in chunks]
        queues["tuvw"[g]] = [(None, (n, g, 1)) for n in range(SPLIT)]

    steps, before, complete, handed = [], [], set(), set()
    for letter in "".join(PROGRAM):
        fn, args = queues[letter].pop(0)
        if fn is not None:
            before.append((fn, args))
            continue
        n, g, q = args
        for r in (range(2) if q == ALL else (q,)):
            if (g, r) not in complete:
                complete.add((g, r))
                before.append((group_complete, (g, r)))
        if n not in handed:
            handed.add(n)
            before.append((handed_over, (n,)))
        if n >= WIDE:
            before.append((sum_narrow, (n, g)))
        else:
            steps.append((before, (n * 4 + g) * 2 + q % 2, q != ALL))
            before = []

    def run(todo):
        for fn, args in todo:
            fn(*args)

    def in_loop(first, last):
        part = steps[first:last]

        def body(k, carry):
            code = part[0][1]
            for i, (todo, this, _) in enumerate(part):
                code = jnp.where(k == first + i, this, code)
                if todo:
                    pl.when(k == first + i)(lambda: run(todo))
            sum_loop(code, any(s for _, _, s in part), any(not s for _, _, s in part))
            return carry

        lax.fori_loop(first, last, body, 0)

    for first in range(0, len(steps), LOOP):
        in_loop(first, min(first + LOOP, len(steps)))
    run(before)

    for i in range(BLOCKS // 4):
        wait(b_all.at[pl.ds(0, 4), pl.ds(0, 15)], zs_sem.at[i])
        wait(crecv.at[pl.ds(0, 4), pl.ds(0, 2)], cs_sem.at[i])
    wait(b_all.at[pl.ds(0, 5)], as_sem)
    for n in range(CHUNKS - SLOTS, CHUNKS):
        keep = rest if n < WIDE else pl.ds(0, narrow)
        wait(c0.at[n % SLOTS, :, :, :, :, keep], c0_sem.at[n % SLOTS])


def solution(mesh):
    def local_product(a_blk, b_blk):
        rows, cols = a_blk.shape
        width = cols // BLOCKS
        few = rows // 16
        dma = pltpu.SemaphoreType.DMA
        c_blk = pl.pallas_call(
            kernel,
            name="matmul_3d",
            out_shape=pltpu.VMEM((2, 4, 2, few, cols), jnp.bfloat16),
            in_specs=[pl.BlockSpec(memory_space=pl.ANY)] * 2,
            out_specs=pl.BlockSpec(memory_space=pltpu.VMEM),
            scratch_shapes=[
                pltpu.VMEM((2, 4, 2, few, cols), jnp.bfloat16),
                pltpu.VMEM((4, 2, 4, 2, few, cols), jnp.bfloat16),
                pltpu.VMEM((3, 2, 2, few, cols), jnp.bfloat16),
                pltpu.VMEM((2, 2, 2, few, cols // 2), jnp.bfloat16),
                pltpu.VMEM((2, 2, 2, few, cols // 2), jnp.bfloat16),
                pltpu.VMEM((BLOCKS, 2 * Z_N, rows, width), jnp.bfloat16),
                pltpu.VMEM((BLOCKS, 3, 2, 4, 2, few, width), jnp.float32),
                pltpu.VMEM((SLOTS, 2, 4, 2, few, width), jnp.float32),
                pltpu.VMEM((2, 4, 2, few, width), jnp.float32),
                dma((4,)), dma((Z_SEMS, 7)), dma((BLOCKS // 4,)), dma((CHUNKS,)),
                dma((3, 2, 2)), dma((2, 2)), dma((2, 2)), dma((3, 2)), dma((4, 2, 2)), dma((4, 2)), dma,
                dma((2 * SPLIT + C_SEMS, 3)), dma((BLOCKS // 4,)), dma((SLOTS,)),
            ],
            compiler_params=pltpu.CompilerParams(
                collective_id=0, has_side_effects=True, vmem_limit_bytes=61 * 1024 * 1024
            ),
        )(a_blk.reshape(2, 4, 2, few, cols), b_blk)
        return c_blk.reshape(rows, cols)

    block_spec = P(("row", "depth"), "col")
    return jax.shard_map(local_product, mesh=mesh, in_specs=(block_spec, block_spec), out_specs=block_spec, check_vma=False)
```

```python
import jax
import jax.numpy as jnp
from jax import lax
from jax.experimental import pallas as pl
from jax.experimental.pallas import tpu as pltpu
from jax.sharding import PartitionSpec as P

MESH = pl.DeviceIdType.MESH
X_N, Y_N, Z_N = 4, 4, 8
BLOCKS = 16
SLOTS = 8
LOOP = 8
WIDE = 15
SPLIT = 4
ALL = 2
Z_SEMS, C_SEMS = 5, 3

PROGRAM = (
    "aiaaifjibjafklibjfabkjbnccnglmlckdhmcfooglkobdgogndmhmedteaf",
    "hcnpepeaothtoobppdontgffqnqcqbehuuaopudogucqbnaqhoegaorpnrrd",
    "cbhrbqfeordofvpcovvovgfgssssedhwarscwqhwgepawbspdbrahefqccpq",
    "bgfsdrdqcfrhgeseapghdrsbfpaheqsacpqgarbdhbqffrcecbsgpdrdcgfs",
    "heqhedgpspherpqsqqrrrsss",
)


def chunk(n):
    return (n, None) if n < WIDE else (WIDE + (n - WIDE) // 2, (n - WIDE) % 2)


CHUNKS = WIDE + 2 * (BLOCKS - WIDE)


def kernel(a_hbm, b_hbm, c_out, a_own, a_all, s1, rl1, rl2, b_all, crecv, c0, prod,
           ld_sem, zr_sem, zs_sem, dr_sem, s1_sem, r1_sem, r2_sem, s2_sem, ag_sem, fw_sem, as_sem,
           cr_sem, cs_sem, c0_sem):
    row, y, z = lax.axis_index("row"), lax.axis_index("col"), lax.axis_index("depth")
    x, c = row // 2, row % 2
    width = b_all.shape[3]
    narrow = width // 2
    cols = a_own.shape[4]
    part_cols = (pl.ds(0, cols // 2), pl.ds(cols // 2, cols // 2))
    rest = slice(None)

    def at_x(dx):
        return {"row": 2 * ((x + dx + X_N) % X_N) + c}

    def at_y(dy):
        return {"col": (y + dy + Y_N) % Y_N}

    step = 1 - 2 * c
    z_long = {"depth": (z + step + Z_N) % Z_N}
    z_short = {"depth": (z - step + Z_N) % Z_N}
    partner = {"row": 2 * x + 1 - c}

    def send(src, dst, ssem, rsem, dev):
        pltpu.make_async_remote_copy(src_ref=src, dst_ref=dst, send_sem=ssem, recv_sem=rsem,
                                     device_id=dev, device_id_type=MESH).start()

    def wait(ref, sem):
        pltpu.make_async_copy(ref, ref, sem).wait()

    e_own = (y - x + Y_N) % Y_N
    flip = e_own // 3
    j_own = e_own

    def b_local(m, sem):
        return pltpu.make_async_copy(b_hbm.at[:, pl.ds(pl.multiple_of(m * width, width), width)],
                                     b_all.at[m, c * Z_N + z], ld_sem.at[sem])

    def a_load(r):
        return pltpu.make_async_copy(a_hbm.at[:, :, r], a_own.at[:, :, r], ld_sem.at[2 + r])

    a_load(0).start()
    b_local(0, 0).start()
    a_load(1).start()
    barrier = pltpu.get_barrier_semaphore()
    for dev in (at_x(1), at_x(-1), at_y(1), at_y(-1), z_long, z_short, partner):
        pl.semaphore_signal(barrier, inc=1, device_id=dev, device_id_type=MESH)
    lax.fori_loop(1, BLOCKS, lambda m, _: (b_local(m, 1).start(), 0)[1], 0)

    def quarter_sem(e, o, r):
        return s1_sem.at[(e + 1) % 2 * (2 - e // 2), o, r]

    def by_e(e, o, r, j, part, fn):
        col_part = rest if part is None else part_cols[part]

        @pl.when(e == 0)
        def _():
            fn(a_all.at[3, o, j, r, :, col_part])

        @pl.when(e != 0)
        def _():
            fn(s1.at[(e + Y_N - 1) % Y_N, o, r, :, col_part])

    for o in range(2):
        for r in range(2):
            by_e(e_own, o, r, 0, None, lambda dst: pltpu.make_async_copy(
                a_hbm.at[(o + flip) % 2, 0, r], dst, quarter_sem(e_own, o, r)).start())
    pl.semaphore_wait(barrier, 7)
    loaded = set()

    def ev_s1(o, r):
        if r not in loaded:
            loaded.add(r)
            a_load(r).wait()
        h = (o + flip) % 2
        send(a_own.at[h, 2, r, :, part_cols[0]], rl1.at[0, o, r], as_sem, r1_sem.at[o, r], at_y(1))
        send(a_own.at[h, 2, r, :, part_cols[1]], rl1.at[1, o, r], as_sem, r1_sem.at[o, r], at_y(-1))
        sem = quarter_sem(e_own, o, r)
        by_e(e_own, o, r, 1, None, lambda dst: send(a_own.at[h, 1, r], dst, as_sem, sem, at_y(1)))
        by_e(e_own, o, r, 3, None, lambda dst: send(a_own.at[h, 3, r], dst, as_sem, sem, at_y(-1)))

    def ev_r1(o, r):
        wait(rl1.at[:, o, r], r1_sem.at[o, r])
        for d, dy in ((0, 1), (1, -1)):
            e = (y - dy - x + 2 * Y_N) % Y_N
            by_e(e, o, r, 2, d, lambda dst: send(rl1.at[d, o, r], dst, as_sem, quarter_sem(e, o, r), at_y(dy)))

    def ev_s2(o, r):
        wait(s1.at[pl.ds(0, 2), o, r], quarter_sem(1, o, r))
        g = 2 * o
        j = (y - x - 1 + 2 * Y_N) % Y_N
        send(s1.at[0, o, r], a_all.at[g, o, j, r], as_sem, s2_sem.at[g, r], at_x(1))
        j = (y - x + 1 + Y_N) % Y_N
        send(s1.at[2, o, r], a_all.at[g, 1 - o, j, r], as_sem, s2_sem.at[g, r], at_x(-1))

    def ev_s2f(o, r):
        wait(s1.at[1, o, r], quarter_sem(2, o, r))
        for d in range(2):
            send(s1.at[1, o, r, :, part_cols[d]], rl2.at[d, o, r], as_sem, r2_sem.at[o, r], at_x(1 - 2 * d))

    def ev_r2(o, r):
        wait(rl2.at[:, o, r], r2_sem.at[o, r])
        for d, dx in ((0, 1), (1, -1)):
            j = (y - x - dx + 2 * Y_N) % Y_N
            send(rl2.at[d, o, r], a_all.at[1, o, j, r, :, part_cols[d]], as_sem, s2_sem.at[1, r], at_x(dx))

    def ev_ag(g, r):
        if g == 3:
            for o in range(2):
                wait(a_all.at[g, o, j_own, r], quarter_sem(0, o, r))
        else:
            wait(a_all.at[g, :, j_own, r], s2_sem.at[g, r])
        for d in range(2):
            quarter = a_all.at[g, d, j_own, r]
            send(quarter, quarter, as_sem, ag_sem.at[g, d, r], at_y(1))
            send(quarter, quarter, as_sem, ag_sem.at[g, d, r], at_y(-1))

    def ev_fw(g, r, d):
        wait(a_all.at[0, 0, 0], ag_sem.at[g, d, r])
        for k, dy in ((0, 1), (1, -1)):
            j = (y - dy - x + 2 * Y_N) % Y_N
            part = a_all.at[g, d, j, r, :, part_cols[k]]
            send(part, part, as_sem, fw_sem.at[g, r], at_y(dy))

    def group_complete(g, r):
        wait(a_all.at[0, 0, 0], fw_sem.at[g, r])

    def block(hop):
        return c * Z_N + (z - hop * step + 2 * Z_N) % Z_N

    def lanes_of(n):
        half = chunk(n)[1]
        return rest if half is None else pl.ds(half * narrow, narrow)

    def piece(n, kb):
        return b_all.at[chunk(n)[0], kb, :, lanes_of(n)]

    def hand_over(n, kb):
        send(piece(n, kb), piece(n, kb), zs_sem.at[chunk(n)[0] // 4], dr_sem.at[n], partner)

    def forward_long(n, hop):
        p = piece(n, block(hop))
        send(p, p, zs_sem.at[chunk(n)[0] // 4], zr_sem.at[n % Z_SEMS, hop], z_long)

    def forward_short(n, hop):
        p = piece(n, block(-hop))
        send(p, p, zs_sem.at[chunk(n)[0] // 4], zr_sem.at[n % Z_SEMS, 4 + hop], z_short)

    def ev_own(n):
        if n == 0:
            b_local(0, 0).wait()
        elif n == 1:
            wait(b_all.at[0, pl.ds(0, BLOCKS - 1)], ld_sem.at[1])
        forward_long(n, 0)
        forward_short(n, 0)
        hand_over(n, block(0))

    def ev_long(n, hop):
        wait(piece(n, block(hop)), zr_sem.at[n % Z_SEMS, hop - 1])
        if hop < 4:
            forward_long(n, hop)
        hand_over(n, block(hop))

    def ev_short(n, hop):
        wait(piece(n, block(-hop)), zr_sem.at[n % Z_SEMS, 4 + hop - 1])
        if hop < 3:
            forward_short(n, hop)
        hand_over(n, block(-hop))

    def handed_over(n):
        wait(b_all.at[0, pl.ds(0, Z_N), :, lanes_of(n)], dr_sem.at[n])

    def dot(a, b):
        return jnp.dot(a.reshape(-1, cols), b.reshape(cols, -1), preferred_element_type=jnp.float32)

    def sum_sem(n, q):
        return 2 * SPLIT + (n - SPLIT) % C_SEMS if isinstance(q, slice) else 2 * n + q

    def sum_stage(n, g, q, m, lanes, first, size, when, reuse, old):
        slot = n % SLOTS
        keep = rest if isinstance(lanes, slice) else pl.ds(0, narrow)
        arrivals = sum_sem(n, q)

        def pass_on(src, ssem):
            for d in range(2):
                send(src.at[d], crecv.at[m, g, d, :, q, :, lanes], ssem, cr_sem.at[arrivals, g], at_x(1 - 2 * d))

        def arrived():
            wait(crecv.at[m, g - 1, :, :, q, :, lanes], cr_sem.at[arrivals, g - 1])

        def begin():
            reuse(lambda: wait(c0.at[slot, :, :, :, :, old], c0_sem.at[slot]))
            c0[slot, :, :, q, :, keep] = prod[:, :, q, :, keep]
            pass_on(c0.at[slot, :, :, q, :, keep], c0_sem.at[slot])

        def middle():
            arrived()
            crecv[m, g - 1, :, :, q, :, lanes] += prod[:, :, q, :, keep]
            pass_on(crecv.at[m, g - 1, :, :, q, :, lanes], cs_sem.at[m // 4])

        def end():
            arrived()
            total = crecv[m, g - 1, :, :, q, :, lanes] + prod[:, :, q, :, keep]
            c_out[:, :, q, :, pl.ds(pl.multiple_of(first, size), size)] = total.astype(c_out.dtype)

        a = a_all[g, :, :, q]
        prod[:, :, q, :, keep] = dot(a, b_all[m, :, :, lanes]).reshape(a.shape[:-1] + (size,))
        when(g == 0, begin)
        when((g == 1) | (g == 2), middle)
        when(g == 3, end)

    def branch(cond, fn):
        pl.when(cond)(fn)

    def fixed(cond, fn):
        if cond:
            fn()

    def sum_loop(code, split, wide):
        n, g, q = code // 8, code // 2 % 4, code % 2
        if split:
            pl.when(n < SPLIT)(lambda: sum_stage(n, g, q, n, rest, n * width, width, branch, lambda fn: None, rest))
        if wide:
            pl.when(n >= SPLIT)(lambda: sum_stage(n, g, rest, n, rest, n * width, width, branch,
                                                  pl.when(n >= SLOTS), rest))

    def sum_narrow(n, g):
        m, half = chunk(n)
        old = rest if n - SLOTS < WIDE else pl.ds(0, narrow)
        sum_stage(n, g, rest, m, lanes_of(n), m * width + half * narrow, narrow, fixed, lambda fn: fn(), old)

    chunks = range(CHUNKS)
    queues = {"a": [(ev_own, (n,)) for n in chunks]}
    for hop in range(1, 5):
        queues["abcde"[hop]] = [(ev_long, (n, hop)) for n in chunks]
    for hop in range(1, 4):
        queues["efgh"[hop]] = [(ev_short, (n, hop)) for n in chunks]
    by_half = [(o, r) for o in range(2) for r in range(2)]
    by_row = [(o, r) for r in range(2) for o in range(2)]
    queues["i"] = [(ev_s1, p) for p in by_half]
    queues["j"] = [(ev_r1, p) for p in by_half]
    queues["k"] = [(ev_s2, p) for p in by_half]
    queues["l"] = [(ev_s2f, p) for p in by_row]
    queues["m"] = [(ev_r2, p) for p in by_row]
    groups = [(g, r) for g in range(4) for r in range(2)]
    queues["n"] = [(ev_ag, p) for p in groups]
    queues["o"] = [(ev_fw, p + (d,)) for p in groups for d in range(2)]
    for g in range(4):
        queues["pqrs"[g]] = [(None, (n, g, 0 if n < SPLIT else ALL)) for n in chunks]
        queues["tuvw"[g]] = [(None, (n, g, 1)) for n in range(SPLIT)]

    steps, before, complete, handed = [], [], set(), set()
    for letter in "".join(PROGRAM):
        fn, args = queues[letter].pop(0)
        if fn is not None:
            before.append((fn, args))
            continue
        n, g, q = args
        for r in (range(2) if q == ALL else (q,)):
            if (g, r) not in complete:
                complete.add((g, r))
                before.append((group_complete, (g, r)))
        if n not in handed:
            handed.add(n)
            before.append((handed_over, (n,)))
        if n >= WIDE:
            before.append((sum_narrow, (n, g)))
        else:
            steps.append((before, (n * 4 + g) * 2 + q % 2, q != ALL))
            before = []

    def run(todo):
        for fn, args in todo:
            fn(*args)

    def in_loop(first, last):
        part = steps[first:last]

        def body(k, carry):
            code = part[0][1]
            for i, (todo, this, _) in enumerate(part):
                code = jnp.where(k == first + i, this, code)
                if todo:
                    pl.when(k == first + i)(lambda: run(todo))
            sum_loop(code, any(s for _, _, s in part), any(not s for _, _, s in part))
            return carry

        lax.fori_loop(first, last, body, 0)

    for first in range(0, len(steps), LOOP):
        in_loop(first, min(first + LOOP, len(steps)))
    run(before)

    for i in range(BLOCKS // 4):
        wait(b_all.at[pl.ds(0, 4), pl.ds(0, 15)], zs_sem.at[i])
        wait(crecv.at[pl.ds(0, 4), pl.ds(0, 2)], cs_sem.at[i])
    wait(b_all.at[pl.ds(0, 5)], as_sem)
    for n in range(CHUNKS - SLOTS, CHUNKS):
        keep = rest if n < WIDE else pl.ds(0, narrow)
        wait(c0.at[n % SLOTS, :, :, :, :, keep], c0_sem.at[n % SLOTS])


def solution(mesh):
    def local_product(a_blk, b_blk):
        rows, cols = a_blk.shape
        width = cols // BLOCKS
        few = rows // 16
        dma = pltpu.SemaphoreType.DMA
        c_blk = pl.pallas_call(
            kernel,
            name="matmul_3d",
            out_shape=pltpu.VMEM((2, 4, 2, few, cols), jnp.bfloat16),
            in_specs=[pl.BlockSpec(memory_space=pl.ANY)] * 2,
            out_specs=pl.BlockSpec(memory_space=pltpu.VMEM),
            scratch_shapes=[
                pltpu.VMEM((2, 4, 2, few, cols), jnp.bfloat16),
                pltpu.VMEM((4, 2, 4, 2, few, cols), jnp.bfloat16),
                pltpu.VMEM((3, 2, 2, few, cols), jnp.bfloat16),
                pltpu.VMEM((2, 2, 2, few, cols // 2), jnp.bfloat16),
                pltpu.VMEM((2, 2, 2, few, cols // 2), jnp.bfloat16),
                pltpu.VMEM((BLOCKS, 2 * Z_N, rows, width), jnp.bfloat16),
                pltpu.VMEM((BLOCKS, 3, 2, 4, 2, few, width), jnp.float32),
                pltpu.VMEM((SLOTS, 2, 4, 2, few, width), jnp.float32),
                pltpu.VMEM((2, 4, 2, few, width), jnp.float32),
                dma((4,)), dma((Z_SEMS, 7)), dma((BLOCKS // 4,)), dma((CHUNKS,)),
                dma((3, 2, 2)), dma((2, 2)), dma((2, 2)), dma((3, 2)), dma((4, 2, 2)), dma((4, 2)), dma,
                dma((2 * SPLIT + C_SEMS, 3)), dma((BLOCKS // 4,)), dma((SLOTS,)),
            ],
            compiler_params=pltpu.CompilerParams(
                collective_id=0, has_side_effects=True, vmem_limit_bytes=61 * 1024 * 1024
            ),
        )(a_blk.reshape(2, 4, 2, few, cols), b_blk)
        return c_blk.reshape(rows, cols)

    block_spec = P(("row", "depth"), "col")
    return jax.shard_map(local_product, mesh=mesh, in_specs=(block_spec, block_spec), out_specs=block_spec, check_vma=False)
```

```python
import jax
import jax.numpy as jnp
from jax import lax
from jax.experimental import pallas as pl
from jax.experimental.pallas import tpu as pltpu
from jax.sharding import PartitionSpec as P

MESH = pl.DeviceIdType.MESH
X_N, Y_N, Z_N = 4, 4, 8
BLOCKS = 16
SLOTS = 8
LOOP = 8
WIDE = 15
SPLIT = 4
ALL = 2
Z_SEMS, C_SEMS = 5, 3

PROGRAM = (
    "aiaiaajibfjbkibfbjfalcknjlnccogdfmcgollmkmddgnoebmdegkhfeoha",
    "nhcpphopteattoobtdogpfnqncqaqheuubogpdoauuqcobafnqherboprrrd",
    "ngocofqbfcrehvvvdopvofggssdscsaawwrehseqwwdhpgspbbrahfqecpcq",
    "sbgrdfdfcqhregsaepghrdsbpfaheqscapbgaqdrbhqffrcecbgpdsdrcgfh",
    "seqehdgpspherpqsqqrrrsss",
)


def chunk(n):
    return (n, None) if n < WIDE else (WIDE + (n - WIDE) // 2, (n - WIDE) % 2)


CHUNKS = WIDE + 2 * (BLOCKS - WIDE)


def kernel(a_hbm, b_hbm, c_out, a_own, a_all, s1, rl1, rl2, b_all, crecv, c0, prod,
           ld_sem, zr_sem, zs_sem, dr_sem, s1_sem, r1_sem, r2_sem, s2_sem, ag_sem, fw_sem, as_sem,
           cr_sem, cs_sem, c0_sem):
    row, y, z = lax.axis_index("row"), lax.axis_index("col"), lax.axis_index("depth")
    x, c = row // 2, row % 2
    width = b_all.shape[3]
    narrow = width // 2
    cols = a_own.shape[4]
    part_cols = (pl.ds(0, cols // 2), pl.ds(cols // 2, cols // 2))
    rest = slice(None)

    def at_x(dx):
        return {"row": 2 * ((x + dx + X_N) % X_N) + c}

    def at_y(dy):
        return {"col": (y + dy + Y_N) % Y_N}

    step = 1 - 2 * c
    z_long = {"depth": (z + step + Z_N) % Z_N}
    z_short = {"depth": (z - step + Z_N) % Z_N}
    partner = {"row": 2 * x + 1 - c}

    def send(src, dst, ssem, rsem, dev):
        pltpu.make_async_remote_copy(src_ref=src, dst_ref=dst, send_sem=ssem, recv_sem=rsem,
                                     device_id=dev, device_id_type=MESH).start()

    def wait(ref, sem):
        pltpu.make_async_copy(ref, ref, sem).wait()

    e_own = (y - x + Y_N) % Y_N
    flip = e_own // 3
    j_own = e_own

    def b_local(m, sem):
        return pltpu.make_async_copy(b_hbm.at[:, pl.ds(pl.multiple_of(m * width, width), width)],
                                     b_all.at[m, c * Z_N + z], ld_sem.at[sem])

    def a_load(r):
        return pltpu.make_async_copy(a_hbm.at[:, :, r], a_own.at[:, :, r], ld_sem.at[2 + r])

    a_load(0).start()
    b_local(0, 0).start()
    a_load(1).start()
    barrier = pltpu.get_barrier_semaphore()
    for dev in (at_x(1), at_x(-1), at_y(1), at_y(-1), z_long, z_short, partner):
        pl.semaphore_signal(barrier, inc=1, device_id=dev, device_id_type=MESH)
    lax.fori_loop(1, BLOCKS, lambda m, _: (b_local(m, 1).start(), 0)[1], 0)

    def quarter_sem(e, o, r):
        return s1_sem.at[(e + 1) % 2 * (2 - e // 2), o, r]

    def by_e(e, o, r, j, part, fn):
        col_part = rest if part is None else part_cols[part]

        @pl.when(e == 0)
        def _():
            fn(a_all.at[3, o, j, r, :, col_part])

        @pl.when(e != 0)
        def _():
            fn(s1.at[(e + Y_N - 1) % Y_N, o, r, :, col_part])

    for o in range(2):
        for r in range(2):
            by_e(e_own, o, r, 0, None, lambda dst: pltpu.make_async_copy(
                a_hbm.at[(o + flip) % 2, 0, r], dst, quarter_sem(e_own, o, r)).start())
    pl.semaphore_wait(barrier, 7)
    loaded = set()

    def ev_s1(o, r):
        if r not in loaded:
            loaded.add(r)
            a_load(r).wait()
        h = (o + flip) % 2
        send(a_own.at[h, 2, r, :, part_cols[0]], rl1.at[0, o, r], as_sem, r1_sem.at[o, r], at_y(1))
        send(a_own.at[h, 2, r, :, part_cols[1]], rl1.at[1, o, r], as_sem, r1_sem.at[o, r], at_y(-1))
        sem = quarter_sem(e_own, o, r)
        by_e(e_own, o, r, 1, None, lambda dst: send(a_own.at[h, 1, r], dst, as_sem, sem, at_y(1)))
        by_e(e_own, o, r, 3, None, lambda dst: send(a_own.at[h, 3, r], dst, as_sem, sem, at_y(-1)))

    def ev_r1(o, r):
        wait(rl1.at[:, o, r], r1_sem.at[o, r])
        for d, dy in ((0, 1), (1, -1)):
            e = (y - dy - x + 2 * Y_N) % Y_N
            by_e(e, o, r, 2, d, lambda dst: send(rl1.at[d, o, r], dst, as_sem, quarter_sem(e, o, r), at_y(dy)))

    def ev_s2(o, r):
        wait(s1.at[pl.ds(0, 2), o, r], quarter_sem(1, o, r))
        g = 2 * o
        j = (y - x - 1 + 2 * Y_N) % Y_N
        send(s1.at[0, o, r], a_all.at[g, o, j, r], as_sem, s2_sem.at[g, r], at_x(1))
        j = (y - x + 1 + Y_N) % Y_N
        send(s1.at[2, o, r], a_all.at[g, 1 - o, j, r], as_sem, s2_sem.at[g, r], at_x(-1))

    def ev_s2f(o, r):
        wait(s1.at[1, o, r], quarter_sem(2, o, r))
        for d in range(2):
            send(s1.at[1, o, r, :, part_cols[d]], rl2.at[d, o, r], as_sem, r2_sem.at[o, r], at_x(1 - 2 * d))

    def ev_r2(o, r):
        wait(rl2.at[:, o, r], r2_sem.at[o, r])
        for d, dx in ((0, 1), (1, -1)):
            j = (y - x - dx + 2 * Y_N) % Y_N
            send(rl2.at[d, o, r], a_all.at[1, o, j, r, :, part_cols[d]], as_sem, s2_sem.at[1, r], at_x(dx))

    def ev_ag(g, r):
        if g == 3:
            for o in range(2):
                wait(a_all.at[g, o, j_own, r], quarter_sem(0, o, r))
        else:
            wait(a_all.at[g, :, j_own, r], s2_sem.at[g, r])
        for d in range(2):
            quarter = a_all.at[g, d, j_own, r]
            send(quarter, quarter, as_sem, ag_sem.at[g, d, r], at_y(1))
            send(quarter, quarter, as_sem, ag_sem.at[g, d, r], at_y(-1))

    def ev_fw(g, r, d):
        wait(a_all.at[0, 0, 0], ag_sem.at[g, d, r])
        for k, dy in ((0, 1), (1, -1)):
            j = (y - dy - x + 2 * Y_N) % Y_N
            part = a_all.at[g, d, j, r, :, part_cols[k]]
            send(part, part, as_sem, fw_sem.at[g, r], at_y(dy))

    def group_complete(g, r):
        wait(a_all.at[0, 0, 0], fw_sem.at[g, r])

    def block(hop):
        return c * Z_N + (z - hop * step + 2 * Z_N) % Z_N

    def lanes_of(n):
        half = chunk(n)[1]
        return rest if half is None else pl.ds(half * narrow, narrow)

    def piece(n, kb):
        return b_all.at[chunk(n)[0], kb, :, lanes_of(n)]

    def hand_over(n, kb):
        send(piece(n, kb), piece(n, kb), zs_sem.at[chunk(n)[0] // 4], dr_sem.at[n], partner)

    def forward_long(n, hop):
        p = piece(n, block(hop))
        send(p, p, zs_sem.at[chunk(n)[0] // 4], zr_sem.at[n % Z_SEMS, hop], z_long)

    def forward_short(n, hop):
        p = piece(n, block(-hop))
        send(p, p, zs_sem.at[chunk(n)[0] // 4], zr_sem.at[n % Z_SEMS, 4 + hop], z_short)

    def ev_own(n):
        if n == 0:
            b_local(0, 0).wait()
        elif n == 1:
            wait(b_all.at[0, pl.ds(0, BLOCKS - 1)], ld_sem.at[1])
        forward_long(n, 0)
        forward_short(n, 0)
        hand_over(n, block(0))

    def ev_long(n, hop):
        wait(piece(n, block(hop)), zr_sem.at[n % Z_SEMS, hop - 1])
        if hop < 4:
            forward_long(n, hop)
        hand_over(n, block(hop))

    def ev_short(n, hop):
        wait(piece(n, block(-hop)), zr_sem.at[n % Z_SEMS, 4 + hop - 1])
        if hop < 3:
            forward_short(n, hop)
        hand_over(n, block(-hop))

    def handed_over(n):
        wait(b_all.at[0, pl.ds(0, Z_N), :, lanes_of(n)], dr_sem.at[n])

    def dot(a, b):
        return jnp.dot(a.reshape(-1, cols), b.reshape(cols, -1), preferred_element_type=jnp.float32)

    def sum_sem(n, q):
        return 2 * SPLIT + (n - SPLIT) % C_SEMS if isinstance(q, slice) else 2 * n + q

    def sum_stage(n, g, q, m, lanes, first, size, when, reuse, old):
        slot = n % SLOTS
        keep = rest if isinstance(lanes, slice) else pl.ds(0, narrow)
        arrivals = sum_sem(n, q)

        def pass_on(src, ssem):
            for d in range(2):
                send(src.at[d], crecv.at[m, g, d, :, q, :, lanes], ssem, cr_sem.at[arrivals, g], at_x(1 - 2 * d))

        def arrived():
            wait(crecv.at[m, g - 1, :, :, q, :, lanes], cr_sem.at[arrivals, g - 1])

        def begin():
            reuse(lambda: wait(c0.at[slot, :, :, :, :, old], c0_sem.at[slot]))
            c0[slot, :, :, q, :, keep] = prod[:, :, q, :, keep]
            pass_on(c0.at[slot, :, :, q, :, keep], c0_sem.at[slot])

        def middle():
            arrived()
            crecv[m, g - 1, :, :, q, :, lanes] += prod[:, :, q, :, keep]
            pass_on(crecv.at[m, g - 1, :, :, q, :, lanes], cs_sem.at[m // 4])

        def end():
            arrived()
            total = crecv[m, g - 1, :, :, q, :, lanes] + prod[:, :, q, :, keep]
            c_out[:, :, q, :, pl.ds(pl.multiple_of(first, size), size)] = total.astype(c_out.dtype)

        a = a_all[g, :, :, q]
        prod[:, :, q, :, keep] = dot(a, b_all[m, :, :, lanes]).reshape(a.shape[:-1] + (size,))
        when(g == 0, begin)
        when((g == 1) | (g == 2), middle)
        when(g == 3, end)

    def branch(cond, fn):
        pl.when(cond)(fn)

    def fixed(cond, fn):
        if cond:
            fn()

    def sum_loop(code, split, wide):
        n, g, q = code // 8, code // 2 % 4, code % 2
        if split:
            pl.when(n < SPLIT)(lambda: sum_stage(n, g, q, n, rest, n * width, width, branch, lambda fn: None, rest))
        if wide:
            pl.when(n >= SPLIT)(lambda: sum_stage(n, g, rest, n, rest, n * width, width, branch,
                                                  pl.when(n >= SLOTS), rest))

    def sum_narrow(n, g):
        m, half = chunk(n)
        old = rest if n - SLOTS < WIDE else pl.ds(0, narrow)
        sum_stage(n, g, rest, m, lanes_of(n), m * width + half * narrow, narrow, fixed, lambda fn: fn(), old)

    chunks = range(CHUNKS)
    queues = {"a": [(ev_own, (n,)) for n in chunks]}
    for hop in range(1, 5):
        queues["abcde"[hop]] = [(ev_long, (n, hop)) for n in chunks]
    for hop in range(1, 4):
        queues["efgh"[hop]] = [(ev_short, (n, hop)) for n in chunks]
    by_half = [(o, r) for o in range(2) for r in range(2)]
    by_row = [(o, r) for r in range(2) for o in range(2)]
    queues["i"] = [(ev_s1, p) for p in by_half]
    queues["j"] = [(ev_r1, p) for p in by_half]
    queues["k"] = [(ev_s2, p) for p in by_half]
    queues["l"] = [(ev_s2f, p) for p in by_row]
    queues["m"] = [(ev_r2, p) for p in by_row]
    groups = [(g, r) for g in range(4) for r in range(2)]
    queues["n"] = [(ev_ag, p) for p in groups]
    queues["o"] = [(ev_fw, p + (d,)) for p in groups for d in range(2)]
    for g in range(4):
        queues["pqrs"[g]] = [(None, (n, g, 0 if n < SPLIT else ALL)) for n in chunks]
        queues["tuvw"[g]] = [(None, (n, g, 1)) for n in range(SPLIT)]

    steps, before, complete, handed = [], [], set(), set()
    for letter in "".join(PROGRAM):
        fn, args = queues[letter].pop(0)
        if fn is not None:
            before.append((fn, args))
            continue
        n, g, q = args
        for r in (range(2) if q == ALL else (q,)):
            if (g, r) not in complete:
                complete.add((g, r))
                before.append((group_complete, (g, r)))
        if n not in handed:
            handed.add(n)
            before.append((handed_over, (n,)))
        if n >= WIDE:
            before.append((sum_narrow, (n, g)))
        else:
            steps.append((before, (n * 4 + g) * 2 + q % 2, q != ALL))
            before = []

    def run(todo):
        for fn, args in todo:
            fn(*args)

    def in_loop(first, last):
        part = steps[first:last]

        def body(k, carry):
            code = part[0][1]
            for i, (todo, this, _) in enumerate(part):
                code = jnp.where(k == first + i, this, code)
                if todo:
                    pl.when(k == first + i)(lambda: run(todo))
            sum_loop(code, any(s for _, _, s in part), any(not s for _, _, s in part))
            return carry

        lax.fori_loop(first, last, body, 0)

    for first in range(0, len(steps), LOOP):
        in_loop(first, min(first + LOOP, len(steps)))
    run(before)

    for i in range(BLOCKS // 4):
        wait(b_all.at[pl.ds(0, 4), pl.ds(0, 15)], zs_sem.at[i])
        wait(crecv.at[pl.ds(0, 4), pl.ds(0, 2)], cs_sem.at[i])
    wait(b_all.at[pl.ds(0, 5)], as_sem)
    for n in range(CHUNKS - SLOTS, CHUNKS):
        keep = rest if n < WIDE else pl.ds(0, narrow)
        wait(c0.at[n % SLOTS, :, :, :, :, keep], c0_sem.at[n % SLOTS])


def solution(mesh):
    def local_product(a_blk, b_blk):
        rows, cols = a_blk.shape
        width = cols // BLOCKS
        few = rows // 16
        dma = pltpu.SemaphoreType.DMA
        c_blk = pl.pallas_call(
            kernel,
            name="matmul_3d",
            out_shape=pltpu.VMEM((2, 4, 2, few, cols), jnp.bfloat16),
            in_specs=[pl.BlockSpec(memory_space=pl.ANY)] * 2,
            out_specs=pl.BlockSpec(memory_space=pltpu.VMEM),
            scratch_shapes=[
                pltpu.VMEM((2, 4, 2, few, cols), jnp.bfloat16),
                pltpu.VMEM((4, 2, 4, 2, few, cols), jnp.bfloat16),
                pltpu.VMEM((3, 2, 2, few, cols), jnp.bfloat16),
                pltpu.VMEM((2, 2, 2, few, cols // 2), jnp.bfloat16),
                pltpu.VMEM((2, 2, 2, few, cols // 2), jnp.bfloat16),
                pltpu.VMEM((BLOCKS, 2 * Z_N, rows, width), jnp.bfloat16),
                pltpu.VMEM((BLOCKS, 3, 2, 4, 2, few, width), jnp.float32),
                pltpu.VMEM((SLOTS, 2, 4, 2, few, width), jnp.float32),
                pltpu.VMEM((2, 4, 2, few, width), jnp.float32),
                dma((4,)), dma((Z_SEMS, 7)), dma((BLOCKS // 4,)), dma((CHUNKS,)),
                dma((3, 2, 2)), dma((2, 2)), dma((2, 2)), dma((3, 2)), dma((4, 2, 2)), dma((4, 2)), dma,
                dma((2 * SPLIT + C_SEMS, 3)), dma((BLOCKS // 4,)), dma((SLOTS,)),
            ],
            compiler_params=pltpu.CompilerParams(
                collective_id=0, has_side_effects=True, vmem_limit_bytes=61 * 1024 * 1024
            ),
        )(a_blk.reshape(2, 4, 2, few, cols), b_blk)
        return c_blk.reshape(rows, cols)

    block_spec = P(("row", "depth"), "col")
    return jax.shard_map(local_product, mesh=mesh, in_specs=(block_spec, block_spec), out_specs=block_spec, check_vma=False)
```
